8 devices in a mesh: dp: 1 (over z), sp: 8 (over y, x, core).
Axes of the slice: x: 2, y: 2, z: 1, core: 2. Of those that a mesh axis runs over, the one named last changes fastest.
Arguments:
- hidden: bfloat16 [128, 6144], P('dp')
- ln_gamma: float32 [6144], replicated
- ln_beta: float32 [6144], replicated
- w_qkv: bfloat16 [6144, 6400], replicated
- w_out: bfloat16 [6144, 6144], replicated
- w_up: bfloat16 [6144, 24576], P(None, 'sp')
- w_down: bfloat16 [24576, 6144], P('sp')
- k_cache: bfloat16 [128, 4096, 128], P('dp', 'sp')
- v_cache: bfloat16 [128, 4096, 128], P('dp', 'sp')
- positions: int32 [128], P('dp')
Outputs:
- output 1: bfloat16 [128, 6144], P('dp')
- output 2: bfloat16 [128, 4096, 128], P('dp', 'sp')
- output 3: bfloat16 [128, 4096, 128], P('dp', 'sp')
All inputs are finite; a program needn't handle non-finite values.
Results may differ from the reference program's by a relative error of at most 0.00574734.
Values sent between devices are 32-bit elements.
A program may use at most 1.25 GiB of HBM per device.

```python
import jax
import jax.numpy as jnp
from jax import lax

BATCH_ROWS = 128
D_MODEL = 6144
N_HEADS = 48
HEAD_DIM = 128
FF_DIM = 24576
SEQ_SHARD = 512
N_SHARDS = 8
SEQ_LEN = N_SHARDS * SEQ_SHARD
LN_EPS = 1e-5
ROPE_BASE = 10000.0
NEG_FILL = -1e30


def setup_inputs(seed: int = 0, part: int = 0) -> dict:
    base_key = jax.random.key(seed)
    weight_keys = jax.random.split(base_key, 6)
    part_keys = jax.random.split(jax.random.fold_in(base_key, part), 4)
    hidden = jax.random.normal(part_keys[0], (BATCH_ROWS, D_MODEL), jnp.float32).astype(jnp.bfloat16)
    ln_gamma = 1.0 + 0.3 * jax.random.normal(weight_keys[0], (D_MODEL,), jnp.float32)
    ln_beta = 0.3 * jax.random.normal(weight_keys[1], (D_MODEL,), jnp.float32)
    w_qkv = (jax.random.normal(weight_keys[2], (D_MODEL, (N_HEADS + 2) * HEAD_DIM), jnp.float32) * D_MODEL ** -0.5).astype(jnp.bfloat16)
    out_scale = 0.5 * SEQ_LEN ** 0.5 * (N_HEADS * HEAD_DIM) ** -0.5
    w_out = (jax.random.normal(weight_keys[3], (N_HEADS * HEAD_DIM, D_MODEL), jnp.float32) * out_scale).astype(jnp.bfloat16)
    w_up = (jax.random.normal(weight_keys[4], (D_MODEL, FF_DIM), jnp.float32) * D_MODEL ** -0.5).astype(jnp.bfloat16)
    w_down = (jax.random.normal(weight_keys[5], (FF_DIM, D_MODEL), jnp.float32) * FF_DIM ** -0.5).astype(jnp.bfloat16)
    k_cache = jax.random.normal(part_keys[1], (BATCH_ROWS, SEQ_LEN, HEAD_DIM), jnp.float32).astype(jnp.bfloat16)
    v_cache = jax.random.normal(part_keys[2], (BATCH_ROWS, SEQ_LEN, HEAD_DIM), jnp.float32).astype(jnp.bfloat16)
    positions = jax.random.randint(part_keys[3], (BATCH_ROWS,), SEQ_LEN // 2, SEQ_LEN, dtype=jnp.int32)
    positions = positions.at[0].set(SEQ_LEN - 1).at[1].set(SEQ_LEN // 2)
    return {'hidden': hidden, 'ln_gamma': ln_gamma, 'ln_beta': ln_beta, 'w_qkv': w_qkv, 'w_out': w_out, 'w_up': w_up, 'w_down': w_down, 'k_cache': k_cache, 'v_cache': v_cache, 'positions': positions}


def layer_norm(hidden, ln_gamma, ln_beta):
    hidden_f32 = hidden.astype(jnp.float32)
    row_mean = jnp.mean(hidden_f32, axis=-1, keepdims=True)
    centered = hidden_f32 - row_mean
    row_var = jnp.mean(centered * centered, axis=-1, keepdims=True)
    return (centered * lax.rsqrt(row_var + LN_EPS) * ln_gamma + ln_beta).astype(jnp.bfloat16)


def rotary_tables(positions, head_dim):
    inv_freq = 1.0 / (ROPE_BASE ** (jnp.arange(0, head_dim, 2, dtype=jnp.float32) / head_dim))
    angles = positions.astype(jnp.float32)[:, None] * inv_freq[None, :]
    cos_half = jnp.cos(angles)
    sin_half = jnp.sin(angles)
    return jnp.concatenate([cos_half, cos_half], axis=-1), jnp.concatenate([sin_half, sin_half], axis=-1)


def apply_rotary(vecs, cos_full, sin_full):
    vecs_f32 = vecs.astype(jnp.float32)
    half_dim = vecs.shape[-1] // 2
    rotated = jnp.concatenate([-vecs_f32[..., half_dim:], vecs_f32[..., :half_dim]], axis=-1)
    return (vecs_f32 * cos_full + rotated * sin_full).astype(jnp.bfloat16)


def row_attention(row_inputs):
    q_row, k_row, v_row, pos_row = row_inputs
    scores = jnp.dot(q_row, k_row.T, preferred_element_type=jnp.float32) * HEAD_DIM ** -0.5
    scores = scores.reshape(N_HEADS, N_SHARDS, SEQ_SHARD)
    valid_mask = (jnp.arange(SEQ_LEN) <= pos_row).reshape(N_SHARDS, SEQ_SHARD)
    masked = jnp.where(valid_mask, scores, NEG_FILL)
    block_max = jnp.max(masked, axis=-1)
    exp_scores = jnp.where(valid_mask, jnp.exp(masked - block_max[..., None]), 0.0)
    block_sum = jnp.sum(exp_scores, axis=-1)
    block_ctx = jnp.einsum('hcs,csd->hcd', exp_scores.astype(jnp.bfloat16).astype(jnp.float32), v_row.reshape(N_SHARDS, SEQ_SHARD, HEAD_DIM).astype(jnp.float32))
    top_max = jnp.max(block_max, axis=-1)
    scale_w = jnp.exp(block_max - top_max[:, None])
    total_sum = jnp.sum(block_sum * scale_w, axis=-1)
    total_ctx = jnp.sum(block_ctx * scale_w[..., None], axis=1)
    return (total_ctx / total_sum[:, None]).astype(jnp.bfloat16)


def reference(hidden, ln_gamma, ln_beta, w_qkv, w_out, w_up, w_down, k_cache, v_cache, positions):
    normed = layer_norm(hidden, ln_gamma, ln_beta)
    qkv_proj = jnp.dot(normed, w_qkv, preferred_element_type=jnp.float32).astype(jnp.bfloat16)
    qkv_proj = qkv_proj.reshape(BATCH_ROWS, N_HEADS + 2, HEAD_DIM)
    cos_full, sin_full = rotary_tables(positions, HEAD_DIM)
    q_rot = apply_rotary(qkv_proj[:, :N_HEADS], cos_full[:, None, :], sin_full[:, None, :])
    k_rot = apply_rotary(qkv_proj[:, N_HEADS], cos_full, sin_full)
    v_new = qkv_proj[:, N_HEADS + 1]
    write_mask = (jnp.arange(SEQ_LEN)[None, :] == positions[:, None])[:, :, None]
    k_next = jnp.where(write_mask, k_rot[:, None, :], k_cache)
    v_next = jnp.where(write_mask, v_new[:, None, :], v_cache)
    context = lax.map(row_attention, (q_rot, k_next, v_next, positions))
    attn_out = jnp.dot(context.reshape(BATCH_ROWS, N_HEADS * HEAD_DIM), w_out, preferred_element_type=jnp.float32)
    up_proj = jnp.dot(normed, w_up, preferred_element_type=jnp.float32)
    activated = jax.nn.gelu(up_proj, approximate=False).astype(jnp.bfloat16)
    mlp_out = jnp.dot(activated, w_down, preferred_element_type=jnp.float32)
    out_hidden = (hidden.astype(jnp.float32) + attn_out + mlp_out).astype(jnp.bfloat16)
    return (out_hidden, k_next, v_next)
```

```python
import functools

import jax
import jax.numpy as jnp
from jax import lax
from jax.experimental import pallas as pl
from jax.experimental.pallas import tpu as pltpu
from jax.sharding import PartitionSpec as P

LN_EPS = 1e-5
ROPE_BASE = 10000.0
NEG_FILL = -1e30
MESH = pl.DeviceIdType.MESH
VMEM_LIMIT = 67_000_000

ROWS = 128
D = 6144
HD = 128
NH = 48
SEQ = 512
FF = 3072
F32 = jnp.float32
BF16 = jnp.bfloat16


def rotary_tables(positions):
    inv_freq = 1.0 / (ROPE_BASE ** (jnp.arange(0, HD, 2, dtype=F32) / HD))
    angles = positions.astype(F32)[:, None] * inv_freq[None, :]
    cos_half = jnp.cos(angles)
    sin_half = jnp.sin(angles)
    return jnp.concatenate([cos_half, cos_half], axis=-1), jnp.concatenate([-sin_half, sin_half], axis=-1)


def place():
    sp = lax.axis_index('sp')
    core = lax.rem(sp, 2)
    x = lax.rem(sp // 2, 2)
    y = sp // 4
    return y, x, core


def device(y, x, core):
    return {'sp': (y * 2 + x) * 2 + core}


def enter(peers):
    barrier = pltpu.get_barrier_semaphore()
    for peer in peers:
        pl.semaphore_signal(barrier, inc=1, device_id=peer, device_id_type=MESH)
    pl.semaphore_wait(barrier, len(peers))


Q_BLOCK = 640
Q_STEPS = 5
Q_SLOTS = 6


def qkv_kernel(hid, gam, bet, cos, sin, w, qkv, normed, wbuf, mine, wsem, lsem, ssem, rsem):
    y, x, core = place()
    partner = device(y, x, 1 - core)

    def fetch(j, half):
        col = pl.multiple_of(core * 3200 + j * Q_BLOCK, 128)
        slot = lax.rem(2 * j + half, Q_SLOTS)
        return pltpu.make_async_copy(w.at[pl.ds(half * 3072, 3072), pl.ds(col, Q_BLOCK)], wbuf.at[slot], wsem.at[slot])

    for j in range(Q_SLOTS // 2):
        fetch(j, 0).start()
        fetch(j, 1).start()
    enter([partner])

    def norm_rows(i, carry):
        rows = pl.ds(pl.multiple_of(i * 16, 16), 16)
        v = hid[rows, :].astype(F32)
        mean = jnp.sum(v, axis=-1, keepdims=True) * (1.0 / D)
        cen = v - mean
        var = jnp.sum(cen * cen, axis=-1, keepdims=True) * (1.0 / D)
        normed[rows, :] = (cen * lax.rsqrt(var + LN_EPS) * gam[...] + bet[...]).astype(BF16)
        return carry

    lax.fori_loop(0, ROWS // 16, norm_rows, 0)

    def remote(j):
        return pltpu.make_async_remote_copy(
            src_ref=mine.at[pl.ds(j * 5, 5)], dst_ref=qkv.at[pl.ds(core * 25 + j * 5, 5)],
            send_sem=ssem.at[j], recv_sem=rsem.at[j], device_id=partner, device_id_type=MESH)

    def local(j):
        return pltpu.make_async_copy(mine.at[pl.ds(j * 5, 5)], qkv.at[pl.ds(core * 25 + j * 5, 5)], lsem.at[j])

    def block(j, carry):
        fetch(j, 0).wait()
        fetch(j, 1).wait()
        s0 = lax.rem(2 * j, Q_SLOTS)
        acc = jnp.dot(normed[:, :3072], wbuf[s0], preferred_element_type=F32)
        acc += jnp.dot(normed[:, 3072:], wbuf[s0 + 1], preferred_element_type=F32)

        @pl.when(j < Q_STEPS - Q_SLOTS // 2)
        def _():
            fetch(j + Q_SLOTS // 2, 0).start()
            fetch(j + Q_SLOTS // 2, 1).start()

        for h in range(5):
            v = acc[:, h * HD:(h + 1) * HD].astype(BF16).astype(F32)
            rot = (v * cos[...] + pltpu.roll(v, 64, 1) * sin[...]).astype(BF16).astype(F32)
            if h == 4:
                rot = jnp.where(core * 25 + j * 5 + h == NH + 1, v, rot)
            mine[j * 5 + h] = rot
        remote(j).start()
        local(j).start()
        return carry

    lax.fori_loop(0, Q_STEPS, block, 0)

    def drain(j, carry):
        local(j).wait()
        remote(j).wait()
        return carry

    lax.fori_loop(0, Q_STEPS, drain, 0)


def qkv_call(hidden, gam, bet, cos, sin, w_qkv):
    vm = pl.BlockSpec(memory_space=pltpu.VMEM)
    anyspace = pl.BlockSpec(memory_space=pl.ANY)
    return pl.pallas_call(
        qkv_kernel,
        out_shape=(jax.ShapeDtypeStruct((NH + 2, ROWS, HD), F32), jax.ShapeDtypeStruct((ROWS, D), BF16)),
        in_specs=[vm, vm, vm, vm, vm, anyspace],
        out_specs=(anyspace, vm),
        scratch_shapes=[
            pltpu.VMEM((Q_SLOTS, 3072, Q_BLOCK), BF16),
            pltpu.VMEM((25, ROWS, HD), F32),
            pltpu.SemaphoreType.DMA((Q_SLOTS,)),
            pltpu.SemaphoreType.DMA((Q_STEPS,)),
            pltpu.SemaphoreType.DMA((Q_STEPS,)),
            pltpu.SemaphoreType.DMA((Q_STEPS,)),
        ],
        compiler_params=pltpu.CompilerParams(collective_id=0, has_side_effects=True, vmem_limit_bytes=VMEM_LIMIT),
        cost_estimate=pl.CostEstimate(flops=2 * ROWS * D * 3200, bytes_accessed=D * 6400, transcendentals=0),
        name='qkv',
    )(hidden, gam, bet, cos, sin, w_qkv)


A_ROWS = 8
A_STEPS = ROWS // A_ROWS
A_SLOTS = 4


def attn_kernel(lp_ref, qkv, kc, vc, o, ml, kn, vn, kbuf, vbuf, isem, osem):
    i = pl.program_id(0)

    def fetch(step):
        slot = lax.rem(step, A_SLOTS)
        rows = pl.ds(step * A_ROWS, A_ROWS)
        return (pltpu.make_async_copy(kc.at[rows], kbuf.at[slot], isem.at[0, slot]),
                pltpu.make_async_copy(vc.at[rows], vbuf.at[slot], isem.at[1, slot]))

    def flush(step):
        slot = lax.rem(step, A_SLOTS)
        rows = pl.ds(step * A_ROWS, A_ROWS)
        return (pltpu.make_async_copy(kbuf.at[slot], kn.at[rows], osem.at[0, slot]),
                pltpu.make_async_copy(vbuf.at[slot], vn.at[rows], osem.at[1, slot]))

    @pl.when(i == 0)
    def _():
        for s in range(2):
            for c in fetch(s):
                c.start()

    @pl.when(i >= 2)
    def _():
        for c in flush(i - 2):
            c.wait()

    @pl.when(i + 2 < A_STEPS)
    def _():
        for c in fetch(i + 2):
            c.start()

    for c in fetch(i):
        c.wait()
    slot = lax.rem(i, A_SLOTS)

    for r in range(A_ROWS):
        lp = lp_ref[i * A_ROWS + r]
        base = pl.multiple_of((jnp.clip(lp, 0, SEQ - 1) // 16) * 16, 16)
        hit = base + lax.broadcasted_iota(jnp.int32, (16, HD), 0) == lp
        for buf, src in ((kbuf, NH), (vbuf, NH + 1)):
            new = jnp.broadcast_to(qkv[src, r:r + 1, :], (16, HD))
            old = buf[slot, r, pl.ds(base, 16), :].astype(F32)
            buf[slot, r, pl.ds(base, 16), :] = jnp.where(hit, new, old).astype(BF16)

    lane = lax.broadcasted_iota(jnp.int32, (NH, HD), 1)
    mcol = jnp.zeros((NH, HD), F32)
    lcol = jnp.zeros((NH, HD), F32)
    for r in range(A_ROWS):
        lp = lp_ref[i * A_ROWS + r]
        q = qkv[0:NH, r, :].astype(BF16)
        s = lax.dot_general(q, kbuf[slot, r], (((1,), (1,)), ((), ())), preferred_element_type=F32) * (HD ** -0.5)
        valid = lax.broadcasted_iota(jnp.int32, (NH, SEQ), 1) <= lp
        s = jnp.where(valid, s, NEG_FILL)
        m = jnp.max(s, axis=-1, keepdims=True)
        e = jnp.where(valid, jnp.exp(s - m), 0.0)
        l = jnp.sum(e, axis=-1, keepdims=True)
        o[:, r, :] = jnp.dot(e.astype(BF16), vbuf[slot, r], preferred_element_type=F32)
        mcol = jnp.where(lane == r, m, mcol)
        lcol = jnp.where(lane == r, l, lcol)
    pad = jnp.zeros((16, HD), F32)
    ml[...] = jnp.transpose(jnp.concatenate([mcol, pad, lcol, pad], axis=0))[:A_ROWS]

    for c in flush(i):
        c.start()

    @pl.when(i == A_STEPS - 1)
    def _():
        for step in (i - 1, i):
            for c in flush(step):
                c.wait()


def attn_call(local_pos, qkv, k_cache, v_cache):
    anyspace = pl.BlockSpec(memory_space=pl.ANY)
    cache = jax.ShapeDtypeStruct((ROWS, SEQ, HD), BF16)
    return pl.pallas_call(
        attn_kernel,
        out_shape=(jax.ShapeDtypeStruct((NH, ROWS, HD), F32), jax.ShapeDtypeStruct((ROWS, HD), F32), cache, cache),
        grid_spec=pltpu.PrefetchScalarGridSpec(
            num_scalar_prefetch=1,
            grid=(A_STEPS,),
            in_specs=[pl.BlockSpec((NH + 2, A_ROWS, HD), lambda i, p: (0, i, 0)), anyspace, anyspace],
            out_specs=(pl.BlockSpec((NH, A_ROWS, HD), lambda i, p: (0, i, 0)), pl.BlockSpec((A_ROWS, HD), lambda i, p: (i, 0)),
                       anyspace, anyspace),
            scratch_shapes=[
                pltpu.VMEM((A_SLOTS, A_ROWS, SEQ, HD), BF16),
                pltpu.VMEM((A_SLOTS, A_ROWS, SEQ, HD), BF16),
                pltpu.SemaphoreType.DMA((2, A_SLOTS)),
                pltpu.SemaphoreType.DMA((2, A_SLOTS)),
            ]),
        compiler_params=pltpu.CompilerParams(vmem_limit_bytes=VMEM_LIMIT, dimension_semantics=('arbitrary',)),
        cost_estimate=pl.CostEstimate(flops=4 * ROWS * NH * SEQ * HD, bytes_accessed=8 * ROWS * SEQ * HD, transcendentals=0),
        name='attn',
    )(local_pos, qkv, k_cache, v_cache)


W_SLOTS = 8
UP_STEPS = 12
DOWN_STEPS = 12
NK = 2
CT = NH // NK


def tail_kernel(normed, hid, ml_in, o_hbm, w_up, w_down, w_out, out,
                wbuf, wobuf, act, part, mine, orecv0, orecv1, orecv2, ml0, mlr, precv0, precv1, precv2, gath, ctx,
                wsem, wosem, mysem, osend, orecv, msend, mrecv, psend, precv, gsend, grecv):
    y, x, core = place()
    first = 1 - core
    partner = device(y, x, 1 - core)
    x_peer = (y, 1 - x, core)
    y_peer = (1 - y, x, core)
    n1 = {'sp': jnp.where(core == 0, device(*x_peer)['sp'], device(*y_peer)['sp'])}
    n2 = {'sp': jnp.where(core == 0, device(*y_peer)['sp'], device(*x_peer)['sp'])}
    a = x * first + y * core
    b = y * first + x * core

    def fetch_up(step):
        slot = lax.rem(step, W_SLOTS)
        col = pl.multiple_of((step // 2) * 512, 512)
        row = pl.multiple_of(lax.rem(step, 2) * 3072, 3072)
        return pltpu.make_async_copy(w_up.at[pl.ds(row, 3072), pl.ds(col, 512)], wbuf.at[slot], wsem.at[slot])

    def fetch_down(step):
        slot = lax.rem(step + UP_STEPS, W_SLOTS)
        col = pl.multiple_of(step * 512, 512)
        return pltpu.make_async_copy(w_down.at[:, pl.ds(col, 512)], wbuf.at[slot], wsem.at[slot])

    head0 = core * 24 + a * 12 + b * 6
    wo_copy = pltpu.make_async_copy(w_out.at[pl.ds(pl.multiple_of(head0 * HD, HD), 6 * HD)], wobuf, wosem)
    my_copy = pltpu.make_async_copy(o_hbm.at[pl.ds(core * 24, 24)], mine, mysem)

    my_copy.start()
    enter([partner, n1, n2])

    def remote(src, dst, send, recv, peer):
        return pltpu.make_async_remote_copy(src_ref=src, dst_ref=dst, send_sem=send, recv_sem=recv,
                                            device_id=peer, device_id_type=MESH)

    o_send0 = remote(o_hbm.at[pl.ds((1 - core) * 24, 24)], orecv0, osend.at[0], orecv.at[0], partner)
    m_send0 = remote(ml_in, mlr.at[0], msend.at[0], mrecv.at[0], partner)
    m_send0.start()
    o_send0.start()
    for s in range(W_SLOTS):
        fetch_up(s).start()

    def up_block(n, carry):
        fetch_up(2 * n).wait()
        s0 = lax.rem(2 * n, W_SLOTS)
        acc = jnp.dot(normed[:, :3072], wbuf[s0], preferred_element_type=F32)
        fetch_up(2 * n + 1).wait()
        acc += jnp.dot(normed[:, 3072:], wbuf[s0 + 1], preferred_element_type=F32)
        for half in range(2):
            nxt = 2 * n + half + W_SLOTS

            @pl.when(nxt < UP_STEPS)
            def _():
                fetch_up(nxt).start()

            @pl.when(nxt >= UP_STEPS)
            def _():
                fetch_down(nxt - UP_STEPS).start()

        act[:, pl.ds(pl.multiple_of(n * 512, 512), 512)] = (
            0.5 * acc * (1.0 + lax.erf(acc * (2.0 ** -0.5)))).astype(BF16)
        return carry

    def down_block(n, carry):
        fetch_down(n).wait()
        acc = jnp.dot(act[...], wbuf[lax.rem(n + UP_STEPS, W_SLOTS)], preferred_element_type=F32)

        @pl.when(n + W_SLOTS < DOWN_STEPS)
        def _():
            fetch_down(n + W_SLOTS).start()

        for t in range(4):
            part[n * 4 + t] = acc[:, t * HD:(t + 1) * HD]
        return carry

    lanes = lax.broadcasted_iota(jnp.int32, (ROWS, HD), 1)

    def merge(stats, theirs, dst, dst0, recv, n):
        top = jnp.maximum(stats, theirs)
        w1 = jnp.exp(stats - top)
        w2 = jnp.exp(theirs - top)
        for h in range(n):
            dst[dst0 + h] = dst[dst0 + h] * w1[:, h:h + 1] + recv[h] * w2[:, h:h + 1]
        total = stats * pltpu.roll(w1, 64, 1) + theirs * pltpu.roll(w2, 64, 1)
        return jnp.where(lanes < 64, top, total)

    def shift(v, by):
        return pltpu.roll(v, lax.rem(HD - by, HD), 1)

    lax.fori_loop(0, 2, up_block, 0)

    my_copy.wait()
    m_send0.wait()
    o_send0.wait()
    ml0[0] = merge(shift(ml_in[...], core * 24), shift(mlr[0], core * 24), mine, 0, orecv0, 24)
    o_send1 = remote(mine.at[pl.ds((1 - a) * 12, 12)], orecv1, osend.at[1], orecv.at[1], n1)
    m_send1 = remote(ml0.at[0], mlr.at[1], msend.at[1], mrecv.at[1], n1)
    m_send1.start()
    o_send1.start()
    wo_copy.start()

    lax.fori_loop(2, 6, up_block, 0)
    lax.fori_loop(0, 4, down_block, 0)

    m_send1.wait()
    o_send1.wait()
    ml0[1] = merge(shift(ml0[0], a * 12), shift(mlr[1], a * 12), mine, a * 12, orecv1, 12)
    o_send2 = remote(mine.at[pl.ds(a * 12 + (1 - b) * 6, 6)], orecv2, osend.at[2], orecv.at[2], n2)
    m_send2 = remote(ml0.at[1], mlr.at[2], msend.at[2], mrecv.at[2], n2)
    m_send2.start()
    o_send2.start()

    lax.fori_loop(4, DOWN_STEPS, down_block, 0)

    m_send2.wait()
    o_send2.wait()
    mine0 = a * 12 + b * 6
    stats = merge(shift(ml0[1], b * 6), shift(mlr[2], b * 6), mine, mine0, orecv2, 6)
    for h in range(6):
        ctx[:, h * HD:(h + 1) * HD] = (mine[mine0 + h] / stats[:, 64 + h:65 + h]).astype(BF16)
    wo_copy.wait()

    half, quarter, eighth = CT // 2, CT // 4, CT // 8

    def p_send0(k):
        return remote(part.at[pl.ds(k * CT + (1 - core) * half, half)], precv0.at[k], psend.at[0, k], precv.at[0, k], partner)

    def p_send1(k):
        return remote(part.at[pl.ds(k * CT + core * half + (1 - a) * quarter, quarter)], precv1.at[k],
                      psend.at[1, k], precv.at[1, k], n1)

    def p_send2(k):
        return remote(part.at[pl.ds(k * CT + core * half + a * quarter + (1 - b) * eighth, eighth)], precv2.at[k],
                      psend.at[2, k], precv.at[2, k], n2)

    def spread(k, start, count, level, peer):
        where = gath.at[pl.ds(k * CT + start, count)]
        return remote(where, where, gsend.at[level, k], grecv.at[level, k], peer)

    def g_send2(k):
        return spread(k, core * half + a * quarter + b * eighth, eighth, 0, n2)

    def g_send1(k):
        return spread(k, core * half + a * quarter, quarter, 1, n1)

    def g_send0(k):
        return spread(k, core * half, half, 2, partner)

    def stage(s, k):
        if s == 0:
            def project(n, carry):
                t0 = k * CT + n * 4
                acc = jnp.dot(ctx[...], wobuf[:, pl.ds(pl.multiple_of(t0 * HD, 512), 512)], preferred_element_type=F32)
                for t in range(4):
                    part[t0 + t] += acc[:, t * HD:(t + 1) * HD]
                return carry

            lax.fori_loop(0, CT // 4, project, 0)
            p_send0(k).start()
        elif s == 1:
            p_send0(k).wait()
            base = k * CT + core * half
            part[pl.ds(base, half)] = part[pl.ds(base, half)] + precv0[k]
            p_send1(k).start()
        elif s == 2:
            p_send1(k).wait()
            base = k * CT + core * half + a * quarter
            part[pl.ds(base, quarter)] = part[pl.ds(base, quarter)] + precv1[k]
            p_send2(k).start()
        elif s == 3:
            p_send2(k).wait()
            base = k * CT + core * half + a * quarter + b * eighth
            for t in range(eighth):
                col = pl.multiple_of((base + t) * HD, HD)
                total = hid[:, pl.ds(col, HD)].astype(F32) + (part[base + t] + precv2[k, t])
                gath[base + t] = total.astype(BF16).astype(F32)
            g_send2(k).start()
        elif s == 4:
            g_send2(k).wait()
            g_send1(k).start()
        elif s == 5:
            g_send1(k).wait()
            g_send0(k).start()
        else:
            g_send0(k).wait()
            for t in range(CT):
                col = (k * CT + t) * HD
                out[:, col:col + HD] = gath[k * CT + t].astype(BF16)

    for wave in range(NK + 6):
        for k in range(NK):
            if 0 <= wave - k < 7:
                stage(wave - k, k)


def tail_call(normed, hidden, ml, o, w_up, w_down, w_out):
    vm = pl.BlockSpec(memory_space=pltpu.VMEM)
    anyspace = pl.BlockSpec(memory_space=pl.ANY)
    dma = pltpu.SemaphoreType.DMA
    return pl.pallas_call(
        tail_kernel,
        out_shape=jax.ShapeDtypeStruct((ROWS, D), BF16),
        in_specs=[vm, vm, vm, anyspace, anyspace, anyspace, anyspace],
        out_specs=vm,
        scratch_shapes=[
            pltpu.VMEM((W_SLOTS, 3072, 512), BF16),
            pltpu.VMEM((6 * HD, D), BF16),
            pltpu.VMEM((ROWS, FF), BF16),
            pltpu.VMEM((NH, ROWS, HD), F32),
            pltpu.VMEM((24, ROWS, HD), F32),
            pltpu.VMEM((24, ROWS, HD), F32),
            pltpu.VMEM((12, ROWS, HD), F32),
            pltpu.VMEM((6, ROWS, HD), F32),
            pltpu.VMEM((2, ROWS, HD), F32),
            pltpu.VMEM((3, ROWS, HD), F32),
            pltpu.VMEM((NK, CT // 2, ROWS, HD), F32),
            pltpu.VMEM((NK, CT // 4, ROWS, HD), F32),
            pltpu.VMEM((NK, CT // 8, ROWS, HD), F32),
            pltpu.VMEM((NH, ROWS, HD), F32),
            pltpu.VMEM((ROWS, 6 * HD), BF16),
            dma((W_SLOTS,)), dma, dma, dma((3,)), dma((3,)), dma((3,)), dma((3,)),
            dma((3, NK)), dma((3, NK)), dma((3, NK)), dma((3, NK)),
        ],
        compiler_params=pltpu.CompilerParams(collective_id=1, has_side_effects=True, vmem_limit_bytes=VMEM_LIMIT),
        cost_estimate=pl.CostEstimate(flops=4 * ROWS * D * FF, bytes_accessed=4 * D * FF, transcendentals=0),
        name='tail',
    )(normed, hidden, ml, o, w_up, w_down, w_out)


def device_step(hidden, ln_gamma, ln_beta, w_qkv, w_out, w_up, w_down, k_cache, v_cache, positions):
    cos, sin = rotary_tables(positions)
    local_pos = positions - lax.axis_index('sp') * SEQ
    qkv, normed = qkv_call(hidden, ln_gamma[None, :], ln_beta[None, :], cos, sin, w_qkv)
    o, ml, k_next, v_next = attn_call(local_pos, qkv, k_cache, v_cache)
    out = tail_call(normed, hidden, ml, o, w_up, w_down, w_out)
    return out, k_next, v_next


def solution(mesh):
    cache_spec = P('dp', 'sp', None)
    in_specs = (P('dp', None), P(None), P(None), P(None, None), P(None, None), P(None, 'sp'), P('sp', None), cache_spec, cache_spec, P('dp'))
    out_specs = (P('dp', None), cache_spec, cache_spec)
    return jax.shard_map(device_step, mesh=mesh, in_specs=in_specs, out_specs=out_specs, check_vma=False)
```

```python
import functools

import jax
import jax.numpy as jnp
from jax import lax
from jax.experimental import pallas as pl
from jax.experimental.pallas import tpu as pltpu
from jax.sharding import PartitionSpec as P

LN_EPS = 1e-5
ROPE_BASE = 10000.0
NEG_FILL = -1e30
SCALE2 = 128 ** -0.5 * 1.4426950408889634
MESH = pl.DeviceIdType.MESH
VMEM_LIMIT = 67_000_000

ROWS = 128
D = 6144
HD = 128
NH = 48
SEQ = 512
FF = 3072
F32 = jnp.float32
BF16 = jnp.bfloat16


def rotary_tables(positions):
    inv_freq = 1.0 / (ROPE_BASE ** (jnp.arange(0, HD, 2, dtype=F32) / HD))
    angles = positions.astype(F32)[:, None] * inv_freq[None, :]
    cos_half = jnp.cos(angles)
    sin_half = jnp.sin(angles)
    return jnp.concatenate([cos_half, cos_half], axis=-1), jnp.concatenate([-sin_half, sin_half], axis=-1)


def place():
    sp = lax.axis_index('sp')
    core = lax.rem(sp, 2)
    x = lax.rem(sp // 2, 2)
    y = sp // 4
    return y, x, core


def device(y, x, core):
    return {'sp': (y * 2 + x) * 2 + core}


def enter(peers):
    barrier = pltpu.get_barrier_semaphore()
    for peer in peers:
        pl.semaphore_signal(barrier, inc=1, device_id=peer, device_id_type=MESH)
    pl.semaphore_wait(barrier, len(peers))


Q_STEPS = 12
Q_SLOTS = 6
Q_HALF = NH // 2


def qkv_kernel(hid, gam, bet, cos, sin, w, qkv, normed, wbuf, wkv, mine, wsem, kvsem, lsem, ssem, rsem):
    y, x, core = place()
    partner = device(y, x, 1 - core)

    def fetch(j):
        col = pl.multiple_of(core * (Q_HALF * HD) + j * 256, 256)
        slot = lax.rem(j, Q_SLOTS)
        return pltpu.make_async_copy(w.at[:, pl.ds(col, 256)], wbuf.at[slot], wsem.at[slot])

    kv_copy = pltpu.make_async_copy(w.at[:, pl.ds(pl.multiple_of((NH + core) * HD, HD), HD)], wkv, kvsem)
    kv_copy.start()
    for j in range(Q_SLOTS):
        fetch(j).start()
    enter([partner])

    def norm_rows(i, carry):
        rows = pl.ds(pl.multiple_of(i * 16, 16), 16)
        v = hid[rows, :].astype(F32)
        mean = jnp.sum(v, axis=-1, keepdims=True) * (1.0 / D)
        cen = v - mean
        var = jnp.sum(cen * cen, axis=-1, keepdims=True) * (1.0 / D)
        normed[rows, :] = (cen * lax.rsqrt(var + LN_EPS) * gam[...] + bet[...]).astype(BF16)
        return carry

    lax.fori_loop(0, ROWS // 16, norm_rows, 0)

    def remote(src, dst, count, sem):
        return pltpu.make_async_remote_copy(
            src_ref=mine.at[pl.ds(src, count)], dst_ref=qkv.at[pl.ds(dst, count)],
            send_sem=ssem.at[sem], recv_sem=rsem.at[sem], device_id=partner, device_id_type=MESH)

    def local(src, dst, count, sem):
        return pltpu.make_async_copy(mine.at[pl.ds(src, count)], qkv.at[pl.ds(dst, count)], lsem.at[sem])

    def pair(j):
        return 2 * j, core * Q_HALF + 2 * j, 2, j

    kv = (Q_HALF, NH + core, 1, Q_STEPS)

    def rotate(v):
        return (v * cos[...] + pltpu.roll(v, 64, 1) * sin[...]).astype(BF16).astype(F32)

    kv_copy.wait()
    v = jnp.dot(normed[...], wkv[...], preferred_element_type=F32).astype(BF16).astype(F32)
    mine[Q_HALF] = jnp.where(core == 0, rotate(v), v)
    remote(*kv).start()
    local(*kv).start()

    def block(j, carry):
        fetch(j).wait()
        acc = jnp.dot(normed[...], wbuf[lax.rem(j, Q_SLOTS)], preferred_element_type=F32)

        @pl.when(j + Q_SLOTS < Q_STEPS)
        def _():
            fetch(j + Q_SLOTS).start()

        for h in range(2):
            mine[2 * j + h] = rotate(acc[:, h * HD:(h + 1) * HD].astype(BF16).astype(F32))
        remote(*pair(j)).start()
        local(*pair(j)).start()
        return carry

    lax.fori_loop(0, Q_STEPS, block, 0)

    def drain(j, carry):
        local(*pair(j)).wait()
        remote(*pair(j)).wait()
        return carry

    lax.fori_loop(0, Q_STEPS, drain, 0)
    local(*kv).wait()
    remote(*kv).wait()


def qkv_call(hidden, gam, bet, cos, sin, w_qkv):
    vm = pl.BlockSpec(memory_space=pltpu.VMEM)
    anyspace = pl.BlockSpec(memory_space=pl.ANY)
    dma = pltpu.SemaphoreType.DMA
    return pl.pallas_call(
        qkv_kernel,
        out_shape=(jax.ShapeDtypeStruct((NH + 2, ROWS, HD), F32), jax.ShapeDtypeStruct((ROWS, D), BF16)),
        in_specs=[vm, vm, vm, vm, vm, anyspace],
        out_specs=(anyspace, vm),
        scratch_shapes=[
            pltpu.VMEM((Q_SLOTS, D, 256), BF16),
            pltpu.VMEM((D, HD), BF16),
            pltpu.VMEM((Q_HALF + 1, ROWS, HD), F32),
            dma((Q_SLOTS,)), dma, dma((Q_STEPS + 1,)), dma((Q_STEPS + 1,)), dma((Q_STEPS + 1,)),
        ],
        compiler_params=pltpu.CompilerParams(collective_id=0, has_side_effects=True, vmem_limit_bytes=VMEM_LIMIT),
        cost_estimate=pl.CostEstimate(flops=2 * ROWS * D * 3200, bytes_accessed=D * 6400, transcendentals=0),
        name='qkv',
    )(hidden, gam, bet, cos, sin, w_qkv)


A_ROWS = 8
A_STEPS = ROWS // A_ROWS
A_SLOTS = 8
A_AHEAD = 4


def attn_kernel(lp_ref, qkv, kc, vc, o, ml, kn, vn, kbuf, vbuf, sbuf, ebuf, isem, osem):
    i = pl.program_id(0)

    def fetch(step):
        slot = lax.rem(step, A_SLOTS)
        rows = pl.ds(step * A_ROWS, A_ROWS)
        return (pltpu.make_async_copy(kc.at[rows], kbuf.at[slot], isem.at[0, slot]),
                pltpu.make_async_copy(vc.at[rows], vbuf.at[slot], isem.at[1, slot]))

    def flush(step):
        slot = lax.rem(step, A_SLOTS)
        rows = pl.ds(step * A_ROWS, A_ROWS)
        return (pltpu.make_async_copy(kbuf.at[slot], kn.at[rows], osem.at[0, slot]),
                pltpu.make_async_copy(vbuf.at[slot], vn.at[rows], osem.at[1, slot]))

    @pl.when(i == 0)
    def _():
        for s in range(A_AHEAD):
            for c in fetch(s):
                c.start()

    @pl.when(i >= A_AHEAD)
    def _():
        for c in flush(i - A_AHEAD):
            c.wait()

    @pl.when(i + A_AHEAD < A_STEPS)
    def _():
        for c in fetch(i + A_AHEAD):
            c.start()

    for c in fetch(i):
        c.wait()
    slot = lax.rem(i, A_SLOTS)

    for r in range(A_ROWS):
        lp = lp_ref[i * A_ROWS + r]
        base = pl.multiple_of((jnp.clip(lp, 0, SEQ - 1) // 16) * 16, 16)
        hit = base + lax.broadcasted_iota(jnp.int32, (16, HD), 0) == lp
        for buf, src in ((kbuf, NH), (vbuf, NH + 1)):
            new = jnp.broadcast_to(qkv[src, r:r + 1, :], (16, HD))
            old = buf[slot, r, pl.ds(base, 16), :].astype(F32)
            buf[slot, r, pl.ds(base, 16), :] = jnp.where(hit, new, old).astype(BF16)

    for r in range(A_ROWS):
        q = qkv[0:NH, r, :].astype(BF16)
        sbuf[r] = lax.dot_general(q, kbuf[slot, r], (((1,), (1,)), ((), ())), preferred_element_type=F32)
    lane = lax.broadcasted_iota(jnp.int32, (NH, HD), 1)
    mcol = jnp.zeros((NH, HD), F32)
    lcol = jnp.zeros((NH, HD), F32)
    for r in range(A_ROWS):
        valid = lax.broadcasted_iota(jnp.int32, (NH, SEQ), 1) <= lp_ref[i * A_ROWS + r]
        s = jnp.where(valid, sbuf[r], -jnp.inf)
        m = jnp.max(s, axis=-1, keepdims=True)
        m = jnp.where(m == -jnp.inf, NEG_FILL, m)
        e = jnp.exp2((s - m) * SCALE2)
        l = jnp.sum(e, axis=-1, keepdims=True)
        ebuf[r] = e.astype(BF16)
        mcol = jnp.where(lane == r, m * SCALE2, mcol)
        lcol = jnp.where(lane == r, l, lcol)
    for r in range(A_ROWS):
        o[:, r, :] = jnp.dot(ebuf[r], vbuf[slot, r], preferred_element_type=F32)
    pad = jnp.zeros((16, HD), F32)
    ml[...] = jnp.transpose(jnp.concatenate([mcol, pad, lcol, pad], axis=0))[:A_ROWS]

    for c in flush(i):
        c.start()

    @pl.when(i == A_STEPS - 1)
    def _():
        for step in range(A_STEPS - A_AHEAD, A_STEPS):
            for c in flush(step):
                c.wait()


def attn_call(local_pos, qkv, k_cache, v_cache):
    anyspace = pl.BlockSpec(memory_space=pl.ANY)
    cache = jax.ShapeDtypeStruct((ROWS, SEQ, HD), BF16)
    return pl.pallas_call(
        attn_kernel,
        out_shape=(jax.ShapeDtypeStruct((NH, ROWS, HD), F32), jax.ShapeDtypeStruct((ROWS, HD), F32), cache, cache),
        grid_spec=pltpu.PrefetchScalarGridSpec(
            num_scalar_prefetch=1,
            grid=(A_STEPS,),
            in_specs=[pl.BlockSpec((NH + 2, A_ROWS, HD), lambda i, p: (0, i, 0)), anyspace, anyspace],
            out_specs=(pl.BlockSpec((NH, A_ROWS, HD), lambda i, p: (0, i, 0)), pl.BlockSpec((A_ROWS, HD), lambda i, p: (i, 0)),
                       anyspace, anyspace),
            scratch_shapes=[
                pltpu.VMEM((A_SLOTS, A_ROWS, SEQ, HD), BF16),
                pltpu.VMEM((A_SLOTS, A_ROWS, SEQ, HD), BF16),
                pltpu.VMEM((A_ROWS, NH, SEQ), F32),
                pltpu.VMEM((A_ROWS, NH, SEQ), BF16),
                pltpu.SemaphoreType.DMA((2, A_SLOTS)),
                pltpu.SemaphoreType.DMA((2, A_SLOTS)),
            ]),
        compiler_params=pltpu.CompilerParams(vmem_limit_bytes=VMEM_LIMIT, dimension_semantics=('arbitrary',)),
        cost_estimate=pl.CostEstimate(flops=4 * ROWS * NH * SEQ * HD, bytes_accessed=8 * ROWS * SEQ * HD, transcendentals=0),
        name='attn',
    )(local_pos, qkv, k_cache, v_cache)


W_SLOTS = 8
UP_STEPS = 12
DOWN_STEPS = 12
NR = 2
RT = NH // NR
NK = 3
CT = NH // NK
DOWN_PER = DOWN_STEPS // NK
OWN = NH // 8
LEVELS = 3


def tail_kernel(normed_hbm, hid_hbm, ml_in, o_hbm, w_up, w_down, w_out, out,
                normed, hid, wbuf, wobuf, act, part, mine, orecv0, orecv1, orecv2, stats, mlr, wts,
                precv0, precv1, precv2, gath, ctx, outbuf,
                insem, wsem, wosem, mysem, osend, orecv, msend, mrecv, psend, precv, gsend, grecv, outsem):
    y, x, core = place()
    first = 1 - core
    partner = device(y, x, 1 - core)
    x_peer = device(y, 1 - x, core)['sp']
    y_peer = device(1 - y, x, core)['sp']
    n1 = {'sp': x_peer * first + y_peer * core}
    n2 = {'sp': y_peer * first + x_peer * core}
    a = x * first + y * core
    b = y * first + x * core
    peers = (partner, n1, n2)

    def own(tiles, level):
        start = core * (tiles // 2)
        if level >= 1:
            start += a * (tiles // 4)
        if level >= 2:
            start += b * (tiles // 8)
        return start

    def other(tiles, level):
        start = 0 if level == 0 else own(tiles, level - 1)
        return start + (1 - (core, a, b)[level]) * (tiles // (2, 4, 8)[level])

    def remote(src, dst, send, recv, peer):
        return pltpu.make_async_remote_copy(src_ref=src, dst_ref=dst, send_sem=send, recv_sem=recv,
                                            device_id=peer, device_id_type=MESH)

    def fetch_up(step):
        slot = lax.rem(step, W_SLOTS)
        col = pl.multiple_of((step // 2) * 512, 512)
        row = pl.multiple_of(lax.rem(step, 2) * 3072, 3072)
        return pltpu.make_async_copy(w_up.at[pl.ds(row, 3072), pl.ds(col, 512)], wbuf.at[slot], wsem.at[slot])

    def fetch_down(step):
        slot = lax.rem(step + UP_STEPS, W_SLOTS)
        col = pl.multiple_of(step * 512, 512)
        return pltpu.make_async_copy(w_down.at[:, pl.ds(col, 512)], wbuf.at[slot], wsem.at[slot])

    normed_copy = pltpu.make_async_copy(normed_hbm, normed, insem.at[0])
    hid_copy = pltpu.make_async_copy(hid_hbm, hid, insem.at[1])

    def my_copy(k):
        return pltpu.make_async_copy(o_hbm.at[pl.ds(k * RT + own(RT, 0), RT // 2)], mine.at[k], mysem.at[k])

    def wo_copy(k):
        rows = pl.ds(pl.multiple_of((k * RT + own(RT, 2)) * HD, HD), RT // 8 * HD)
        return pltpu.make_async_copy(w_out.at[rows], wobuf.at[pl.ds(k * (RT // 8 * HD), RT // 8 * HD)], wosem.at[k])

    def out_copy(k):
        cols = pl.ds(k * CT * HD, CT * HD)
        return pltpu.make_async_copy(outbuf.at[:, cols], out.at[:, cols], outsem.at[k])

    o_to = (orecv0, orecv1, orecv2)

    def o_send(level, k):
        if level == 0:
            src = o_hbm.at[pl.ds(k * RT + other(RT, 0), RT // 2)]
        else:
            src = mine.at[k, pl.ds(other(RT, level) - own(RT, 0), RT // (2, 4, 8)[level])]
        return remote(src, o_to[level].at[k], osend.at[level, k], orecv.at[level, k], peers[level])

    def m_send(level):
        src = ml_in if level == 0 else stats.at[level - 1]
        return remote(src, mlr.at[level], msend.at[level], mrecv.at[level], peers[level])

    lanes = lax.broadcasted_iota(jnp.int32, (ROWS, HD), 1)

    def merge_stats(level):
        m_send(level).wait()
        ours = ml_in[...] if level == 0 else stats[level - 1]
        theirs = mlr[level]
        top = jnp.maximum(ours, theirs)
        w1 = jnp.exp2(ours - top)
        w2 = jnp.exp2(theirs - top)
        total = ours * pltpu.roll(w1, 64, 1) + theirs * pltpu.roll(w2, 64, 1)
        wts[level, 0] = w1
        wts[level, 1] = w2
        stats[level] = jnp.where(lanes < 64, top, total)

    def shift(v, by):
        return pltpu.roll(v, lax.rem(HD - by, HD), 1)

    def merge_heads(level, k):
        if level == 0:
            my_copy(k).wait()
        o_send(level, k).wait()
        first_head = k * RT + own(RT, level)
        w1 = shift(wts[level, 0], first_head)
        w2 = shift(wts[level, 1], first_head)
        base = own(RT, level) - own(RT, 0)
        for h in range(RT // (2, 4, 8)[level]):
            mine[k, base + h] = mine[k, base + h] * w1[:, h:h + 1] + o_to[level][k, h] * w2[:, h:h + 1]
        if level < 2:
            if k == 0:
                m_send(level + 1).start()
            o_send(level + 1, k).start()
        else:
            l = shift(stats[2], first_head)
            for h in range(RT // 8):
                col = (k * (RT // 8) + h) * HD
                ctx[:, col:col + HD] = (mine[k, base + h] / l[:, 64 + h:65 + h]).astype(BF16)

    def up_block(n, carry):
        fetch_up(2 * n).wait()
        s0 = lax.rem(2 * n, W_SLOTS)
        acc = jnp.dot(normed[:, :3072], wbuf[s0], preferred_element_type=F32)
        fetch_up(2 * n + 1).wait()
        acc += jnp.dot(normed[:, 3072:], wbuf[s0 + 1], preferred_element_type=F32)
        for half in range(2):
            nxt = 2 * n + half + W_SLOTS

            @pl.when(nxt < UP_STEPS)
            def _():
                fetch_up(nxt).start()

            @pl.when(nxt >= UP_STEPS)
            def _():
                fetch_down(nxt - UP_STEPS).start()

        act[:, pl.ds(pl.multiple_of(n * 512, 512), 512)] = (
            0.5 * acc * (1.0 + lax.erf(acc * (2.0 ** -0.5)))).astype(BF16)
        return carry

    def down_block(n, carry):
        fetch_down(n).wait()
        acc = jnp.dot(act[...], wbuf[lax.rem(n + UP_STEPS, W_SLOTS)], preferred_element_type=F32)

        @pl.when(n + W_SLOTS < DOWN_STEPS)
        def _():
            fetch_down(n + W_SLOTS).start()

        for t in range(4):
            part[n * 4 + t] = acc[:, t * HD:(t + 1) * HD]
        return carry

    def up(lo, hi):
        lax.fori_loop(lo, hi, up_block, 0)

    def down(lo, hi):
        lax.fori_loop(lo, hi, down_block, 0)

    p_to = (precv0, precv1, precv2)

    def p_send(level, k):
        src = part.at[pl.ds(k * CT + other(CT, level), CT // (2, 4, 8)[level])]
        return remote(src, p_to[level].at[k], psend.at[level, k], precv.at[level, k], peers[level])

    def g_send(level, k):
        where = gath.at[pl.ds(k * CT + own(CT, level), CT // (2, 4, 8)[level])]
        return remote(where, where, gsend.at[level, k], grecv.at[level, k], peers[level])

    def project(k):
        def tiles(n, carry):
            t0 = k * CT + n * 4
            acc = jnp.dot(ctx[...], wobuf[:, pl.ds(pl.multiple_of(t0 * HD, 512), 512)], preferred_element_type=F32)
            for t in range(4):
                part[t0 + t] += acc[:, t * HD:(t + 1) * HD]
            return carry

        lax.fori_loop(0, CT // 4, tiles, 0)
        p_send(0, k).start()

    def reduce(level, k):
        p_send(level, k).wait()
        base, count = k * CT + own(CT, level), CT // (2, 4, 8)[level]
        if level < 2:
            part[pl.ds(base, count)] = part[pl.ds(base, count)] + p_to[level][k]
            p_send(level + 1, k).start()
        else:
            for t in range(count):
                col = pl.multiple_of((base + t) * HD, HD)
                total = hid[:, pl.ds(col, HD)].astype(F32) + (part[base + t] + p_to[2][k, t])
                gath[base + t] = total.astype(BF16).astype(F32)
            g_send(2, k).start()

    def gather(level, k):
        g_send(level, k).wait()
        if level > 0:
            g_send(level - 1, k).start()
        else:
            for t in range(CT):
                col = (k * CT + t) * HD
                outbuf[:, col:col + HD] = gath[k * CT + t].astype(BF16)
            out_copy(k).start()

    normed_copy.start()
    for k in range(NR):
        my_copy(k).start()
    enter(peers)
    m_send(0).start()
    for k in range(NR):
        o_send(0, k).start()
    for s in range(W_SLOTS):
        fetch_up(s).start()
    normed_copy.wait()

    up(0, 1)
    merge_stats(0)
    merge_heads(0, 0)
    merge_heads(0, 1)
    up(1, 4)
    merge_stats(1)
    merge_heads(1, 0)
    for k in range(NR):
        wo_copy(k).start()
    hid_copy.start()
    up(4, 6)
    down(0, 1)
    merge_heads(1, 1)
    down(1, 4)
    merge_stats(2)
    merge_heads(2, 0)
    down(4, 6)
    merge_heads(2, 1)
    for k in range(NR):
        wo_copy(k).wait()
    hid_copy.wait()
    project(0)
    down(6, 8)
    project(1)
    reduce(0, 0)
    down(8, 12)
    project(2)
    reduce(0, 1)
    reduce(0, 2)
    for wave in range(1, NK + 5):
        for k in range(NK):
            s = wave - k
            if 1 <= s <= 2:
                reduce(s, k)
            elif 3 <= s <= 5:
                gather(5 - s, k)
    for k in range(NK):
        out_copy(k).wait()


def tail_call(normed, hidden, ml, o, w_up, w_down, w_out):
    vm = pl.BlockSpec(memory_space=pltpu.VMEM)
    anyspace = pl.BlockSpec(memory_space=pl.ANY)
    dma = pltpu.SemaphoreType.DMA
    return pl.pallas_call(
        tail_kernel,
        out_shape=jax.ShapeDtypeStruct((ROWS, D), BF16),
        in_specs=[anyspace, anyspace, vm, anyspace, anyspace, anyspace, anyspace],
        out_specs=anyspace,
        scratch_shapes=[
            pltpu.VMEM((ROWS, D), BF16),
            pltpu.VMEM((ROWS, D), BF16),
            pltpu.VMEM((W_SLOTS, 3072, 512), BF16),
            pltpu.VMEM((OWN * HD, D), BF16),
            pltpu.VMEM((ROWS, FF), BF16),
            pltpu.VMEM((NH, ROWS, HD), F32),
            pltpu.VMEM((NR, RT // 2, ROWS, HD), F32),
            pltpu.VMEM((NR, RT // 2, ROWS, HD), F32),
            pltpu.VMEM((NR, RT // 4, ROWS, HD), F32),
            pltpu.VMEM((NR, RT // 8, ROWS, HD), F32),
            pltpu.VMEM((LEVELS, ROWS, HD), F32),
            pltpu.VMEM((LEVELS, ROWS, HD), F32),
            pltpu.VMEM((LEVELS, 2, ROWS, HD), F32),
            pltpu.VMEM((NK, CT // 2, ROWS, HD), F32),
            pltpu.VMEM((NK, CT // 4, ROWS, HD), F32),
            pltpu.VMEM((NK, CT // 8, ROWS, HD), F32),
            pltpu.VMEM((NH, ROWS, HD), F32),
            pltpu.VMEM((ROWS, OWN * HD), BF16),
            pltpu.VMEM((ROWS, D), BF16),
            dma((2,)), dma((W_SLOTS,)), dma((NR,)), dma((NR,)),
            dma((LEVELS, NR)), dma((LEVELS, NR)), dma((LEVELS,)), dma((LEVELS,)),
            dma((LEVELS, NK)), dma((LEVELS, NK)), dma((LEVELS, NK)), dma((LEVELS, NK)), dma((NK,)),
        ],
        compiler_params=pltpu.CompilerParams(collective_id=1, has_side_effects=True, vmem_limit_bytes=VMEM_LIMIT),
        cost_estimate=pl.CostEstimate(flops=4 * ROWS * D * FF, bytes_accessed=4 * D * FF, transcendentals=0),
        name='tail',
    )(normed, hidden, ml, o, w_up, w_down, w_out)


def device_step(hidden, ln_gamma, ln_beta, w_qkv, w_out, w_up, w_down, k_cache, v_cache, positions):
    cos, sin = rotary_tables(positions)
    local_pos = positions - lax.axis_index('sp') * SEQ
    qkv, normed = qkv_call(hidden, ln_gamma[None, :], ln_beta[None, :], cos, sin, w_qkv)
    o, ml, k_next, v_next = attn_call(local_pos, qkv, k_cache, v_cache)
    out = tail_call(normed, hidden, ml, o, w_up, w_down, w_out)
    return out, k_next, v_next


def solution(mesh):
    cache_spec = P('dp', 'sp', None)
    in_specs = (P('dp', None), P(None), P(None), P(None, None), P(None, None), P(None, 'sp'), P('sp', None), cache_spec, cache_spec, P('dp'))
    out_specs = (P('dp', None), cache_spec, cache_spec)
    return jax.shard_map(device_step, mesh=mesh, in_specs=in_specs, out_specs=out_specs, check_vma=False)
```

```python
import functools

import jax
import jax.numpy as jnp
from jax import lax
from jax.experimental import pallas as pl
from jax.experimental.pallas import tpu as pltpu
from jax.sharding import PartitionSpec as P

LN_EPS = 1e-5
ROPE_BASE = 10000.0
NEG_FILL = -1e30
SCALE2 = 128 ** -0.5 * 1.4426950408889634
MESH = pl.DeviceIdType.MESH
FRONT_LIMIT = 46_000_000
ATTN_LIMIT = 40_000_000
TAIL_LIMIT = 48_500_000

ROWS = 128
D = 6144
HD = 128
NH = 48
SEQ = 512
FF = 3072
F32 = jnp.float32
BF16 = jnp.bfloat16


def device(y, x, core):
    return {'sp': (y * 2 + x) * 2 + core}


class Place:
    def __init__(self):
        sp = lax.axis_index('sp')
        core = lax.rem(sp, 2)
        x = lax.rem(sp // 2, 2)
        y = sp // 4
        first = 1 - core
        x_peer = device(y, 1 - x, core)['sp']
        y_peer = device(1 - y, x, core)['sp']
        self.sides = (core, x * first + y * core, y * first + x * core)
        self.peers = (device(y, x, first), {'sp': x_peer * first + y_peer * core}, {'sp': y_peer * first + x_peer * core})

    def own(self, tiles, level):
        return sum(self.sides[n] * (tiles // (2, 4, 8)[n]) for n in range(level + 1))

    def other(self, tiles, level):
        start = self.own(tiles, level - 1) if level else 0
        return start + (1 - self.sides[level]) * (tiles // (2, 4, 8)[level])

    def remote(self, level, src, dst, send, recv):
        return pltpu.make_async_remote_copy(src_ref=src, dst_ref=dst, send_sem=send, recv_sem=recv,
                                            device_id=self.peers[level], device_id_type=MESH)

    def enter(self):
        barrier = pltpu.get_barrier_semaphore()
        for peer in self.peers:
            pl.semaphore_signal(barrier, inc=1, device_id=peer, device_id_type=MESH)
        pl.semaphore_wait(barrier, len(self.peers))


PART = (2, 4, 8)
LEVELS = 3


NQ = 3
QT = NH // NQ
U_SLOTS = 6
UP_STEPS = 12


def front_kernel(hid, gam, bet, pos, freq, w, w_up, qkv, act, normed, qbuf, wbuf, cos, sin, qsem, wsem, gsend, grecv):
    here = Place()

    def fetch_q(k):
        col = k * QT + here.own(QT, 2) if k < NQ else NH
        return pltpu.make_async_copy(w.at[:, pl.ds(pl.multiple_of(col * HD, 256), 256)], qbuf.at[k], qsem.at[k])

    def fetch_up(step):
        slot = lax.rem(step, U_SLOTS)
        col = pl.multiple_of((step // 2) * 512, 512)
        row = pl.multiple_of(lax.rem(step, 2) * 3072, 3072)
        return pltpu.make_async_copy(w_up.at[pl.ds(row, 3072), pl.ds(col, 512)], wbuf.at[slot], wsem.at[slot])

    for k in range(NQ + 1):
        fetch_q(k).start()
    for step in range(U_SLOTS):
        fetch_up(step).start()
    here.enter()

    def norm_rows(i, carry):
        rows = pl.ds(pl.multiple_of(i * 16, 16), 16)
        v = hid[rows, :].astype(F32)
        mean = jnp.sum(v, axis=-1, keepdims=True) * (1.0 / D)
        cen = v - mean
        var = jnp.sum(cen * cen, axis=-1, keepdims=True) * (1.0 / D)
        normed[rows, :] = (cen * lax.rsqrt(var + LN_EPS) * gam[...] + bet[...]).astype(BF16)
        return carry

    lax.fori_loop(0, ROWS // 16, norm_rows, 0)

    angle = jnp.transpose(jnp.broadcast_to(pos[...].astype(F32), (ROWS, HD))) * freq[...]
    cos[...] = jnp.cos(angle)
    lanes = lax.broadcasted_iota(jnp.int32, (ROWS, HD), 1)
    sine = jnp.sin(angle)
    sin[...] = jnp.where(lanes < HD // 2, -sine, sine)

    def rotate(v):
        return (v * cos[...] + pltpu.roll(v, HD // 2, 1) * sin[...]).astype(BF16).astype(F32)

    def g_send(level, k):
        where = qkv.at[pl.ds(k * QT + here.own(QT, level), QT // PART[level])]
        return here.remote(level, where, where, gsend.at[level, k], grecv.at[level, k])

    def project(k):
        fetch_q(k).wait()
        acc = jnp.dot(normed[...], qbuf[k], preferred_element_type=F32)
        return [acc[:, h * HD:(h + 1) * HD].astype(BF16).astype(F32) for h in range(2)]

    def query(k):
        for h, v in enumerate(project(k)):
            qkv[k * QT + here.own(QT, 2) + h] = rotate(v)
        g_send(2, k).start()

    def gather(level, k):
        g_send(level, k).wait()
        if level:
            g_send(level - 1, k).start()

    def up_block(n, carry):
        fetch_up(2 * n).wait()
        s0 = lax.rem(2 * n, U_SLOTS)
        acc = jnp.dot(normed[:, :3072], wbuf[s0], preferred_element_type=F32)
        fetch_up(2 * n + 1).wait()
        acc += jnp.dot(normed[:, 3072:], wbuf[s0 + 1], preferred_element_type=F32)
        for half in range(2):
            nxt = 2 * n + half + U_SLOTS

            @pl.when(nxt < UP_STEPS)
            def _():
                fetch_up(nxt).start()

        act[:, pl.ds(pl.multiple_of(n * 512, 512), 512)] = (
            0.5 * acc * (1.0 + lax.erf(acc * (2.0 ** -0.5)))).astype(BF16)
        return carry

    def up(lo, hi):
        lax.fori_loop(lo, hi, up_block, 0)

    query(0)
    query(1)
    query(2)
    k_new, v_new = project(NQ)
    qkv[NH] = rotate(k_new)
    qkv[NH + 1] = v_new
    gather(2, 0)
    up(0, 1)
    gather(2, 1)
    gather(2, 2)
    up(1, 2)
    gather(1, 0)
    up(2, 4)
    gather(1, 1)
    up(4, 6)
    gather(1, 2)
    for k in range(NQ):
        gather(0, k)


def front_call(hidden, gam, bet, pos, freq, w_qkv, w_up):
    vm = pl.BlockSpec(memory_space=pltpu.VMEM)
    anyspace = pl.BlockSpec(memory_space=pl.ANY)
    dma = pltpu.SemaphoreType.DMA
    return pl.pallas_call(
        front_kernel,
        out_shape=(jax.ShapeDtypeStruct((NH + 2, ROWS, HD), F32), jax.ShapeDtypeStruct((ROWS, FF), BF16)),
        in_specs=[vm, vm, vm, vm, vm, anyspace, anyspace],
        out_specs=(vm, vm),
        scratch_shapes=[
            pltpu.VMEM((ROWS, D), BF16),
            pltpu.VMEM((NQ + 1, D, 256), BF16),
            pltpu.VMEM((U_SLOTS, 3072, 512), BF16),
            pltpu.VMEM((ROWS, HD), F32),
            pltpu.VMEM((ROWS, HD), F32),
            dma((NQ + 1,)), dma((U_SLOTS,)), dma((LEVELS, NQ)), dma((LEVELS, NQ)),
        ],
        compiler_params=pltpu.CompilerParams(collective_id=0, has_side_effects=True, vmem_limit_bytes=FRONT_LIMIT),
        cost_estimate=pl.CostEstimate(flops=2 * ROWS * D * (FF + 1024), bytes_accessed=2 * D * (FF + 1024), transcendentals=0),
        name='front',
    )(hidden, gam, bet, pos, freq, w_qkv, w_up)


A_ROWS = 8
A_STEPS = ROWS // A_ROWS
A_SLOTS = 6
A_AHEAD = 3


def attn_kernel(pos_ref, qkv, kc, vc, o, ml, kn, vn, kbuf, vbuf, sbuf, ebuf, isem, osem):
    i = pl.program_id(0)
    origin = lax.axis_index('sp') * SEQ

    def fetch(step):
        slot = lax.rem(step, A_SLOTS)
        rows = pl.ds(step * A_ROWS, A_ROWS)
        return (pltpu.make_async_copy(kc.at[rows], kbuf.at[slot], isem.at[0, slot]),
                pltpu.make_async_copy(vc.at[rows], vbuf.at[slot], isem.at[1, slot]))

    def flush(step):
        slot = lax.rem(step, A_SLOTS)
        rows = pl.ds(step * A_ROWS, A_ROWS)
        return (pltpu.make_async_copy(kbuf.at[slot], kn.at[rows], osem.at[0, slot]),
                pltpu.make_async_copy(vbuf.at[slot], vn.at[rows], osem.at[1, slot]))

    @pl.when(i == 0)
    def _():
        for s in range(A_AHEAD):
            for c in fetch(s):
                c.start()

    @pl.when(i >= A_AHEAD)
    def _():
        for c in flush(i - A_AHEAD):
            c.wait()

    @pl.when(i + A_AHEAD < A_STEPS)
    def _():
        for c in fetch(i + A_AHEAD):
            c.start()

    for c in fetch(i):
        c.wait()
    slot = lax.rem(i, A_SLOTS)

    for r in range(A_ROWS):
        lp = pos_ref[i * A_ROWS + r] - origin
        base = pl.multiple_of((jnp.clip(lp, 0, SEQ - 1) // 16) * 16, 16)
        hit = base + lax.broadcasted_iota(jnp.int32, (16, HD), 0) == lp
        for buf, src in ((kbuf, NH), (vbuf, NH + 1)):
            new = jnp.broadcast_to(qkv[src, r:r + 1, :], (16, HD))
            old = buf[slot, r, pl.ds(base, 16), :].astype(F32)
            buf[slot, r, pl.ds(base, 16), :] = jnp.where(hit, new, old).astype(BF16)

    for r in range(A_ROWS):
        q = qkv[0:NH, r, :].astype(BF16)
        sbuf[r] = lax.dot_general(q, kbuf[slot, r], (((1,), (1,)), ((), ())), preferred_element_type=F32)
    lane = lax.broadcasted_iota(jnp.int32, (NH, HD), 1)
    mcol = jnp.zeros((NH, HD), F32)
    lcol = jnp.zeros((NH, HD), F32)
    for r in range(A_ROWS):
        valid = lax.broadcasted_iota(jnp.int32, (NH, SEQ), 1) <= pos_ref[i * A_ROWS + r] - origin
        s = jnp.where(valid, sbuf[r], -jnp.inf)
        m = jnp.max(s, axis=-1, keepdims=True)
        m = jnp.where(m == -jnp.inf, NEG_FILL, m)
        e = jnp.exp2((s - m) * SCALE2)
        l = jnp.sum(e, axis=-1, keepdims=True)
        ebuf[r] = e.astype(BF16)
        mcol = jnp.where(lane == r, m * SCALE2, mcol)
        lcol = jnp.where(lane == r, l, lcol)
    for r in range(A_ROWS):
        o[:, r, :] = jnp.dot(ebuf[r], vbuf[slot, r], preferred_element_type=F32)
    pad = jnp.zeros((16, HD), F32)
    ml[...] = jnp.transpose(jnp.concatenate([mcol, pad, lcol, pad], axis=0))[:A_ROWS]

    for c in flush(i):
        c.start()

    @pl.when(i == A_STEPS - 1)
    def _():
        for step in range(A_STEPS - A_AHEAD, A_STEPS):
            for c in flush(step):
                c.wait()


def attn_call(positions, qkv, k_cache, v_cache):
    anyspace = pl.BlockSpec(memory_space=pl.ANY)
    cache = jax.ShapeDtypeStruct((ROWS, SEQ, HD), BF16)
    return pl.pallas_call(
        attn_kernel,
        out_shape=(jax.ShapeDtypeStruct((NH, ROWS, HD), F32), jax.ShapeDtypeStruct((ROWS, HD), F32), cache, cache),
        grid_spec=pltpu.PrefetchScalarGridSpec(
            num_scalar_prefetch=1,
            grid=(A_STEPS,),
            in_specs=[pl.BlockSpec((NH + 2, A_ROWS, HD), lambda i, p: (0, i, 0)), anyspace, anyspace],
            out_specs=(pl.BlockSpec((NH, A_ROWS, HD), lambda i, p: (0, i, 0)), pl.BlockSpec((A_ROWS, HD), lambda i, p: (i, 0)),
                       anyspace, anyspace),
            scratch_shapes=[
                pltpu.VMEM((A_SLOTS, A_ROWS, SEQ, HD), BF16),
                pltpu.VMEM((A_SLOTS, A_ROWS, SEQ, HD), BF16),
                pltpu.VMEM((A_ROWS, NH, SEQ), F32),
                pltpu.VMEM((A_ROWS, NH, SEQ), BF16),
                pltpu.SemaphoreType.DMA((2, A_SLOTS)),
                pltpu.SemaphoreType.DMA((2, A_SLOTS)),
            ]),
        compiler_params=pltpu.CompilerParams(vmem_limit_bytes=ATTN_LIMIT, dimension_semantics=('arbitrary',)),
        cost_estimate=pl.CostEstimate(flops=4 * ROWS * NH * SEQ * HD, bytes_accessed=8 * ROWS * SEQ * HD, transcendentals=0),
        name='attn',
    )(positions, qkv, k_cache, v_cache)


W_SLOTS = 6
DOWN_STEPS = 12
NR = 3
RT = NH // NR
NK = 3
CT = NH // NK
OWN = NH // 8


def tail_kernel(act, ml_in, o_in, hid, w_down, w_out, out,
                wbuf, wobuf, part, mine, orecv0, orecv1, orecv2, stats, mlr, wts,
                precv0, precv1, precv2, gath, ctx,
                wsem, wosem, osend, orecv, msend, mrecv, psend, precv, gsend, grecv):
    here = Place()
    own, other = here.own, here.other

    def fetch_down(step):
        slot = lax.rem(step, W_SLOTS)
        col = pl.multiple_of(step * 512, 512)
        return pltpu.make_async_copy(w_down.at[:, pl.ds(col, 512)], wbuf.at[slot], wsem.at[slot])

    def wo_copy(k):
        rows = pl.ds(pl.multiple_of((k * RT + own(RT, 2)) * HD, HD), RT // 8 * HD)
        return pltpu.make_async_copy(w_out.at[rows], wobuf.at[pl.ds(k * (RT // 8 * HD), RT // 8 * HD)], wosem.at[k])

    o_to = (orecv0, orecv1, orecv2)

    def o_send(level, k):
        if level == 0:
            src = o_in.at[pl.ds(k * RT + other(RT, 0), RT // 2)]
        else:
            src = mine.at[k, pl.ds(other(RT, level) - own(RT, 0), RT // PART[level])]
        return here.remote(level, src, o_to[level].at[k], osend.at[level, k], orecv.at[level, k])

    def m_send(level):
        src = ml_in if level == 0 else stats.at[level - 1]
        return here.remote(level, src, mlr.at[level], msend.at[level], mrecv.at[level])

    lanes = lax.broadcasted_iota(jnp.int32, (ROWS, HD), 1)

    def merge_stats(level):
        m_send(level).wait()
        ours = ml_in[...] if level == 0 else stats[level - 1]
        theirs = mlr[level]
        top = jnp.maximum(ours, theirs)
        w1 = jnp.exp2(ours - top)
        w2 = jnp.exp2(theirs - top)
        total = ours * pltpu.roll(w1, 64, 1) + theirs * pltpu.roll(w2, 64, 1)
        wts[level, 0] = w1
        wts[level, 1] = w2
        stats[level] = jnp.where(lanes < 64, top, total)

    def shift(v, by):
        return pltpu.roll(v, lax.rem(HD - by, HD), 1)

    def merge_heads(level, k):
        o_send(level, k).wait()
        first_head = k * RT + own(RT, level)
        w1 = shift(wts[level, 0], first_head)
        w2 = shift(wts[level, 1], first_head)
        base = own(RT, level) - own(RT, 0)
        for h in range(RT // PART[level]):
            ours = o_in[first_head + h] if level == 0 else mine[k, base + h]
            mine[k, base + h] = ours * w1[:, h:h + 1] + o_to[level][k, h] * w2[:, h:h + 1]
        if level < 2:
            if k == 0:
                m_send(level + 1).start()
            o_send(level + 1, k).start()
        else:
            l = shift(stats[2], first_head)
            for h in range(RT // 8):
                col = (k * (RT // 8) + h) * HD
                ctx[:, col:col + HD] = (mine[k, base + h] / l[:, 64 + h:65 + h]).astype(BF16)

    def down_block(n, carry):
        fetch_down(n).wait()
        acc = jnp.dot(act[...], wbuf[lax.rem(n, W_SLOTS)], preferred_element_type=F32)

        @pl.when(n + W_SLOTS < DOWN_STEPS)
        def _():
            fetch_down(n + W_SLOTS).start()

        for t in range(4):
            part[n * 4 + t] = acc[:, t * HD:(t + 1) * HD]
        return carry

    def down(lo, hi):
        lax.fori_loop(lo, hi, down_block, 0)

    p_to = (precv0, precv1, precv2)

    def p_send(level, k):
        src = part.at[pl.ds(k * CT + other(CT, level), CT // PART[level])]
        return here.remote(level, src, p_to[level].at[k], psend.at[level, k], precv.at[level, k])

    def g_send(level, k):
        where = gath.at[pl.ds(k * CT + own(CT, level), CT // PART[level])]
        return here.remote(level, where, where, gsend.at[level, k], grecv.at[level, k])

    def project(k):
        def tiles(n, carry):
            t0 = k * CT + n * 4
            acc = jnp.dot(ctx[...], wobuf[:, pl.ds(pl.multiple_of(t0 * HD, 512), 512)], preferred_element_type=F32)
            for t in range(4):
                part[t0 + t] += acc[:, t * HD:(t + 1) * HD]
            return carry

        lax.fori_loop(0, CT // 4, tiles, 0)
        p_send(0, k).start()

    def reduce(level, k):
        p_send(level, k).wait()
        base, count = k * CT + own(CT, level), CT // PART[level]
        if level < 2:
            part[pl.ds(base, count)] = part[pl.ds(base, count)] + p_to[level][k]
            p_send(level + 1, k).start()
        else:
            for t in range(count):
                col = pl.multiple_of((base + t) * HD, HD)
                total = hid[:, pl.ds(col, HD)].astype(F32) + (part[base + t] + p_to[2][k, t])
                gath[base + t] = total.astype(BF16).astype(F32)
            g_send(2, k).start()

    def gather(level, k):
        g_send(level, k).wait()
        if level > 0:
            g_send(level - 1, k).start()
        else:
            for t in range(CT):
                col = (k * CT + t) * HD
                out[:, col:col + HD] = gath[k * CT + t].astype(BF16)

    here.enter()
    m_send(0).start()
    for k in range(NR):
        o_send(0, k).start()
    for s in range(W_SLOTS):
        fetch_down(s).start()
    for k in range(NR):
        wo_copy(k).start()

    merge_stats(0)
    for k in range(NR):
        merge_heads(0, k)
    down(0, 3)
    merge_stats(1)
    merge_heads(1, 0)
    down(3, 6)
    merge_heads(1, 1)
    down(6, 9)
    merge_stats(2)
    merge_heads(2, 0)
    merge_heads(1, 2)
    down(9, 12)
    merge_heads(2, 1)
    for k in range(NR):
        wo_copy(k).wait()
    merge_heads(2, 2)
    project(0)
    project(1)
    reduce(0, 0)
    project(2)
    reduce(0, 1)
    reduce(0, 2)
    for wave in range(1, NK + 5):
        for k in range(NK):
            s = wave - k
            if 1 <= s <= 2:
                reduce(s, k)
            elif 3 <= s <= 5:
                gather(5 - s, k)


def tail_call(act, ml, o, hidden, w_down, w_out):
    vm = pl.BlockSpec(memory_space=pltpu.VMEM)
    anyspace = pl.BlockSpec(memory_space=pl.ANY)
    dma = pltpu.SemaphoreType.DMA
    return pl.pallas_call(
        tail_kernel,
        out_shape=jax.ShapeDtypeStruct((ROWS, D), BF16),
        in_specs=[vm, vm, vm, vm, anyspace, anyspace],
        out_specs=vm,
        scratch_shapes=[
            pltpu.VMEM((W_SLOTS, 3072, 512), BF16),
            pltpu.VMEM((OWN * HD, D), BF16),
            pltpu.VMEM((NH, ROWS, HD), F32),
            pltpu.VMEM((NR, RT // 2, ROWS, HD), F32),
            pltpu.VMEM((NR, RT // 2, ROWS, HD), F32),
            pltpu.VMEM((NR, RT // 4, ROWS, HD), F32),
            pltpu.VMEM((NR, RT // 8, ROWS, HD), F32),
            pltpu.VMEM((LEVELS, ROWS, HD), F32),
            pltpu.VMEM((LEVELS, ROWS, HD), F32),
            pltpu.VMEM((LEVELS, 2, ROWS, HD), F32),
            pltpu.VMEM((NK, CT // 2, ROWS, HD), F32),
            pltpu.VMEM((NK, CT // 4, ROWS, HD), F32),
            pltpu.VMEM((NK, CT // 8, ROWS, HD), F32),
            pltpu.VMEM((NH, ROWS, HD), F32),
            pltpu.VMEM((ROWS, OWN * HD), BF16),
            dma((W_SLOTS,)), dma((NR,)),
            dma((LEVELS, NR)), dma((LEVELS, NR)), dma((LEVELS,)), dma((LEVELS,)),
            dma((LEVELS, NK)), dma((LEVELS, NK)), dma((LEVELS, NK)), dma((LEVELS, NK)),
        ],
        compiler_params=pltpu.CompilerParams(collective_id=1, has_side_effects=True, vmem_limit_bytes=TAIL_LIMIT),
        cost_estimate=pl.CostEstimate(flops=2 * ROWS * D * FF, bytes_accessed=2 * D * FF, transcendentals=0),
        name='tail',
    )(act, ml, o, hidden, w_down, w_out)


def device_step(hidden, ln_gamma, ln_beta, w_qkv, w_out, w_up, w_down, k_cache, v_cache, positions):
    inv_freq = 1.0 / (ROPE_BASE ** (jnp.arange(0, HD, 2, dtype=F32) / HD))
    freq = jnp.concatenate([inv_freq, inv_freq])[None, :]
    qkv, act = front_call(hidden, ln_gamma[None, :], ln_beta[None, :], positions[None, :], freq, w_qkv, w_up)
    o, ml, k_next, v_next = attn_call(positions, qkv, k_cache, v_cache)
    out = tail_call(act, ml, o, hidden, w_down, w_out)
    return out, k_next, v_next


def solution(mesh):
    cache_spec = P('dp', 'sp', None)
    in_specs = (P('dp', None), P(None), P(None), P(None, None), P(None, None), P(None, 'sp'), P('sp', None), cache_spec, cache_spec, P('dp'))
    out_specs = (P('dp', None), cache_spec, cache_spec)
    return jax.shard_map(device_step, mesh=mesh, in_specs=in_specs, out_specs=out_specs, check_vma=False)
```

```python
import functools

import jax
import jax.numpy as jnp
from jax import lax
from jax.experimental import pallas as pl
from jax.experimental.pallas import tpu as pltpu
from jax.sharding import PartitionSpec as P

LN_EPS = 1e-5
ROPE_BASE = 10000.0
NEG_FILL = -1e30
SCALE2 = 128 ** -0.5 * 1.4426950408889634
MESH = pl.DeviceIdType.MESH
FRONT_LIMIT = 46_000_000
ATTN_LIMIT = 40_000_000
TAIL_LIMIT = 48_500_000

ROWS = 128
D = 6144
HD = 128
NH = 48
SEQ = 512
FF = 3072
F32 = jnp.float32
BF16 = jnp.bfloat16


def device(y, x, core):
    return {'sp': (y * 2 + x) * 2 + core}


class Place:
    def __init__(self):
        sp = lax.axis_index('sp')
        core = lax.rem(sp, 2)
        x = lax.rem(sp // 2, 2)
        y = sp // 4
        first = 1 - core
        x_peer = device(y, 1 - x, core)['sp']
        y_peer = device(1 - y, x, core)['sp']
        self.sides = (core, x * first + y * core, y * first + x * core)
        self.peers = (device(y, x, first), {'sp': x_peer * first + y_peer * core}, {'sp': y_peer * first + x_peer * core})

    def own(self, tiles, level):
        return sum(self.sides[n] * (tiles // (2, 4, 8)[n]) for n in range(level + 1))

    def other(self, tiles, level):
        start = self.own(tiles, level - 1) if level else 0
        return start + (1 - self.sides[level]) * (tiles // (2, 4, 8)[level])

    def remote(self, level, src, dst, send, recv):
        return pltpu.make_async_remote_copy(src_ref=src, dst_ref=dst, send_sem=send, recv_sem=recv,
                                            device_id=self.peers[level], device_id_type=MESH)

    def enter(self):
        barrier = pltpu.get_barrier_semaphore()
        for peer in self.peers:
            pl.semaphore_signal(barrier, inc=1, device_id=peer, device_id_type=MESH)
        pl.semaphore_wait(barrier, len(self.peers))


PART = (2, 4, 8)
LEVELS = 3


NQ = 3
QT = NH // NQ
U_SLOTS = 6
UP_STEPS = 12


def front_kernel(hid_hbm, gam_hbm, bet_hbm, pos_hbm, freq, w, w_up, qkv, act,
                 hid, gam, bet, pos, normed, qbuf, wbuf, cos, sin, insem, qsem, wsem, gsend, grecv):
    here = Place()
    inputs = [pltpu.make_async_copy(src, dst, insem.at[n]) for n, (src, dst) in enumerate(
        ((hid_hbm, hid), (gam_hbm, gam), (bet_hbm, bet), (pos_hbm, pos)))]
    for copy in inputs:
        copy.start()

    def fetch_q(k):
        col = k * QT + here.own(QT, 2) if k < NQ else NH
        return pltpu.make_async_copy(w.at[:, pl.ds(pl.multiple_of(col * HD, 256), 256)], qbuf.at[k], qsem.at[k])

    def fetch_up(step):
        slot = lax.rem(step, U_SLOTS)
        col = pl.multiple_of((step // 2) * 512, 512)
        row = pl.multiple_of(lax.rem(step, 2) * 3072, 3072)
        return pltpu.make_async_copy(w_up.at[pl.ds(row, 3072), pl.ds(col, 512)], wbuf.at[slot], wsem.at[slot])

    for k in range(NQ + 1):
        fetch_q(k).start()
    here.enter()
    for copy in inputs:
        copy.wait()

    def norm_rows(i, carry):
        rows = pl.ds(pl.multiple_of(i * 16, 16), 16)
        v = hid[rows, :].astype(F32)
        mean = jnp.sum(v, axis=-1, keepdims=True) * (1.0 / D)
        cen = v - mean
        var = jnp.sum(cen * cen, axis=-1, keepdims=True) * (1.0 / D)
        normed[rows, :] = (cen * lax.rsqrt(var + LN_EPS) * gam[...] + bet[...]).astype(BF16)
        return carry

    lax.fori_loop(0, ROWS // 16, norm_rows, 0)
    for step in range(2):
        fetch_up(step).start()

    angle = jnp.transpose(jnp.broadcast_to(pos[...].astype(F32), (ROWS, HD))) * freq[...]
    cos[...] = jnp.cos(angle)
    lanes = lax.broadcasted_iota(jnp.int32, (ROWS, HD), 1)
    sine = jnp.sin(angle)
    sin[...] = jnp.where(lanes < HD // 2, -sine, sine)

    def rotate(v):
        return (v * cos[...] + pltpu.roll(v, HD // 2, 1) * sin[...]).astype(BF16).astype(F32)

    def g_send(level, k):
        where = qkv.at[pl.ds(k * QT + here.own(QT, level), QT // PART[level])]
        return here.remote(level, where, where, gsend.at[level, k], grecv.at[level, k])

    def project(k):
        fetch_q(k).wait()
        acc = jnp.dot(normed[...], qbuf[k], preferred_element_type=F32)
        return [acc[:, h * HD:(h + 1) * HD].astype(BF16).astype(F32) for h in range(2)]

    def query(k):
        for h, v in enumerate(project(k)):
            qkv[k * QT + here.own(QT, 2) + h] = rotate(v)
        g_send(2, k).start()

    def gather(level, k):
        g_send(level, k).wait()
        if level:
            g_send(level - 1, k).start()

    def up_block(n, carry):
        fetch_up(2 * n).wait()
        s0 = lax.rem(2 * n, U_SLOTS)
        acc = jnp.dot(normed[:, :3072], wbuf[s0], preferred_element_type=F32)
        fetch_up(2 * n + 1).wait()
        acc += jnp.dot(normed[:, 3072:], wbuf[s0 + 1], preferred_element_type=F32)
        for half in range(2):
            nxt = 2 * n + half + U_SLOTS

            @pl.when(nxt < UP_STEPS)
            def _():
                fetch_up(nxt).start()

        act[:, pl.ds(pl.multiple_of(n * 512, 512), 512)] = (
            0.5 * acc * (1.0 + lax.erf(acc * (2.0 ** -0.5)))).astype(BF16)
        return carry

    def up(lo, hi):
        lax.fori_loop(lo, hi, up_block, 0)

    query(0)
    for step in range(2, 4):
        fetch_up(step).start()
    query(1)
    query(2)
    for step in range(4, U_SLOTS):
        fetch_up(step).start()
    k_new, v_new = project(NQ)
    qkv[NH] = rotate(k_new)
    qkv[NH + 1] = v_new
    gather(2, 0)
    up(0, 1)
    gather(2, 1)
    gather(2, 2)
    up(1, 2)
    gather(1, 0)
    up(2, 4)
    gather(1, 1)
    up(4, 6)
    gather(1, 2)
    for k in range(NQ):
        gather(0, k)


def front_call(hidden, gam, bet, pos, freq, w_qkv, w_up):
    vm = pl.BlockSpec(memory_space=pltpu.VMEM)
    hbm = pl.BlockSpec(memory_space=pltpu.HBM)
    dma = pltpu.SemaphoreType.DMA
    return pl.pallas_call(
        front_kernel,
        out_shape=(jax.ShapeDtypeStruct((NH + 2, ROWS, HD), F32), jax.ShapeDtypeStruct((ROWS, FF), BF16)),
        in_specs=[hbm, hbm, hbm, hbm, vm, hbm, hbm],
        out_specs=(vm, vm),
        scratch_shapes=[
            pltpu.VMEM((ROWS, D), BF16),
            pltpu.VMEM((1, D), F32),
            pltpu.VMEM((1, D), F32),
            pltpu.VMEM((1, ROWS), jnp.int32),
            pltpu.VMEM((ROWS, D), BF16),
            pltpu.VMEM((NQ + 1, D, 256), BF16),
            pltpu.VMEM((U_SLOTS, 3072, 512), BF16),
            pltpu.VMEM((ROWS, HD), F32),
            pltpu.VMEM((ROWS, HD), F32),
            dma((4,)), dma((NQ + 1,)), dma((U_SLOTS,)), dma((LEVELS, NQ)), dma((LEVELS, NQ)),
        ],
        compiler_params=pltpu.CompilerParams(collective_id=0, has_side_effects=True, vmem_limit_bytes=FRONT_LIMIT),
        cost_estimate=pl.CostEstimate(flops=2 * ROWS * D * (FF + 1024), bytes_accessed=2 * D * (FF + 1024), transcendentals=0),
        name='front',
    )(hidden, gam, bet, pos, freq, w_qkv, w_up)


A_ROWS = 8
A_STEPS = ROWS // A_ROWS
A_SLOTS = 6
A_AHEAD = 3


def attn_kernel(pos_ref, qkv, kc, vc, o, ml, kn, vn, kbuf, vbuf, sbuf, ebuf, isem, osem):
    i = pl.program_id(0)
    origin = lax.axis_index('sp') * SEQ

    def fetch(step):
        slot = lax.rem(step, A_SLOTS)
        rows = pl.ds(step * A_ROWS, A_ROWS)
        return (pltpu.make_async_copy(kc.at[rows], kbuf.at[slot], isem.at[0, slot]),
                pltpu.make_async_copy(vc.at[rows], vbuf.at[slot], isem.at[1, slot]))

    def flush(step):
        slot = lax.rem(step, A_SLOTS)
        rows = pl.ds(step * A_ROWS, A_ROWS)
        return (pltpu.make_async_copy(kbuf.at[slot], kn.at[rows], osem.at[0, slot]),
                pltpu.make_async_copy(vbuf.at[slot], vn.at[rows], osem.at[1, slot]))

    @pl.when(i == 0)
    def _():
        for s in range(A_AHEAD):
            for c in fetch(s):
                c.start()

    @pl.when(i >= A_AHEAD)
    def _():
        for c in flush(i - A_AHEAD):
            c.wait()

    @pl.when(i + A_AHEAD < A_STEPS)
    def _():
        for c in fetch(i + A_AHEAD):
            c.start()

    for c in fetch(i):
        c.wait()
    slot = lax.rem(i, A_SLOTS)

    for r in range(A_ROWS):
        lp = pos_ref[i * A_ROWS + r] - origin
        base = pl.multiple_of((jnp.clip(lp, 0, SEQ - 1) // 16) * 16, 16)
        hit = base + lax.broadcasted_iota(jnp.int32, (16, HD), 0) == lp
        for buf, src in ((kbuf, NH), (vbuf, NH + 1)):
            new = jnp.broadcast_to(qkv[src, r:r + 1, :], (16, HD))
            old = buf[slot, r, pl.ds(base, 16), :].astype(F32)
            buf[slot, r, pl.ds(base, 16), :] = jnp.where(hit, new, old).astype(BF16)

    for r in range(A_ROWS):
        q = qkv[0:NH, r, :].astype(BF16)
        sbuf[r] = lax.dot_general(q, kbuf[slot, r], (((1,), (1,)), ((), ())), preferred_element_type=F32)
    lane = lax.broadcasted_iota(jnp.int32, (NH, HD), 1)
    mcol = jnp.zeros((NH, HD), F32)
    lcol = jnp.zeros((NH, HD), F32)
    for r in range(A_ROWS):
        valid = lax.broadcasted_iota(jnp.int32, (NH, SEQ), 1) <= pos_ref[i * A_ROWS + r] - origin
        s = jnp.where(valid, sbuf[r], -jnp.inf)
        m = jnp.max(s, axis=-1, keepdims=True)
        m = jnp.where(m == -jnp.inf, NEG_FILL, m)
        e = jnp.exp2((s - m) * SCALE2)
        l = jnp.sum(e, axis=-1, keepdims=True)
        ebuf[r] = e.astype(BF16)
        mcol = jnp.where(lane == r, m * SCALE2, mcol)
        lcol = jnp.where(lane == r, l, lcol)
    for r in range(A_ROWS):
        o[:, r, :] = jnp.dot(ebuf[r], vbuf[slot, r], preferred_element_type=F32)
    pad = jnp.zeros((16, HD), F32)
    ml[...] = jnp.transpose(jnp.concatenate([mcol, pad, lcol, pad], axis=0))[:A_ROWS]

    for c in flush(i):
        c.start()

    @pl.when(i == A_STEPS - 1)
    def _():
        for step in range(A_STEPS - A_AHEAD, A_STEPS):
            for c in flush(step):
                c.wait()


def attn_call(positions, qkv, k_cache, v_cache):
    anyspace = pl.BlockSpec(memory_space=pl.ANY)
    cache = jax.ShapeDtypeStruct((ROWS, SEQ, HD), BF16)
    return pl.pallas_call(
        attn_kernel,
        out_shape=(jax.ShapeDtypeStruct((NH, ROWS, HD), F32), jax.ShapeDtypeStruct((ROWS, HD), F32), cache, cache),
        grid_spec=pltpu.PrefetchScalarGridSpec(
            num_scalar_prefetch=1,
            grid=(A_STEPS,),
            in_specs=[pl.BlockSpec((NH + 2, A_ROWS, HD), lambda i, p: (0, i, 0)), anyspace, anyspace],
            out_specs=(pl.BlockSpec((NH, A_ROWS, HD), lambda i, p: (0, i, 0)), pl.BlockSpec((A_ROWS, HD), lambda i, p: (i, 0)),
                       anyspace, anyspace),
            scratch_shapes=[
                pltpu.VMEM((A_SLOTS, A_ROWS, SEQ, HD), BF16),
                pltpu.VMEM((A_SLOTS, A_ROWS, SEQ, HD), BF16),
                pltpu.VMEM((A_ROWS, NH, SEQ), F32),
                pltpu.VMEM((A_ROWS, NH, SEQ), BF16),
                pltpu.SemaphoreType.DMA((2, A_SLOTS)),
                pltpu.SemaphoreType.DMA((2, A_SLOTS)),
            ]),
        compiler_params=pltpu.CompilerParams(vmem_limit_bytes=ATTN_LIMIT, dimension_semantics=('arbitrary',)),
        cost_estimate=pl.CostEstimate(flops=4 * ROWS * NH * SEQ * HD, bytes_accessed=8 * ROWS * SEQ * HD, transcendentals=0),
        name='attn',
    )(positions, qkv, k_cache, v_cache)


W_SLOTS = 6
DOWN_STEPS = 12
NR = 3
RT = NH // NR
NK = 3
CT = NH // NK
OWN = NH // 8


def tail_kernel(act, ml_in, o_in, hid, w_down, w_out, out,
                wbuf, wobuf, part, mine, orecv0, orecv1, orecv2, stats, mlr, wts,
                precv0, precv1, precv2, gath, ctx,
                wsem, wosem, osend, orecv, msend, mrecv, psend, precv, gsend, grecv):
    here = Place()
    own, other = here.own, here.other

    def fetch_down(step):
        slot = lax.rem(step, W_SLOTS)
        col = pl.multiple_of(step * 512, 512)
        return pltpu.make_async_copy(w_down.at[:, pl.ds(col, 512)], wbuf.at[slot], wsem.at[slot])

    def wo_copy(k):
        rows = pl.ds(pl.multiple_of((k * RT + own(RT, 2)) * HD, HD), RT // 8 * HD)
        return pltpu.make_async_copy(w_out.at[rows], wobuf.at[pl.ds(k * (RT // 8 * HD), RT // 8 * HD)], wosem.at[k])

    o_to = (orecv0, orecv1, orecv2)

    def o_send(level, k):
        if level == 0:
            src = o_in.at[pl.ds(k * RT + other(RT, 0), RT // 2)]
        else:
            src = mine.at[k, pl.ds(other(RT, level) - own(RT, 0), RT // PART[level])]
        return here.remote(level, src, o_to[level].at[k], osend.at[level, k], orecv.at[level, k])

    def m_send(level):
        src = ml_in if level == 0 else stats.at[level - 1]
        return here.remote(level, src, mlr.at[level], msend.at[level], mrecv.at[level])

    lanes = lax.broadcasted_iota(jnp.int32, (ROWS, HD), 1)

    def merge_stats(level):
        m_send(level).wait()
        ours = ml_in[...] if level == 0 else stats[level - 1]
        theirs = mlr[level]
        top = jnp.maximum(ours, theirs)
        w1 = jnp.exp2(ours - top)
        w2 = jnp.exp2(theirs - top)
        total = ours * pltpu.roll(w1, 64, 1) + theirs * pltpu.roll(w2, 64, 1)
        wts[level, 0] = w1
        wts[level, 1] = w2
        stats[level] = jnp.where(lanes < 64, top, total)

    def shift(v, by):
        return pltpu.roll(v, lax.rem(HD - by, HD), 1)

    def merge_heads(level, k):
        o_send(level, k).wait()
        first_head = k * RT + own(RT, level)
        w1 = shift(wts[level, 0], first_head)
        w2 = shift(wts[level, 1], first_head)
        base = own(RT, level) - own(RT, 0)
        for h in range(RT // PART[level]):
            ours = o_in[first_head + h] if level == 0 else mine[k, base + h]
            mine[k, base + h] = ours * w1[:, h:h + 1] + o_to[level][k, h] * w2[:, h:h + 1]
        if level < 2:
            if k == 0:
                m_send(level + 1).start()
            o_send(level + 1, k).start()
        else:
            l = shift(stats[2], first_head)
            for h in range(RT // 8):
                col = (k * (RT // 8) + h) * HD
                ctx[:, col:col + HD] = (mine[k, base + h] / l[:, 64 + h:65 + h]).astype(BF16)

    def down_block(n, carry):
        fetch_down(n).wait()
        acc = jnp.dot(act[...], wbuf[lax.rem(n, W_SLOTS)], preferred_element_type=F32)

        @pl.when(n + W_SLOTS < DOWN_STEPS)
        def _():
            fetch_down(n + W_SLOTS).start()

        for t in range(4):
            part[n * 4 + t] = acc[:, t * HD:(t + 1) * HD]
        return carry

    def down(lo, hi):
        lax.fori_loop(lo, hi, down_block, 0)

    p_to = (precv0, precv1, precv2)

    def p_send(level, k):
        src = part.at[pl.ds(k * CT + other(CT, level), CT // PART[level])]
        return here.remote(level, src, p_to[level].at[k], psend.at[level, k], precv.at[level, k])

    def g_send(level, k):
        where = gath.at[pl.ds(k * CT + own(CT, level), CT // PART[level])]
        return here.remote(level, where, where, gsend.at[level, k], grecv.at[level, k])

    def project(k):
        def tiles(n, carry):
            t0 = k * CT + n * 4
            acc = jnp.dot(ctx[...], wobuf[:, pl.ds(pl.multiple_of(t0 * HD, 512), 512)], preferred_element_type=F32)
            for t in range(4):
                part[t0 + t] += acc[:, t * HD:(t + 1) * HD]
            return carry

        lax.fori_loop(0, CT // 4, tiles, 0)
        p_send(0, k).start()

    def reduce(level, k):
        p_send(level, k).wait()
        base, count = k * CT + own(CT, level), CT // PART[level]
        if level < 2:
            part[pl.ds(base, count)] = part[pl.ds(base, count)] + p_to[level][k]
            p_send(level + 1, k).start()
        else:
            for t in range(count):
                col = pl.multiple_of((base + t) * HD, HD)
                total = hid[:, pl.ds(col, HD)].astype(F32) + (part[base + t] + p_to[2][k, t])
                gath[base + t] = total.astype(BF16).astype(F32)
            g_send(2, k).start()

    def gather(level, k):
        g_send(level, k).wait()
        if level > 0:
            g_send(level - 1, k).start()
        else:
            for t in range(CT):
                col = (k * CT + t) * HD
                out[:, col:col + HD] = gath[k * CT + t].astype(BF16)

    here.enter()
    m_send(0).start()
    for k in range(NR):
        o_send(0, k).start()
    for s in range(4):
        fetch_down(s).start()

    merge_stats(0)
    for k in range(NR):
        merge_heads(0, k)
    for s in range(4, W_SLOTS):
        fetch_down(s).start()
    down(0, 3)
    merge_stats(1)
    merge_heads(1, 0)
    down(3, 5)
    for k in range(NR):
        wo_copy(k).start()
    merge_heads(1, 1)
    merge_stats(2)
    merge_heads(2, 0)
    down(5, 6)
    merge_heads(1, 2)
    merge_heads(2, 1)
    down(6, 8)
    for k in range(NR):
        wo_copy(k).wait()
    merge_heads(2, 2)
    project(0)
    project(1)
    reduce(0, 0)
    down(8, 10)
    reduce(0, 1)
    down(10, 12)
    project(2)
    reduce(0, 2)
    for wave in range(1, NK + 5):
        for k in range(NK):
            s = wave - k
            if 1 <= s <= 2:
                reduce(s, k)
            elif 3 <= s <= 5:
                gather(5 - s, k)


def tail_call(act, ml, o, hidden, w_down, w_out):
    vm = pl.BlockSpec(memory_space=pltpu.VMEM)
    anyspace = pl.BlockSpec(memory_space=pl.ANY)
    dma = pltpu.SemaphoreType.DMA
    return pl.pallas_call(
        tail_kernel,
        out_shape=jax.ShapeDtypeStruct((ROWS, D), BF16),
        in_specs=[vm, vm, vm, vm, anyspace, anyspace],
        out_specs=vm,
        scratch_shapes=[
            pltpu.VMEM((W_SLOTS, 3072, 512), BF16),
            pltpu.VMEM((OWN * HD, D), BF16),
            pltpu.VMEM((NH, ROWS, HD), F32),
            pltpu.VMEM((NR, RT // 2, ROWS, HD), F32),
            pltpu.VMEM((NR, RT // 2, ROWS, HD), F32),
            pltpu.VMEM((NR, RT // 4, ROWS, HD), F32),
            pltpu.VMEM((NR, RT // 8, ROWS, HD), F32),
            pltpu.VMEM((LEVELS, ROWS, HD), F32),
            pltpu.VMEM((LEVELS, ROWS, HD), F32),
            pltpu.VMEM((LEVELS, 2, ROWS, HD), F32),
            pltpu.VMEM((NK, CT // 2, ROWS, HD), F32),
            pltpu.VMEM((NK, CT // 4, ROWS, HD), F32),
            pltpu.VMEM((NK, CT // 8, ROWS, HD), F32),
            pltpu.VMEM((NH, ROWS, HD), F32),
            pltpu.VMEM((ROWS, OWN * HD), BF16),
            dma((W_SLOTS,)), dma((NR,)),
            dma((LEVELS, NR)), dma((LEVELS, NR)), dma((LEVELS,)), dma((LEVELS,)),
            dma((LEVELS, NK)), dma((LEVELS, NK)), dma((LEVELS, NK)), dma((LEVELS, NK)),
        ],
        compiler_params=pltpu.CompilerParams(collective_id=1, has_side_effects=True, vmem_limit_bytes=TAIL_LIMIT),
        cost_estimate=pl.CostEstimate(flops=2 * ROWS * D * FF, bytes_accessed=2 * D * FF, transcendentals=0),
        name='tail',
    )(act, ml, o, hidden, w_down, w_out)


def device_step(hidden, ln_gamma, ln_beta, w_qkv, w_out, w_up, w_down, k_cache, v_cache, positions):
    inv_freq = 1.0 / (ROPE_BASE ** (jnp.arange(0, HD, 2, dtype=F32) / HD))
    freq = jnp.concatenate([inv_freq, inv_freq])[None, :]
    inputs = [pltpu.with_memory_space_constraint(v, pltpu.HBM)
              for v in (hidden, ln_gamma[None, :], ln_beta[None, :], positions[None, :])]
    qkv, act = front_call(*inputs, freq, w_qkv, w_up)
    o, ml, k_next, v_next = attn_call(positions, qkv, k_cache, v_cache)
    out = tail_call(act, ml, o, hidden, w_down, w_out)
    return out, k_next, v_next


def solution(mesh):
    cache_spec = P('dp', 'sp', None)
    in_specs = (P('dp', None), P(None), P(None), P(None, None), P(None, None), P(None, 'sp'), P('sp', None), cache_spec, cache_spec, P('dp'))
    out_specs = (P('dp', None), cache_spec, cache_spec)
    return jax.shard_map(device_step, mesh=mesh, in_specs=in_specs, out_specs=out_specs, check_vma=False)
```

```python
import functools

import jax
import jax.numpy as jnp
from jax import lax
from jax.experimental import pallas as pl
from jax.experimental.pallas import tpu as pltpu
from jax.sharding import PartitionSpec as P

LN_EPS = 1e-5
ROPE_BASE = 10000.0
NEG_FILL = -1e30
SCALE2 = 128 ** -0.5 * 1.4426950408889634
MESH = pl.DeviceIdType.MESH
FRONT_LIMIT = 46_000_000
ATTN_LIMIT = 40_000_000
TAIL_LIMIT = 48_500_000

ROWS = 128
D = 6144
HD = 128
NH = 48
SEQ = 512
FF = 3072
F32 = jnp.float32
BF16 = jnp.bfloat16


def device(y, x, core):
    return {'sp': (y * 2 + x) * 2 + core}


class Place:
    def __init__(self):
        sp = lax.axis_index('sp')
        core = lax.rem(sp, 2)
        x = lax.rem(sp // 2, 2)
        y = sp // 4
        first = 1 - core
        x_peer = device(y, 1 - x, core)['sp']
        y_peer = device(1 - y, x, core)['sp']
        self.sides = (core, x * first + y * core, y * first + x * core)
        self.peers = (device(y, x, first), {'sp': x_peer * first + y_peer * core}, {'sp': y_peer * first + x_peer * core})

    def own(self, tiles, level):
        return sum(self.sides[n] * (tiles // (2, 4, 8)[n]) for n in range(level + 1))

    def other(self, tiles, level):
        start = self.own(tiles, level - 1) if level else 0
        return start + (1 - self.sides[level]) * (tiles // (2, 4, 8)[level])

    def remote(self, level, src, dst, send, recv):
        return pltpu.make_async_remote_copy(src_ref=src, dst_ref=dst, send_sem=send, recv_sem=recv,
                                            device_id=self.peers[level], device_id_type=MESH)

    def arrive(self):
        for peer in self.peers:
            pl.semaphore_signal(pltpu.get_barrier_semaphore(), inc=1, device_id=peer, device_id_type=MESH)

    def meet(self):
        pl.semaphore_wait(pltpu.get_barrier_semaphore(), len(self.peers))


PART = (2, 4, 8)
LEVELS = 3
SIZE = (8, 16, 16, 8)
BASE = (0, 8, 24, 40)
CHUNKS = len(SIZE)


def span(k, level):
    return pl.ds(BASE[k] // PART[level], SIZE[k] // PART[level])


U_SLOTS = 6
OWN = NH // 8
UP_STEPS = 12


def front_kernel(hid_hbm, gam_hbm, bet_hbm, pos_hbm, freq, w, w_up, qkv, act,
                 hid, gam, bet, pos, normed, qbuf, kvbuf, wbuf, cos, sin, insem, qsem, wsem, gsend, grecv):
    here = Place()
    inputs = [pltpu.make_async_copy(src, dst, insem.at[n]) for n, (src, dst) in enumerate(
        ((pos_hbm, pos), (hid_hbm, hid), (gam_hbm, gam), (bet_hbm, bet)))]
    for copy in inputs:
        copy.start()
    here.arrive()

    def part_of(k):
        return pl.ds(BASE[k] // 8 * HD, SIZE[k] // 8 * HD)

    def fetch_q(k):
        if k == CHUNKS:
            return pltpu.make_async_copy(w.at[:, pl.ds(NH * HD, 2 * HD)], kvbuf, qsem.at[k])
        col = pl.multiple_of((BASE[k] + here.own(SIZE[k], 2)) * HD, HD)
        return pltpu.make_async_copy(w.at[:, pl.ds(col, SIZE[k] // 8 * HD)], qbuf.at[:, part_of(k)], qsem.at[k])

    def fetch_up(step):
        slot = lax.rem(step, U_SLOTS)
        col = pl.multiple_of((step // 2) * 512, 512)
        row = pl.multiple_of(lax.rem(step, 2) * 3072, 3072)
        return pltpu.make_async_copy(w_up.at[pl.ds(row, 3072), pl.ds(col, 512)], wbuf.at[slot], wsem.at[slot])

    for k in range(CHUNKS + 1):
        fetch_q(k).start()

    inputs[0].wait()
    angle = jnp.transpose(jnp.broadcast_to(pos[...].astype(F32), (ROWS, HD))) * freq[...]
    cos[...] = jnp.cos(angle)
    lanes = lax.broadcasted_iota(jnp.int32, (ROWS, HD), 1)
    sine = jnp.sin(angle)
    sin[...] = jnp.where(lanes < HD // 2, -sine, sine)

    def norm_rows(i, carry):
        rows = pl.ds(pl.multiple_of(i * 16, 16), 16)
        v = hid[rows, :].astype(F32)
        mean = jnp.sum(v, axis=-1, keepdims=True) * (1.0 / D)
        cen = v - mean
        var = jnp.sum(cen * cen, axis=-1, keepdims=True) * (1.0 / D)
        normed[rows, :] = (cen * lax.rsqrt(var + LN_EPS) * gam[...] + bet[...]).astype(BF16)
        return carry

    for copy in inputs[1:]:
        copy.wait()
    for step in range(2):
        fetch_up(step).start()
    lax.fori_loop(0, ROWS // 16, norm_rows, 0, unroll=4)
    here.meet()

    def rotate(v):
        return (v * cos[...] + pltpu.roll(v, HD // 2, 1) * sin[...]).astype(BF16).astype(F32)

    def g_send(level, k):
        where = qkv.at[pl.ds(BASE[k] + here.own(SIZE[k], level), SIZE[k] // PART[level])]
        return here.remote(level, where, where, gsend.at[level, k], grecv.at[level, k])

    def project(weights):
        acc = jnp.dot(normed[...], weights[...], preferred_element_type=F32)
        return [acc[:, h:h + HD].astype(BF16).astype(F32) for h in range(0, acc.shape[1], HD)]

    def queries(chunks):
        for k in chunks:
            fetch_q(k).wait()
        first = BASE[chunks[0]] // 8
        heads = project(qbuf.at[:, pl.ds(first * HD, OWN // 2 * HD)])
        for k in chunks:
            for h in range(SIZE[k] // 8):
                qkv[BASE[k] + here.own(SIZE[k], 2) + h] = rotate(heads[BASE[k] // 8 - first + h])
            g_send(2, k).start()

    def gather(level, k):
        g_send(level, k).wait()
        if level:
            g_send(level - 1, k).start()

    def up_block(n, carry):
        fetch_up(2 * n).wait()
        s0 = lax.rem(2 * n, U_SLOTS)
        acc = jnp.dot(normed[:, :3072], wbuf[s0], preferred_element_type=F32)
        fetch_up(2 * n + 1).wait()
        acc += jnp.dot(normed[:, 3072:], wbuf[s0 + 1], preferred_element_type=F32)
        for half in range(2):
            nxt = 2 * n + half + U_SLOTS

            @pl.when(nxt < UP_STEPS)
            def _():
                fetch_up(nxt).start()

        act[:, pl.ds(pl.multiple_of(n * 512, 512), 512)] = (
            0.5 * acc * (1.0 + lax.erf(acc * (2.0 ** -0.5)))).astype(BF16)
        return carry

    def up(lo, hi):
        lax.fori_loop(lo, hi, up_block, 0)

    queries((0, 1))
    queries((2, 3))
    for step in range(2, U_SLOTS):
        fetch_up(step).start()
    fetch_q(CHUNKS).wait()
    k_new, v_new = project(kvbuf)
    qkv[NH] = rotate(k_new)
    qkv[NH + 1] = v_new
    gather(2, 0)
    gather(2, 1)
    up(0, 1)
    gather(2, 2)
    up(1, 2)
    gather(2, 3)
    gather(1, 0)
    up(2, 3)
    gather(0, 0)
    gather(1, 1)
    up(3, 4)
    gather(0, 1)
    up(4, 5)
    gather(1, 2)
    gather(1, 3)
    up(5, 6)
    gather(0, 2)
    gather(0, 3)


def front_call(hidden, gam, bet, pos, freq, w_qkv, w_up):
    vm = pl.BlockSpec(memory_space=pltpu.VMEM)
    hbm = pl.BlockSpec(memory_space=pltpu.HBM)
    dma = pltpu.SemaphoreType.DMA
    return pl.pallas_call(
        front_kernel,
        out_shape=(jax.ShapeDtypeStruct((NH + 2, ROWS, HD), F32), jax.ShapeDtypeStruct((ROWS, FF), BF16)),
        in_specs=[hbm, hbm, hbm, hbm, vm, hbm, hbm],
        out_specs=(vm, vm),
        scratch_shapes=[
            pltpu.VMEM((ROWS, D), BF16),
            pltpu.VMEM((1, D), F32),
            pltpu.VMEM((1, D), F32),
            pltpu.VMEM((1, ROWS), jnp.int32),
            pltpu.VMEM((ROWS, D), BF16),
            pltpu.VMEM((D, OWN * HD), BF16),
            pltpu.VMEM((D, 2 * HD), BF16),
            pltpu.VMEM((U_SLOTS, 3072, 512), BF16),
            pltpu.VMEM((ROWS, HD), F32),
            pltpu.VMEM((ROWS, HD), F32),
            dma((4,)), dma((CHUNKS + 1,)), dma((U_SLOTS,)), dma((LEVELS, CHUNKS)), dma((LEVELS, CHUNKS)),
        ],
        compiler_params=pltpu.CompilerParams(collective_id=0, has_side_effects=True, vmem_limit_bytes=FRONT_LIMIT),
        cost_estimate=pl.CostEstimate(flops=2 * ROWS * D * (FF + 1024), bytes_accessed=2 * D * (FF + 1024), transcendentals=0),
        name='front',
    )(hidden, gam, bet, pos, freq, w_qkv, w_up)


A_ROWS = 8
A_STEPS = ROWS // A_ROWS
A_SLOTS = 6
A_AHEAD = 3


def attn_kernel(pos_ref, qkv, kc, vc, o, ml, kn, vn, kbuf, vbuf, sbuf, ebuf, isem, osem):
    i = pl.program_id(0)
    origin = lax.axis_index('sp') * SEQ

    def fetch(step):
        slot = lax.rem(step, A_SLOTS)
        rows = pl.ds(step * A_ROWS, A_ROWS)
        return (pltpu.make_async_copy(kc.at[rows], kbuf.at[slot], isem.at[0, slot]),
                pltpu.make_async_copy(vc.at[rows], vbuf.at[slot], isem.at[1, slot]))

    def flush(step):
        slot = lax.rem(step, A_SLOTS)
        rows = pl.ds(step * A_ROWS, A_ROWS)
        return (pltpu.make_async_copy(kbuf.at[slot], kn.at[rows], osem.at[0, slot]),
                pltpu.make_async_copy(vbuf.at[slot], vn.at[rows], osem.at[1, slot]))

    @pl.when(i == 0)
    def _():
        for s in range(A_AHEAD):
            for c in fetch(s):
                c.start()

    @pl.when(i >= A_AHEAD)
    def _():
        for c in flush(i - A_AHEAD):
            c.wait()

    @pl.when(i + A_AHEAD < A_STEPS)
    def _():
        for c in fetch(i + A_AHEAD):
            c.start()

    for c in fetch(i):
        c.wait()
    slot = lax.rem(i, A_SLOTS)

    for r in range(A_ROWS):
        lp = pos_ref[i * A_ROWS + r] - origin
        base = pl.multiple_of((jnp.clip(lp, 0, SEQ - 1) // 16) * 16, 16)
        hit = base + lax.broadcasted_iota(jnp.int32, (16, HD), 0) == lp
        for buf, src in ((kbuf, NH), (vbuf, NH + 1)):
            new = jnp.broadcast_to(qkv[src, r:r + 1, :], (16, HD))
            old = buf[slot, r, pl.ds(base, 16), :].astype(F32)
            buf[slot, r, pl.ds(base, 16), :] = jnp.where(hit, new, old).astype(BF16)

    for r in range(A_ROWS):
        q = qkv[0:NH, r, :].astype(BF16)
        sbuf[r] = lax.dot_general(q, kbuf[slot, r], (((1,), (1,)), ((), ())), preferred_element_type=F32)
    lane = lax.broadcasted_iota(jnp.int32, (NH, HD), 1)
    mcol = jnp.zeros((NH, HD), F32)
    lcol = jnp.zeros((NH, HD), F32)
    for r in range(A_ROWS):
        valid = lax.broadcasted_iota(jnp.int32, (NH, SEQ), 1) <= pos_ref[i * A_ROWS + r] - origin
        s = jnp.where(valid, sbuf[r], -jnp.inf)
        m = jnp.max(s, axis=-1, keepdims=True)
        m = jnp.where(m == -jnp.inf, NEG_FILL, m)
        e = jnp.exp2((s - m) * SCALE2)
        l = jnp.sum(e, axis=-1, keepdims=True)
        ebuf[r] = e.astype(BF16)
        mcol = jnp.where(lane == r, m * SCALE2, mcol)
        lcol = jnp.where(lane == r, l, lcol)
    for r in range(A_ROWS):
        o[:, r, :] = jnp.dot(ebuf[r], vbuf[slot, r], preferred_element_type=F32)
    pad = jnp.zeros((16, HD), F32)
    ml[...] = jnp.transpose(jnp.concatenate([mcol, pad, lcol, pad], axis=0))[:A_ROWS]

    for c in flush(i):
        c.start()

    @pl.when(i == A_STEPS - 1)
    def _():
        for step in range(A_STEPS - A_AHEAD, A_STEPS):
            for c in flush(step):
                c.wait()


def attn_call(positions, qkv, k_cache, v_cache):
    anyspace = pl.BlockSpec(memory_space=pl.ANY)
    cache = jax.ShapeDtypeStruct((ROWS, SEQ, HD), BF16)
    return pl.pallas_call(
        attn_kernel,
        out_shape=(jax.ShapeDtypeStruct((NH, ROWS, HD), F32), jax.ShapeDtypeStruct((ROWS, HD), F32), cache, cache),
        grid_spec=pltpu.PrefetchScalarGridSpec(
            num_scalar_prefetch=1,
            grid=(A_STEPS,),
            in_specs=[pl.BlockSpec((NH + 2, A_ROWS, HD), lambda i, p: (0, i, 0)), anyspace, anyspace],
            out_specs=(pl.BlockSpec((NH, A_ROWS, HD), lambda i, p: (0, i, 0)), pl.BlockSpec((A_ROWS, HD), lambda i, p: (i, 0)),
                       anyspace, anyspace),
            scratch_shapes=[
                pltpu.VMEM((A_SLOTS, A_ROWS, SEQ, HD), BF16),
                pltpu.VMEM((A_SLOTS, A_ROWS, SEQ, HD), BF16),
                pltpu.VMEM((A_ROWS, NH, SEQ), F32),
                pltpu.VMEM((A_ROWS, NH, SEQ), BF16),
                pltpu.SemaphoreType.DMA((2, A_SLOTS)),
                pltpu.SemaphoreType.DMA((2, A_SLOTS)),
            ]),
        compiler_params=pltpu.CompilerParams(vmem_limit_bytes=ATTN_LIMIT, dimension_semantics=('arbitrary',)),
        cost_estimate=pl.CostEstimate(flops=4 * ROWS * NH * SEQ * HD, bytes_accessed=8 * ROWS * SEQ * HD, transcendentals=0),
        name='attn',
    )(positions, qkv, k_cache, v_cache)


W_SLOTS = 6
DOWN_STEPS = 12
ORDER = ((0, 0), (1, 0), (0, 1), (2, 0), (1, 1), (3, 0), (2, 1), (3, 1), (0, 2), (1, 2), (0, 3), (2, 2), (1, 3), (3, 2),
         (0, 4), (2, 3), (1, 4), (3, 3), (0, 5), (2, 4), (0, 6), (3, 4), (1, 5), (1, 6), (2, 5), (3, 5), (2, 6), (3, 6))


def tail_kernel(act, ml_in, o_in, hid, w_down, w_out, out,
                wbuf, wobuf, part, mine, orecv0, orecv1, orecv2, stats, mlr, wts,
                precv0, precv1, precv2, gath, ctx,
                wsem, wosem, osend, orecv, msend, mrecv, psend, precv, gsend, grecv):
    here = Place()
    own, other = here.own, here.other

    def fetch_down(step):
        slot = lax.rem(step, W_SLOTS)
        col = pl.multiple_of(step * 512, 512)
        return pltpu.make_async_copy(w_down.at[:, pl.ds(col, 512)], wbuf.at[slot], wsem.at[slot])

    def wo_copy(k):
        rows = pl.ds(pl.multiple_of((BASE[k] + own(SIZE[k], 2)) * HD, HD), SIZE[k] // 8 * HD)
        return pltpu.make_async_copy(w_out.at[rows], wobuf.at[pl.ds(BASE[k] // 8 * HD, SIZE[k] // 8 * HD)], wosem.at[k])

    o_to = (orecv0, orecv1, orecv2)

    def mine_at(k, start):
        return BASE[k] // 2 + start - own(SIZE[k], 0)

    def o_send(level, k):
        start, count = other(SIZE[k], level), SIZE[k] // PART[level]
        src = mine.at[pl.ds(mine_at(k, start), count)] if level else o_in.at[pl.ds(BASE[k] + start, count)]
        return here.remote(level, src, o_to[level].at[span(k, level)], osend.at[level, k], orecv.at[level, k])

    def m_send(level):
        src = ml_in if level == 0 else stats.at[level - 1]
        return here.remote(level, src, mlr.at[level], msend.at[level], mrecv.at[level])

    lanes = lax.broadcasted_iota(jnp.int32, (ROWS, HD), 1)

    def merge_stats(level):
        m_send(level).wait()
        ours = ml_in[...] if level == 0 else stats[level - 1]
        theirs = mlr[level]
        top = jnp.maximum(ours, theirs)
        w1 = jnp.exp2(ours - top)
        w2 = jnp.exp2(theirs - top)
        total = ours * pltpu.roll(w1, 64, 1) + theirs * pltpu.roll(w2, 64, 1)
        wts[level, 0] = w1
        wts[level, 1] = w2
        stats[level] = jnp.where(lanes < 64, top, total)

    def shift(v, by):
        return pltpu.roll(v, lax.rem(HD - by, HD), 1)

    def merge_heads(level, k):
        if k == 0:
            merge_stats(level)
        o_send(level, k).wait()
        start = own(SIZE[k], level)
        w1 = shift(wts[level, 0], BASE[k] + start)
        w2 = shift(wts[level, 1], BASE[k] + start)
        base = mine_at(k, start)
        for h in range(SIZE[k] // PART[level]):
            ours = mine[base + h] if level else o_in[BASE[k] + start + h]
            mine[base + h] = ours * w1[:, h:h + 1] + o_to[level][BASE[k] // PART[level] + h] * w2[:, h:h + 1]
        if level < 2:
            if k == 0:
                m_send(level + 1).start()
            o_send(level + 1, k).start()
        else:
            l = shift(stats[2], BASE[k] + start)
            for h in range(SIZE[k] // 8):
                col = (BASE[k] // 8 + h) * HD
                ctx[:, col:col + HD] = (mine[base + h] / l[:, 64 + h:65 + h]).astype(BF16)

    def down_block(n, carry):
        fetch_down(n).wait()
        acc = jnp.dot(act[...], wbuf[lax.rem(n, W_SLOTS)], preferred_element_type=F32)

        @pl.when(n + W_SLOTS < DOWN_STEPS)
        def _():
            fetch_down(n + W_SLOTS).start()

        for t in range(4):
            part[n * 4 + t] = acc[:, t * HD:(t + 1) * HD]
        return carry

    def down(lo, hi):
        lax.fori_loop(lo, hi, down_block, 0)

    p_to = (precv0, precv1, precv2)

    def p_send(level, k):
        src = part.at[pl.ds(BASE[k] + other(SIZE[k], level), SIZE[k] // PART[level])]
        return here.remote(level, src, p_to[level].at[span(k, level)], psend.at[level, k], precv.at[level, k])

    def g_send(level, k):
        where = gath.at[pl.ds(BASE[k] + own(SIZE[k], level), SIZE[k] // PART[level])]
        return here.remote(level, where, where, gsend.at[level, k], grecv.at[level, k])

    def project(k):
        def tiles(n, carry):
            t0 = BASE[k] + n * 4
            acc = jnp.dot(ctx[...], wobuf[:, pl.ds(pl.multiple_of(t0 * HD, 512), 512)], preferred_element_type=F32)
            for t in range(4):
                part[t0 + t] += acc[:, t * HD:(t + 1) * HD]
            return carry

        lax.fori_loop(0, SIZE[k] // 4, tiles, 0)
        p_send(0, k).start()

    def reduce(level, k):
        p_send(level, k).wait()
        base, count = BASE[k] + own(SIZE[k], level), SIZE[k] // PART[level]
        if level < 2:
            part[pl.ds(base, count)] = part[pl.ds(base, count)] + p_to[level][span(k, level)]
            p_send(level + 1, k).start()
        else:
            for t in range(count):
                col = pl.multiple_of((base + t) * HD, HD)
                total = hid[:, pl.ds(col, HD)].astype(F32) + (part[base + t] + p_to[2][BASE[k] // 8 + t])
                gath[base + t] = total.astype(BF16).astype(F32)
            g_send(2, k).start()

    def gather(level, k):
        g_send(level, k).wait()
        if level > 0:
            g_send(level - 1, k).start()
        else:
            for t in range(BASE[k], BASE[k] + SIZE[k]):
                out[:, t * HD:(t + 1) * HD] = gath[t].astype(BF16)

    here.arrive()
    for s in range(4):
        fetch_down(s).start()
    here.meet()
    m_send(0).start()
    for k in range(CHUNKS):
        o_send(0, k).start()
    for k in range(CHUNKS):
        merge_heads(0, k)
    for s in range(4, W_SLOTS):
        fetch_down(s).start()
    down(0, 2)
    merge_heads(1, 0)
    down(2, 6)
    for k in range(CHUNKS):
        wo_copy(k).start()
    merge_heads(1, 1)
    merge_heads(2, 0)
    down(6, 8)
    merge_heads(1, 2)
    down(8, 10)
    merge_heads(1, 3)
    merge_heads(2, 1)
    merge_heads(2, 2)
    down(10, 12)
    for k in range(CHUNKS):
        wo_copy(k).wait()
    merge_heads(2, 3)
    for k, stage in ORDER:
        if stage == 0:
            project(k)
        elif stage <= 3:
            reduce(stage - 1, k)
        else:
            gather(6 - stage, k)


def tail_call(act, ml, o, hidden, w_down, w_out):
    vm = pl.BlockSpec(memory_space=pltpu.VMEM)
    anyspace = pl.BlockSpec(memory_space=pl.ANY)
    dma = pltpu.SemaphoreType.DMA
    return pl.pallas_call(
        tail_kernel,
        out_shape=jax.ShapeDtypeStruct((ROWS, D), BF16),
        in_specs=[vm, vm, vm, vm, anyspace, anyspace],
        out_specs=vm,
        scratch_shapes=[
            pltpu.VMEM((W_SLOTS, 3072, 512), BF16),
            pltpu.VMEM((OWN * HD, D), BF16),
            pltpu.VMEM((NH, ROWS, HD), F32),
            pltpu.VMEM((NH // 2, ROWS, HD), F32),
            pltpu.VMEM((NH // 2, ROWS, HD), F32),
            pltpu.VMEM((NH // 4, ROWS, HD), F32),
            pltpu.VMEM((NH // 8, ROWS, HD), F32),
            pltpu.VMEM((LEVELS, ROWS, HD), F32),
            pltpu.VMEM((LEVELS, ROWS, HD), F32),
            pltpu.VMEM((LEVELS, 2, ROWS, HD), F32),
            pltpu.VMEM((NH // 2, ROWS, HD), F32),
            pltpu.VMEM((NH // 4, ROWS, HD), F32),
            pltpu.VMEM((NH // 8, ROWS, HD), F32),
            pltpu.VMEM((NH, ROWS, HD), F32),
            pltpu.VMEM((ROWS, OWN * HD), BF16),
            dma((W_SLOTS,)), dma((CHUNKS,)),
            dma((LEVELS, CHUNKS)), dma((LEVELS, CHUNKS)), dma((LEVELS,)), dma((LEVELS,)),
            dma((LEVELS, CHUNKS)), dma((LEVELS, CHUNKS)), dma((LEVELS, CHUNKS)), dma((LEVELS, CHUNKS)),
        ],
        compiler_params=pltpu.CompilerParams(collective_id=1, has_side_effects=True, vmem_limit_bytes=TAIL_LIMIT),
        cost_estimate=pl.CostEstimate(flops=2 * ROWS * D * FF, bytes_accessed=2 * D * FF, transcendentals=0),
        name='tail',
    )(act, ml, o, hidden, w_down, w_out)


def device_step(hidden, ln_gamma, ln_beta, w_qkv, w_out, w_up, w_down, k_cache, v_cache, positions):
    inv_freq = 1.0 / (ROPE_BASE ** (jnp.arange(0, HD, 2, dtype=F32) / HD))
    freq = jnp.concatenate([inv_freq, inv_freq])[None, :]
    inputs = [pltpu.with_memory_space_constraint(v, pltpu.HBM)
              for v in (hidden, ln_gamma[None, :], ln_beta[None, :], positions[None, :])]
    qkv, act = front_call(*inputs, freq, w_qkv, w_up)
    o, ml, k_next, v_next = attn_call(positions, qkv, k_cache, v_cache)
    out = tail_call(act, ml, o, hidden, w_down, w_out)
    return out, k_next, v_next


def solution(mesh):
    cache_spec = P('dp', 'sp', None)
    in_specs = (P('dp', None), P(None), P(None), P(None, None), P(None, None), P(None, 'sp'), P('sp', None), cache_spec, cache_spec, P('dp'))
    out_specs = (P('dp', None), cache_spec, cache_spec)
    return jax.shard_map(device_step, mesh=mesh, in_specs=in_specs, out_specs=out_specs, check_vma=False)
```

```python
import functools

import jax
import jax.numpy as jnp
from jax import lax
from jax.experimental import pallas as pl
from jax.experimental.pallas import tpu as pltpu
from jax.sharding import PartitionSpec as P

LN_EPS = 1e-5
ROPE_BASE = 10000.0
NEG_FILL = -1e30
SCALE2 = 128 ** -0.5 * 1.4426950408889634
MESH = pl.DeviceIdType.MESH
FRONT_LIMIT = 46_000_000
ATTN_LIMIT = 40_000_000
TAIL_LIMIT = 47_000_000

ROWS = 128
D = 6144
HD = 128
NH = 48
SEQ = 512
FF = 3072
F32 = jnp.float32
BF16 = jnp.bfloat16


def device(y, x, core):
    return {'sp': (y * 2 + x) * 2 + core}


class Place:
    def __init__(self):
        sp = lax.axis_index('sp')
        core = lax.rem(sp, 2)
        x = lax.rem(sp // 2, 2)
        y = sp // 4
        self.x, self.y = x, y
        first = 1 - core
        x_peer = device(y, 1 - x, core)['sp']
        y_peer = device(1 - y, x, core)['sp']
        self.sides = (core, x * first + y * core, y * first + x * core)
        self.peers = (device(y, x, first), {'sp': x_peer * first + y_peer * core}, {'sp': y_peer * first + x_peer * core})

    def own(self, tiles, level):
        return sum(self.sides[n] * (tiles // (2, 4, 8)[n]) for n in range(level + 1))

    def other(self, tiles, level):
        start = self.own(tiles, level - 1) if level else 0
        return start + (1 - self.sides[level]) * (tiles // (2, 4, 8)[level])

    def remote(self, level, src, dst, send, recv):
        return pltpu.make_async_remote_copy(src_ref=src, dst_ref=dst, send_sem=send, recv_sem=recv,
                                            device_id=self.peers[level], device_id_type=MESH)

    def arrive(self):
        for peer in self.peers:
            pl.semaphore_signal(pltpu.get_barrier_semaphore(), inc=1, device_id=peer, device_id_type=MESH)

    def meet(self):
        pl.semaphore_wait(pltpu.get_barrier_semaphore(), len(self.peers))


PART = (2, 4, 8)
LEVELS = 3
SIZE = (8, 16, 16, 8)
BASE = (0, 8, 24, 40)
CHUNKS = len(SIZE)


def span(k, level):
    return pl.ds(BASE[k] // PART[level], SIZE[k] // PART[level])


U_SLOTS = 6
OWN = NH // 8
UP_STEPS = 12


def front_kernel(hid_hbm, gam_hbm, bet_hbm, pos_hbm, freq, w, w_up, qkv, act,
                 hid, gam, bet, pos, normed, qbuf, kvbuf, wbuf, cos, sin, insem, qsem, wsem, gsend, grecv):
    here = Place()
    inputs = [pltpu.make_async_copy(src, dst, insem.at[n]) for n, (src, dst) in enumerate(
        ((pos_hbm, pos), (hid_hbm, hid), (gam_hbm, gam), (bet_hbm, bet)))]
    for copy in inputs:
        copy.start()
    here.arrive()

    def part_of(k):
        return pl.ds(BASE[k] // 8 * HD, SIZE[k] // 8 * HD)

    def fetch_q(k):
        if k == CHUNKS:
            return pltpu.make_async_copy(w.at[:, pl.ds(NH * HD, 2 * HD)], kvbuf, qsem.at[k])
        col = pl.multiple_of((BASE[k] + here.own(SIZE[k], 2)) * HD, HD)
        return pltpu.make_async_copy(w.at[:, pl.ds(col, SIZE[k] // 8 * HD)], qbuf.at[:, part_of(k)], qsem.at[k])

    def fetch_up(step):
        slot = lax.rem(step, U_SLOTS)
        col = pl.multiple_of((step // 2) * 512, 512)
        row = pl.multiple_of(lax.rem(step, 2) * 3072, 3072)
        return pltpu.make_async_copy(w_up.at[pl.ds(row, 3072), pl.ds(col, 512)], wbuf.at[slot], wsem.at[slot])

    for k in range(CHUNKS + 1):
        fetch_q(k).start()

    inputs[0].wait()
    angle = jnp.transpose(jnp.broadcast_to(pos[...].astype(F32), (ROWS, HD))) * freq[...]
    cos[...] = jnp.cos(angle)
    lanes = lax.broadcasted_iota(jnp.int32, (ROWS, HD), 1)
    sine = jnp.sin(angle)
    sin[...] = jnp.where(lanes < HD // 2, -sine, sine)

    def norm_rows(i, carry):
        rows = pl.ds(pl.multiple_of(i * 16, 16), 16)
        v = hid[rows, :].astype(F32)
        mean = jnp.sum(v, axis=-1, keepdims=True) * (1.0 / D)
        cen = v - mean
        var = jnp.sum(cen * cen, axis=-1, keepdims=True) * (1.0 / D)
        normed[rows, :] = (cen * lax.rsqrt(var + LN_EPS) * gam[...] + bet[...]).astype(BF16)
        return carry

    for copy in inputs[1:]:
        copy.wait()
    for step in range(2):
        fetch_up(step).start()
    lax.fori_loop(0, ROWS // 16, norm_rows, 0, unroll=4)
    here.meet()

    def rotate(v):
        return (v * cos[...] + pltpu.roll(v, HD // 2, 1) * sin[...]).astype(BF16).astype(F32)

    def g_send(level, k):
        where = qkv.at[pl.ds(BASE[k] + here.own(SIZE[k], level), SIZE[k] // PART[level])]
        return here.remote(level, where, where, gsend.at[level, k], grecv.at[level, k])

    def project(weights):
        acc = jnp.dot(normed[...], weights[...], preferred_element_type=F32)
        return [acc[:, h:h + HD].astype(BF16).astype(F32) for h in range(0, acc.shape[1], HD)]

    def queries(chunks):
        for k in chunks:
            fetch_q(k).wait()
        first = BASE[chunks[0]] // 8
        heads = project(qbuf.at[:, pl.ds(first * HD, OWN // 2 * HD)])
        for k in chunks:
            for h in range(SIZE[k] // 8):
                qkv[BASE[k] + here.own(SIZE[k], 2) + h] = rotate(heads[BASE[k] // 8 - first + h])
            g_send(2, k).start()

    def gather(level, k):
        g_send(level, k).wait()
        if level:
            g_send(level - 1, k).start()

    def up_block(n, carry):
        fetch_up(2 * n).wait()
        s0 = lax.rem(2 * n, U_SLOTS)
        acc = jnp.dot(normed[:, :3072], wbuf[s0], preferred_element_type=F32)
        fetch_up(2 * n + 1).wait()
        acc += jnp.dot(normed[:, 3072:], wbuf[s0 + 1], preferred_element_type=F32)
        for half in range(2):
            nxt = 2 * n + half + U_SLOTS

            @pl.when(nxt < UP_STEPS)
            def _():
                fetch_up(nxt).start()

        act[:, pl.ds(pl.multiple_of(n * 512, 512), 512)] = (
            0.5 * acc * (1.0 + lax.erf(acc * (2.0 ** -0.5)))).astype(BF16)
        return carry

    def up(lo, hi):
        lax.fori_loop(lo, hi, up_block, 0)

    queries((0, 1))
    queries((2, 3))
    for step in range(2, U_SLOTS):
        fetch_up(step).start()
    fetch_q(CHUNKS).wait()
    k_new, v_new = project(kvbuf)
    qkv[NH] = rotate(k_new)
    qkv[NH + 1] = v_new
    gather(2, 0)
    gather(2, 1)
    up(0, 1)
    gather(2, 2)
    up(1, 2)
    gather(2, 3)
    gather(1, 0)
    up(2, 3)
    gather(0, 0)
    gather(1, 1)
    up(3, 4)
    gather(0, 1)
    up(4, 5)
    gather(1, 2)
    gather(1, 3)
    up(5, 6)
    gather(0, 2)
    gather(0, 3)


def front_call(hidden, gam, bet, pos, freq, w_qkv, w_up):
    vm = pl.BlockSpec(memory_space=pltpu.VMEM)
    hbm = pl.BlockSpec(memory_space=pltpu.HBM)
    dma = pltpu.SemaphoreType.DMA
    return pl.pallas_call(
        front_kernel,
        out_shape=(jax.ShapeDtypeStruct((NH + 2, ROWS, HD), F32), jax.ShapeDtypeStruct((ROWS, FF), BF16)),
        in_specs=[hbm, hbm, hbm, hbm, vm, hbm, hbm],
        out_specs=(vm, vm),
        scratch_shapes=[
            pltpu.VMEM((ROWS, D), BF16),
            pltpu.VMEM((1, D), F32),
            pltpu.VMEM((1, D), F32),
            pltpu.VMEM((1, ROWS), jnp.int32),
            pltpu.VMEM((ROWS, D), BF16),
            pltpu.VMEM((D, OWN * HD), BF16),
            pltpu.VMEM((D, 2 * HD), BF16),
            pltpu.VMEM((U_SLOTS, 3072, 512), BF16),
            pltpu.VMEM((ROWS, HD), F32),
            pltpu.VMEM((ROWS, HD), F32),
            dma((4,)), dma((CHUNKS + 1,)), dma((U_SLOTS,)), dma((LEVELS, CHUNKS)), dma((LEVELS, CHUNKS)),
        ],
        compiler_params=pltpu.CompilerParams(collective_id=0, has_side_effects=True, vmem_limit_bytes=FRONT_LIMIT),
        cost_estimate=pl.CostEstimate(flops=2 * ROWS * D * (FF + 1024), bytes_accessed=2 * D * (FF + 1024), transcendentals=0),
        name='front',
    )(hidden, gam, bet, pos, freq, w_qkv, w_up)


A_ROWS = 8
A_STEPS = ROWS // A_ROWS
A_SLOTS = 6
A_AHEAD = 3


def attn_kernel(pos_ref, qkv, kc, vc, o, ml, kn, vn, kbuf, vbuf, sbuf, ebuf, isem, osem):
    i = pl.program_id(0)
    origin = lax.axis_index('sp') * SEQ

    def fetch(step):
        slot = lax.rem(step, A_SLOTS)
        rows = pl.ds(step * A_ROWS, A_ROWS)
        return (pltpu.make_async_copy(kc.at[rows], kbuf.at[slot], isem.at[0, slot]),
                pltpu.make_async_copy(vc.at[rows], vbuf.at[slot], isem.at[1, slot]))

    def flush(step):
        slot = lax.rem(step, A_SLOTS)
        rows = pl.ds(step * A_ROWS, A_ROWS)
        return (pltpu.make_async_copy(kbuf.at[slot], kn.at[rows], osem.at[0, slot]),
                pltpu.make_async_copy(vbuf.at[slot], vn.at[rows], osem.at[1, slot]))

    @pl.when(i == 0)
    def _():
        for s in range(A_AHEAD):
            for c in fetch(s):
                c.start()

    @pl.when(i >= A_AHEAD)
    def _():
        for c in flush(i - A_AHEAD):
            c.wait()

    @pl.when(i + A_AHEAD < A_STEPS)
    def _():
        for c in fetch(i + A_AHEAD):
            c.start()

    for c in fetch(i):
        c.wait()
    slot = lax.rem(i, A_SLOTS)

    for r in range(A_ROWS):
        lp = pos_ref[i * A_ROWS + r] - origin
        base = pl.multiple_of((jnp.clip(lp, 0, SEQ - 1) // 16) * 16, 16)
        hit = base + lax.broadcasted_iota(jnp.int32, (16, HD), 0) == lp
        for buf, src in ((kbuf, NH), (vbuf, NH + 1)):
            new = jnp.broadcast_to(qkv[src, r:r + 1, :], (16, HD))
            old = buf[slot, r, pl.ds(base, 16), :].astype(F32)
            buf[slot, r, pl.ds(base, 16), :] = jnp.where(hit, new, old).astype(BF16)

    for r in range(A_ROWS):
        q = qkv[0:NH, r, :].astype(BF16)
        sbuf[r] = lax.dot_general(q, kbuf[slot, r], (((1,), (1,)), ((), ())), preferred_element_type=F32)
    lane = lax.broadcasted_iota(jnp.int32, (NH, HD), 1)
    mcol = jnp.zeros((NH, HD), F32)
    lcol = jnp.zeros((NH, HD), F32)
    for r in range(A_ROWS):
        valid = lax.broadcasted_iota(jnp.int32, (NH, SEQ), 1) <= pos_ref[i * A_ROWS + r] - origin
        s = jnp.where(valid, sbuf[r], -jnp.inf)
        m = jnp.max(s, axis=-1, keepdims=True)
        m = jnp.where(m == -jnp.inf, NEG_FILL, m)
        e = jnp.exp2((s - m) * SCALE2)
        l = jnp.sum(e, axis=-1, keepdims=True)
        ebuf[r] = e.astype(BF16)
        mcol = jnp.where(lane == r, m * SCALE2, mcol)
        lcol = jnp.where(lane == r, l, lcol)
    for r in range(A_ROWS):
        o[:, r, :] = jnp.dot(ebuf[r], vbuf[slot, r], preferred_element_type=F32)
    pad = jnp.zeros((16, HD), F32)
    ml[...] = jnp.transpose(jnp.concatenate([mcol, pad, lcol, pad], axis=0))[:A_ROWS]

    for c in flush(i):
        c.start()

    @pl.when(i == A_STEPS - 1)
    def _():
        for step in range(A_STEPS - A_AHEAD, A_STEPS):
            for c in flush(step):
                c.wait()


def attn_call(positions, qkv, k_cache, v_cache):
    anyspace = pl.BlockSpec(memory_space=pl.ANY)
    cache = jax.ShapeDtypeStruct((ROWS, SEQ, HD), BF16)
    return pl.pallas_call(
        attn_kernel,
        out_shape=(jax.ShapeDtypeStruct((NH, ROWS, HD), F32), jax.ShapeDtypeStruct((ROWS, HD), F32), cache, cache),
        grid_spec=pltpu.PrefetchScalarGridSpec(
            num_scalar_prefetch=1,
            grid=(A_STEPS,),
            in_specs=[pl.BlockSpec((NH + 2, A_ROWS, HD), lambda i, p: (0, i, 0)), anyspace, anyspace],
            out_specs=(pl.BlockSpec((NH, A_ROWS, HD), lambda i, p: (0, i, 0)), pl.BlockSpec((A_ROWS, HD), lambda i, p: (i, 0)),
                       anyspace, anyspace),
            scratch_shapes=[
                pltpu.VMEM((A_SLOTS, A_ROWS, SEQ, HD), BF16),
                pltpu.VMEM((A_SLOTS, A_ROWS, SEQ, HD), BF16),
                pltpu.VMEM((A_ROWS, NH, SEQ), F32),
                pltpu.VMEM((A_ROWS, NH, SEQ), BF16),
                pltpu.SemaphoreType.DMA((2, A_SLOTS)),
                pltpu.SemaphoreType.DMA((2, A_SLOTS)),
            ]),
        compiler_params=pltpu.CompilerParams(vmem_limit_bytes=ATTN_LIMIT, dimension_semantics=('arbitrary',)),
        cost_estimate=pl.CostEstimate(flops=4 * ROWS * NH * SEQ * HD, bytes_accessed=8 * ROWS * SEQ * HD, transcendentals=0),
        name='attn',
    )(positions, qkv, k_cache, v_cache)


W_SLOTS = 5
DOWN_STEPS = 12
F_CHUNKS = 6
HALF = NH // 2
ORDER = ((0, 0), (1, 0), (2, 0), (3, 0), (4, 0), (5, 0), (0, 2), (1, 2), (2, 2), (0, 3), (3, 2), (1, 3),
         (2, 3), (4, 2), (0, 4), (5, 2), (3, 3), (1, 4), (2, 4), (4, 3), (0, 5), (5, 3), (0, 6), (3, 4),
         (1, 5), (4, 4), (1, 6), (5, 4), (2, 5), (3, 5), (2, 6), (4, 5), (3, 6), (4, 6), (5, 5), (5, 6))


def tail_kernel(act, ml_in, o_in, hid, w_down, w_out, out,
                wbuf, wobuf, part, mine, orecv0, orecv1, orecv2, stats, mlr, wts,
                precv0, precv1, precv2, gath, ctxf, ctx,
                wsem, wosem, osend, orecv, msend, mrecv, csend, crecv, psend, precv, gsend, grecv):
    here = Place()
    own, other = here.own, here.other

    def fetch_down(step):
        slot = lax.rem(step, W_SLOTS)
        col = pl.multiple_of((lax.rem(step, 2) * F_CHUNKS + step // 2) * 512, 512)
        return pltpu.make_async_copy(w_down.at[:, pl.ds(col, 512)], wbuf.at[slot], wsem.at[slot])

    def head_at(core, k):
        turn = (here.x, here.y) if core == 0 else (here.y, here.x)
        return BASE[k] + core * (SIZE[k] // 2) + turn[0] * (SIZE[k] // 4) + turn[1] * (SIZE[k] // 8)

    def wo_copy(core, k):
        rows = pl.ds(pl.multiple_of(head_at(core, k) * HD, HD), SIZE[k] // 8 * HD)
        cols = pl.ds(pl.multiple_of(here.sides[0] * (HALF * HD), HALF * HD), HALF * HD)
        dst = wobuf.at[pl.ds((core * OWN + BASE[k] // 8) * HD, SIZE[k] // 8 * HD)]
        return pltpu.make_async_copy(w_out.at[rows, cols], dst, wosem.at[core, k])

    o_to = (orecv0, orecv1, orecv2)

    def mine_at(k, start):
        return BASE[k] // 2 + start - own(SIZE[k], 0)

    def o_send(level, k):
        start, count = other(SIZE[k], level), SIZE[k] // PART[level]
        src = mine.at[pl.ds(mine_at(k, start), count)] if level else o_in.at[pl.ds(BASE[k] + start, count)]
        return here.remote(level, src, o_to[level].at[span(k, level)], osend.at[level, k], orecv.at[level, k])

    def m_send(level):
        src = ml_in if level == 0 else stats.at[level - 1]
        return here.remote(level, src, mlr.at[level], msend.at[level], mrecv.at[level])

    lanes = lax.broadcasted_iota(jnp.int32, (ROWS, HD), 1)

    def merge_stats(level):
        m_send(level).wait()
        ours = ml_in[...] if level == 0 else stats[level - 1]
        theirs = mlr[level]
        top = jnp.maximum(ours, theirs)
        w1 = jnp.exp2(ours - top)
        w2 = jnp.exp2(theirs - top)
        total = ours * pltpu.roll(w1, 64, 1) + theirs * pltpu.roll(w2, 64, 1)
        wts[level, 0] = w1
        wts[level, 1] = w2
        stats[level] = jnp.where(lanes < 64, top, total)

    def shift(v, by):
        return pltpu.roll(v, lax.rem(HD - by, HD), 1)

    def c_send(k):
        where = ctxf.at[pl.ds(here.sides[0] * OWN + BASE[k] // 8, SIZE[k] // 8)]
        return here.remote(0, where, where, csend.at[k], crecv.at[k])

    def merge_heads(level, k):
        if k == 0:
            merge_stats(level)
        o_send(level, k).wait()
        start = own(SIZE[k], level)
        w1 = shift(wts[level, 0], BASE[k] + start)
        w2 = shift(wts[level, 1], BASE[k] + start)
        base = mine_at(k, start)
        for h in range(SIZE[k] // PART[level]):
            ours = mine[base + h] if level else o_in[BASE[k] + start + h]
            mine[base + h] = ours * w1[:, h:h + 1] + o_to[level][BASE[k] // PART[level] + h] * w2[:, h:h + 1]
        if level < 2:
            if k == 0:
                m_send(level + 1).start()
            o_send(level + 1, k).start()
        else:
            l = shift(stats[2], BASE[k] + start)
            for h in range(SIZE[k] // 8):
                value = (mine[base + h] / l[:, 64 + h:65 + h]).astype(BF16)
                ctxf[here.sides[0] * OWN + BASE[k] // 8 + h] = value.astype(F32)
            c_send(k).start()

    def d_send(k):
        src = part.at[pl.ds((1 - here.sides[0]) * HALF + 4 * k, 4)]
        return here.remote(0, src, precv0.at[pl.ds(4 * k, 4)], psend.at[0, k], precv.at[0, k])

    def down_pair(k, carry):
        for side in range(2):
            n = 2 * k + side
            fetch_down(n).wait()
            acc = jnp.dot(act[...], wbuf[lax.rem(n, W_SLOTS)], preferred_element_type=F32)

            @pl.when(n + W_SLOTS < DOWN_STEPS)
            def _():
                fetch_down(n + W_SLOTS).start()

            for t in range(4):
                part[side * HALF + 4 * k + t] = acc[:, t * HD:(t + 1) * HD]
        d_send(k).start()
        return carry

    def down(lo, hi):
        lax.fori_loop(lo, hi, down_pair, 0)

    p_to = (precv0, precv1, precv2)

    def tile(k, level):
        return here.sides[0] * HALF + 4 * k + own(8, level) - own(8, 0)

    def p_send(level, k):
        count = 8 // PART[level]
        src = part.at[pl.ds(here.sides[0] * HALF + 4 * k + other(8, level) - own(8, 0), count)]
        return here.remote(level, src, p_to[level].at[pl.ds(k * count, count)], psend.at[level, k], precv.at[level, k])

    def g_send(level, k):
        where = gath.at[pl.ds(tile(k, level), 8 // PART[level])]
        return here.remote(level, where, where, gsend.at[level, k], grecv.at[level, k])

    def project(k):
        d_send(k).wait()
        acc = jnp.dot(ctx[...], wobuf[:, k * 512:(k + 1) * 512], preferred_element_type=F32)
        for t in range(4):
            part[tile(k, 0) + t] = (part[tile(k, 0) + t] + precv0[4 * k + t]) + acc[:, t * HD:(t + 1) * HD]
        p_send(1, k).start()

    def reduce(level, k):
        p_send(level, k).wait()
        base, count = tile(k, level), 8 // PART[level]
        if level < 2:
            part[pl.ds(base, count)] = part[pl.ds(base, count)] + p_to[level][pl.ds(k * count, count)]
            p_send(level + 1, k).start()
        else:
            col = pl.multiple_of(base * HD, HD)
            total = hid[:, pl.ds(col, HD)].astype(F32) + (part[base] + precv2[k])
            gath[base] = total.astype(BF16).astype(F32)
            g_send(2, k).start()

    def gather(level, k):
        g_send(level, k).wait()
        if level > 0:
            g_send(level - 1, k).start()
        else:
            for t in range(4 * k, 4 * k + 4):
                for col in (t, HALF + t):
                    out[:, col * HD:(col + 1) * HD] = gath[col].astype(BF16)

    here.arrive()
    for s in range(4):
        fetch_down(s).start()
    here.meet()
    m_send(0).start()
    for k in range(CHUNKS):
        o_send(0, k).start()
    for k in range(CHUNKS):
        merge_heads(0, k)
    for s in range(4, W_SLOTS):
        fetch_down(s).start()
    down(0, 1)
    merge_heads(1, 0)
    down(1, 3)
    for core in range(2):
        for k in range(CHUNKS):
            wo_copy(core, k).start()
    merge_heads(1, 1)
    merge_heads(2, 0)
    down(3, 4)
    merge_heads(1, 2)
    down(4, 5)
    merge_heads(1, 3)
    merge_heads(2, 1)
    merge_heads(2, 2)
    down(5, 6)
    for core in range(2):
        for k in range(CHUNKS):
            wo_copy(core, k).wait()
    merge_heads(2, 3)
    for k in range(CHUNKS):
        c_send(k).wait()
    for h in range(2 * OWN):
        ctx[:, h * HD:(h + 1) * HD] = ctxf[h].astype(BF16)
    for k, stage in ORDER:
        if stage == 0:
            project(k)
        elif stage <= 3:
            reduce(stage - 1, k)
        else:
            gather(6 - stage, k)


def tail_call(act, ml, o, hidden, w_down, w_out):
    vm = pl.BlockSpec(memory_space=pltpu.VMEM)
    anyspace = pl.BlockSpec(memory_space=pl.ANY)
    dma = pltpu.SemaphoreType.DMA
    return pl.pallas_call(
        tail_kernel,
        out_shape=jax.ShapeDtypeStruct((ROWS, D), BF16),
        in_specs=[vm, vm, vm, vm, anyspace, anyspace],
        out_specs=vm,
        scratch_shapes=[
            pltpu.VMEM((W_SLOTS, 3072, 512), BF16),
            pltpu.VMEM((2 * OWN * HD, HALF * HD), BF16),
            pltpu.VMEM((NH, ROWS, HD), F32),
            pltpu.VMEM((NH // 2, ROWS, HD), F32),
            pltpu.VMEM((NH // 2, ROWS, HD), F32),
            pltpu.VMEM((NH // 4, ROWS, HD), F32),
            pltpu.VMEM((NH // 8, ROWS, HD), F32),
            pltpu.VMEM((LEVELS, ROWS, HD), F32),
            pltpu.VMEM((LEVELS, ROWS, HD), F32),
            pltpu.VMEM((LEVELS, 2, ROWS, HD), F32),
            pltpu.VMEM((NH // 2, ROWS, HD), F32),
            pltpu.VMEM((NH // 4, ROWS, HD), F32),
            pltpu.VMEM((NH // 8, ROWS, HD), F32),
            pltpu.VMEM((NH, ROWS, HD), F32),
            pltpu.VMEM((2 * OWN, ROWS, HD), F32),
            pltpu.VMEM((ROWS, 2 * OWN * HD), BF16),
            dma((W_SLOTS,)), dma((2, CHUNKS)),
            dma((LEVELS, CHUNKS)), dma((LEVELS, CHUNKS)), dma((LEVELS,)), dma((LEVELS,)), dma((CHUNKS,)), dma((CHUNKS,)),
            dma((LEVELS, F_CHUNKS)), dma((LEVELS, F_CHUNKS)), dma((LEVELS, F_CHUNKS)), dma((LEVELS, F_CHUNKS)),
        ],
        compiler_params=pltpu.CompilerParams(collective_id=1, has_side_effects=True, vmem_limit_bytes=TAIL_LIMIT),
        cost_estimate=pl.CostEstimate(flops=2 * ROWS * D * FF, bytes_accessed=2 * D * FF, transcendentals=0),
        name='tail',
    )(act, ml, o, hidden, w_down, w_out)


def device_step(hidden, ln_gamma, ln_beta, w_qkv, w_out, w_up, w_down, k_cache, v_cache, positions):
    inv_freq = 1.0 / (ROPE_BASE ** (jnp.arange(0, HD, 2, dtype=F32) / HD))
    freq = jnp.concatenate([inv_freq, inv_freq])[None, :]
    inputs = [pltpu.with_memory_space_constraint(v, pltpu.HBM)
              for v in (hidden, ln_gamma[None, :], ln_beta[None, :], positions[None, :])]
    qkv, act = front_call(*inputs, freq, w_qkv, w_up)
    o, ml, k_next, v_next = attn_call(positions, qkv, k_cache, v_cache)
    out = tail_call(act, ml, o, hidden, w_down, w_out)
    return out, k_next, v_next


def solution(mesh):
    cache_spec = P('dp', 'sp', None)
    in_specs = (P('dp', None), P(None), P(None), P(None, None), P(None, None), P(None, 'sp'), P('sp', None), cache_spec, cache_spec, P('dp'))
    out_specs = (P('dp', None), cache_spec, cache_spec)
    return jax.shard_map(device_step, mesh=mesh, in_specs=in_specs, out_specs=out_specs, check_vma=False)
```

```python
import functools

import jax
import jax.numpy as jnp
from jax import lax
from jax.experimental import pallas as pl
from jax.experimental.pallas import tpu as pltpu
from jax.sharding import PartitionSpec as P

LN_EPS = 1e-5
ROPE_BASE = 10000.0
NEG_FILL = -1e30
SCALE2 = 128 ** -0.5 * 1.4426950408889634
MESH = pl.DeviceIdType.MESH
FRONT_LIMIT = 46_000_000
ATTN_LIMIT = 40_000_000
TAIL_LIMIT = 47_000_000

ROWS = 128
D = 6144
HD = 128
NH = 48
SEQ = 512
FF = 3072
F32 = jnp.float32
BF16 = jnp.bfloat16


def device(y, x, core):
    return {'sp': (y * 2 + x) * 2 + core}


class Place:
    def __init__(self):
        sp = lax.axis_index('sp')
        core = lax.rem(sp, 2)
        x = lax.rem(sp // 2, 2)
        y = sp // 4
        self.x, self.y = x, y
        first = 1 - core
        x_peer = device(y, 1 - x, core)['sp']
        y_peer = device(1 - y, x, core)['sp']
        self.sides = (core, x * first + y * core, y * first + x * core)
        self.peers = (device(y, x, first), {'sp': x_peer * first + y_peer * core}, {'sp': y_peer * first + x_peer * core})

    def own(self, tiles, level):
        return sum(self.sides[n] * (tiles // (2, 4, 8)[n]) for n in range(level + 1))

    def other(self, tiles, level):
        start = self.own(tiles, level - 1) if level else 0
        return start + (1 - self.sides[level]) * (tiles // (2, 4, 8)[level])

    def remote(self, level, src, dst, send, recv):
        return pltpu.make_async_remote_copy(src_ref=src, dst_ref=dst, send_sem=send, recv_sem=recv,
                                            device_id=self.peers[level], device_id_type=MESH)

    def arrive(self):
        for peer in self.peers:
            pl.semaphore_signal(pltpu.get_barrier_semaphore(), inc=1, device_id=peer, device_id_type=MESH)

    def meet(self):
        pl.semaphore_wait(pltpu.get_barrier_semaphore(), len(self.peers))


PART = (2, 4, 8)
LEVELS = 3
SIZE = (8, 16, 16, 8)
BASE = (0, 8, 24, 40)
CHUNKS = len(SIZE)


def span(k, level):
    return pl.ds(BASE[k] // PART[level], SIZE[k] // PART[level])


U_SLOTS = 6
OWN = NH // 8
UP_STEPS = 12


def front_kernel(hid_hbm, gam_hbm, bet_hbm, pos_hbm, freq, w, w_up, qkv, act,
                 hid, gam, bet, pos, normed, qbuf, kvbuf, wbuf, cos, sin, insem, qsem, wsem, gsend, grecv):
    here = Place()
    inputs = [pltpu.make_async_copy(src, dst, insem.at[n]) for n, (src, dst) in enumerate(
        ((pos_hbm, pos), (hid_hbm, hid), (gam_hbm, gam), (bet_hbm, bet)))]
    for copy in inputs:
        copy.start()
    here.arrive()

    def part_of(k):
        return pl.ds(BASE[k] // 8 * HD, SIZE[k] // 8 * HD)

    def fetch_q(k):
        if k == CHUNKS:
            return pltpu.make_async_copy(w.at[:, pl.ds(NH * HD, 2 * HD)], kvbuf, qsem.at[k])
        col = pl.multiple_of((BASE[k] + here.own(SIZE[k], 2)) * HD, HD)
        return pltpu.make_async_copy(w.at[:, pl.ds(col, SIZE[k] // 8 * HD)], qbuf.at[:, part_of(k)], qsem.at[k])

    def fetch_up(step):
        slot = lax.rem(step, U_SLOTS)
        col = pl.multiple_of((step // 2) * 512, 512)
        row = pl.multiple_of(lax.rem(step, 2) * 3072, 3072)
        return pltpu.make_async_copy(w_up.at[pl.ds(row, 3072), pl.ds(col, 512)], wbuf.at[slot], wsem.at[slot])

    for k in range(CHUNKS + 1):
        fetch_q(k).start()

    inputs[0].wait()
    angle = jnp.transpose(jnp.broadcast_to(pos[...].astype(F32), (ROWS, HD))) * freq[...]
    cos[...] = jnp.cos(angle)
    lanes = lax.broadcasted_iota(jnp.int32, (ROWS, HD), 1)
    sine = jnp.sin(angle)
    sin[...] = jnp.where(lanes < HD // 2, -sine, sine)

    def norm_rows(i, carry):
        rows = pl.ds(pl.multiple_of(i * 16, 16), 16)
        v = hid[rows, :].astype(F32)
        mean = jnp.sum(v, axis=-1, keepdims=True) * (1.0 / D)
        cen = v - mean
        var = jnp.sum(cen * cen, axis=-1, keepdims=True) * (1.0 / D)
        normed[rows, :] = (cen * lax.rsqrt(var + LN_EPS) * gam[...] + bet[...]).astype(BF16)
        return carry

    for copy in inputs[1:]:
        copy.wait()
    for step in range(2):
        fetch_up(step).start()
    lax.fori_loop(0, ROWS // 16, norm_rows, 0, unroll=4)
    here.meet()

    def rotate(v):
        return (v * cos[...] + pltpu.roll(v, HD // 2, 1) * sin[...]).astype(BF16).astype(F32)

    def g_send(level, k):
        where = qkv.at[pl.ds(BASE[k] + here.own(SIZE[k], level), SIZE[k] // PART[level])]
        return here.remote(level, where, where, gsend.at[level, k], grecv.at[level, k])

    def project(weights):
        acc = jnp.dot(normed[...], weights[...], preferred_element_type=F32)
        return [acc[:, h:h + HD].astype(BF16).astype(F32) for h in range(0, acc.shape[1], HD)]

    def queries(chunks):
        for k in chunks:
            fetch_q(k).wait()
        first = BASE[chunks[0]] // 8
        heads = project(qbuf.at[:, pl.ds(first * HD, OWN // 2 * HD)])
        for k in chunks:
            for h in range(SIZE[k] // 8):
                qkv[BASE[k] + here.own(SIZE[k], 2) + h] = rotate(heads[BASE[k] // 8 - first + h])
            g_send(2, k).start()

    def gather(level, k):
        g_send(level, k).wait()
        if level:
            g_send(level - 1, k).start()

    def up_block(n, carry):
        fetch_up(2 * n).wait()
        s0 = lax.rem(2 * n, U_SLOTS)
        acc = jnp.dot(normed[:, :3072], wbuf[s0], preferred_element_type=F32)
        fetch_up(2 * n + 1).wait()
        acc += jnp.dot(normed[:, 3072:], wbuf[s0 + 1], preferred_element_type=F32)
        for half in range(2):
            nxt = 2 * n + half + U_SLOTS

            @pl.when(nxt < UP_STEPS)
            def _():
                fetch_up(nxt).start()

        act[:, pl.ds(pl.multiple_of(n * 512, 512), 512)] = (
            0.5 * acc * (1.0 + lax.erf(acc * (2.0 ** -0.5)))).astype(BF16)
        return carry

    def up(lo, hi):
        lax.fori_loop(lo, hi, up_block, 0)

    queries((0, 1))
    queries((2, 3))
    for step in range(2, U_SLOTS):
        fetch_up(step).start()
    fetch_q(CHUNKS).wait()
    k_new, v_new = project(kvbuf)
    qkv[NH] = rotate(k_new)
    qkv[NH + 1] = v_new
    gather(2, 0)
    gather(2, 1)
    up(0, 1)
    gather(2, 2)
    up(1, 2)
    gather(2, 3)
    gather(1, 0)
    up(2, 3)
    gather(0, 0)
    gather(1, 1)
    up(3, 4)
    gather(0, 1)
    up(4, 5)
    gather(1, 2)
    gather(1, 3)
    up(5, 6)
    gather(0, 2)
    gather(0, 3)


def front_call(hidden, gam, bet, pos, freq, w_qkv, w_up):
    vm = pl.BlockSpec(memory_space=pltpu.VMEM)
    hbm = pl.BlockSpec(memory_space=pltpu.HBM)
    dma = pltpu.SemaphoreType.DMA
    return pl.pallas_call(
        front_kernel,
        out_shape=(jax.ShapeDtypeStruct((NH + 2, ROWS, HD), F32), jax.ShapeDtypeStruct((ROWS, FF), BF16)),
        in_specs=[hbm, hbm, hbm, hbm, vm, hbm, hbm],
        out_specs=(vm, vm),
        scratch_shapes=[
            pltpu.VMEM((ROWS, D), BF16),
            pltpu.VMEM((1, D), F32),
            pltpu.VMEM((1, D), F32),
            pltpu.VMEM((1, ROWS), jnp.int32),
            pltpu.VMEM((ROWS, D), BF16),
            pltpu.VMEM((D, OWN * HD), BF16),
            pltpu.VMEM((D, 2 * HD), BF16),
            pltpu.VMEM((U_SLOTS, 3072, 512), BF16),
            pltpu.VMEM((ROWS, HD), F32),
            pltpu.VMEM((ROWS, HD), F32),
            dma((4,)), dma((CHUNKS + 1,)), dma((U_SLOTS,)), dma((LEVELS, CHUNKS)), dma((LEVELS, CHUNKS)),
        ],
        compiler_params=pltpu.CompilerParams(collective_id=0, has_side_effects=True, vmem_limit_bytes=FRONT_LIMIT),
        cost_estimate=pl.CostEstimate(flops=2 * ROWS * D * (FF + 1024), bytes_accessed=2 * D * (FF + 1024), transcendentals=0),
        name='front',
    )(hidden, gam, bet, pos, freq, w_qkv, w_up)


A_ROWS = 8
A_STEPS = ROWS // A_ROWS
A_SLOTS = 6
A_AHEAD = 3


def attn_kernel(pos_ref, qkv, kc, vc, o, ml, kn, vn, kbuf, vbuf, sbuf, ebuf, isem, osem):
    i = pl.program_id(0)
    origin = lax.axis_index('sp') * SEQ

    def fetch(step):
        slot = lax.rem(step, A_SLOTS)
        rows = pl.ds(step * A_ROWS, A_ROWS)
        return (pltpu.make_async_copy(kc.at[rows], kbuf.at[slot], isem.at[0, slot]),
                pltpu.make_async_copy(vc.at[rows], vbuf.at[slot], isem.at[1, slot]))

    def flush(step):
        slot = lax.rem(step, A_SLOTS)
        rows = pl.ds(step * A_ROWS, A_ROWS)
        return (pltpu.make_async_copy(kbuf.at[slot], kn.at[rows], osem.at[0, slot]),
                pltpu.make_async_copy(vbuf.at[slot], vn.at[rows], osem.at[1, slot]))

    @pl.when(i == 0)
    def _():
        for s in range(A_AHEAD):
            for c in fetch(s):
                c.start()

    @pl.when(i >= A_AHEAD)
    def _():
        for c in flush(i - A_AHEAD):
            c.wait()

    @pl.when(i + A_AHEAD < A_STEPS)
    def _():
        for c in fetch(i + A_AHEAD):
            c.start()

    for c in fetch(i):
        c.wait()
    slot = lax.rem(i, A_SLOTS)

    for r in range(A_ROWS):
        lp = pos_ref[i * A_ROWS + r] - origin
        base = pl.multiple_of((jnp.clip(lp, 0, SEQ - 1) // 16) * 16, 16)
        hit = base + lax.broadcasted_iota(jnp.int32, (16, HD), 0) == lp
        for buf, src in ((kbuf, NH), (vbuf, NH + 1)):
            new = jnp.broadcast_to(qkv[src, r:r + 1, :], (16, HD))
            old = buf[slot, r, pl.ds(base, 16), :].astype(F32)
            buf[slot, r, pl.ds(base, 16), :] = jnp.where(hit, new, old).astype(BF16)

    for r in range(A_ROWS):
        q = qkv[0:NH, r, :].astype(BF16)
        sbuf[r] = lax.dot_general(q, kbuf[slot, r], (((1,), (1,)), ((), ())), preferred_element_type=F32)
    lane = lax.broadcasted_iota(jnp.int32, (NH, HD), 1)
    mcol = jnp.zeros((NH, HD), F32)
    lcol = jnp.zeros((NH, HD), F32)
    for r in range(A_ROWS):
        valid = lax.broadcasted_iota(jnp.int32, (NH, SEQ), 1) <= pos_ref[i * A_ROWS + r] - origin
        s = jnp.where(valid, sbuf[r], -jnp.inf)
        m = jnp.max(s, axis=-1, keepdims=True)
        m = jnp.where(m == -jnp.inf, NEG_FILL, m)
        e = jnp.exp2((s - m) * SCALE2)
        l = jnp.sum(e, axis=-1, keepdims=True)
        ebuf[r] = e.astype(BF16)
        mcol = jnp.where(lane == r, m * SCALE2, mcol)
        lcol = jnp.where(lane == r, l, lcol)
    for r in range(A_ROWS):
        o[:, r, :] = jnp.dot(ebuf[r], vbuf[slot, r], preferred_element_type=F32)
    pad = jnp.zeros((16, HD), F32)
    ml[...] = jnp.transpose(jnp.concatenate([mcol, pad, lcol, pad], axis=0))[:A_ROWS]

    for c in flush(i):
        c.start()

    @pl.when(i == A_STEPS - 1)
    def _():
        for step in range(A_STEPS - A_AHEAD, A_STEPS):
            for c in flush(step):
                c.wait()


def attn_call(positions, qkv, k_cache, v_cache):
    anyspace = pl.BlockSpec(memory_space=pl.ANY)
    cache = jax.ShapeDtypeStruct((ROWS, SEQ, HD), BF16)
    return pl.pallas_call(
        attn_kernel,
        out_shape=(jax.ShapeDtypeStruct((NH, ROWS, HD), F32), jax.ShapeDtypeStruct((ROWS, HD), F32), cache, cache),
        grid_spec=pltpu.PrefetchScalarGridSpec(
            num_scalar_prefetch=1,
            grid=(A_STEPS,),
            in_specs=[pl.BlockSpec((NH + 2, A_ROWS, HD), lambda i, p: (0, i, 0)), anyspace, anyspace],
            out_specs=(pl.BlockSpec((NH, A_ROWS, HD), lambda i, p: (0, i, 0)), pl.BlockSpec((A_ROWS, HD), lambda i, p: (i, 0)),
                       anyspace, anyspace),
            scratch_shapes=[
                pltpu.VMEM((A_SLOTS, A_ROWS, SEQ, HD), BF16),
                pltpu.VMEM((A_SLOTS, A_ROWS, SEQ, HD), BF16),
                pltpu.VMEM((A_ROWS, NH, SEQ), F32),
                pltpu.VMEM((A_ROWS, NH, SEQ), BF16),
                pltpu.SemaphoreType.DMA((2, A_SLOTS)),
                pltpu.SemaphoreType.DMA((2, A_SLOTS)),
            ]),
        compiler_params=pltpu.CompilerParams(vmem_limit_bytes=ATTN_LIMIT, dimension_semantics=('arbitrary',)),
        cost_estimate=pl.CostEstimate(flops=4 * ROWS * NH * SEQ * HD, bytes_accessed=8 * ROWS * SEQ * HD, transcendentals=0),
        name='attn',
    )(positions, qkv, k_cache, v_cache)


W_SLOTS = 5
DOWN_STEPS = 12
F_CHUNKS = 6
HALF = NH // 2
ORDER = ((0, 0), (1, 0), (2, 0), (3, 0), (4, 0), (5, 0), (0, 2), (1, 2), (2, 2), (0, 3), (3, 2), (1, 3),
         (2, 3), (4, 2), (0, 4), (5, 2), (3, 3), (1, 4), (2, 4), (4, 3), (0, 5), (5, 3), (0, 6), (3, 4),
         (1, 5), (4, 4), (1, 6), (5, 4), (2, 5), (3, 5), (2, 6), (4, 5), (3, 6), (4, 6), (5, 5), (5, 6))


def tail_kernel(act, ml_in, o_in, hid, w_down, w_out, out,
                wbuf, wobuf, part, mine, orecv0, orecv1, orecv2, stats, mlr, wts,
                precv0, precv1, precv2, gath, ctxf, ctx,
                wsem, wosem, osend, orecv, msend, mrecv, csend, crecv, psend, precv, gsend, grecv):
    here = Place()
    own, other = here.own, here.other

    def fetch_down(step):
        slot = lax.rem(step, W_SLOTS)
        col = pl.multiple_of((lax.rem(step, 2) * F_CHUNKS + step // 2) * 512, 512)
        return pltpu.make_async_copy(w_down.at[:, pl.ds(col, 512)], wbuf.at[slot], wsem.at[slot])

    def head_at(core, k):
        turn = (here.x, here.y) if core == 0 else (here.y, here.x)
        return BASE[k] + core * (SIZE[k] // 2) + turn[0] * (SIZE[k] // 4) + turn[1] * (SIZE[k] // 8)

    def wo_copy(core, k):
        rows = pl.ds(pl.multiple_of(head_at(core, k) * HD, HD), SIZE[k] // 8 * HD)
        cols = pl.ds(pl.multiple_of(here.sides[0] * (HALF * HD), HALF * HD), HALF * HD)
        dst = wobuf.at[pl.ds((core * OWN + BASE[k] // 8) * HD, SIZE[k] // 8 * HD)]
        return pltpu.make_async_copy(w_out.at[rows, cols], dst, wosem.at[core, k])

    o_to = (orecv0, orecv1, orecv2)

    def mine_at(k, start):
        return BASE[k] // 2 + start - own(SIZE[k], 0)

    def o_send(level, k):
        start, count = other(SIZE[k], level), SIZE[k] // PART[level]
        src = mine.at[pl.ds(mine_at(k, start), count)] if level else o_in.at[pl.ds(BASE[k] + start, count)]
        return here.remote(level, src, o_to[level].at[span(k, level)], osend.at[level, k], orecv.at[level, k])

    def m_send(level):
        src = ml_in if level == 0 else stats.at[level - 1]
        return here.remote(level, src, mlr.at[level], msend.at[level], mrecv.at[level])

    lanes = lax.broadcasted_iota(jnp.int32, (ROWS, HD), 1)

    def merge_stats(level):
        m_send(level).wait()
        ours = ml_in[...] if level == 0 else stats[level - 1]
        theirs = mlr[level]
        top = jnp.maximum(ours, theirs)
        w1 = jnp.exp2(ours - top)
        w2 = jnp.exp2(theirs - top)
        total = ours * pltpu.roll(w1, 64, 1) + theirs * pltpu.roll(w2, 64, 1)
        wts[level, 0] = w1
        wts[level, 1] = w2
        stats[level] = jnp.where(lanes < 64, top, total)
        if level < 2:
            m_send(level + 1).start()

    def shift(v, by):
        return pltpu.roll(v, lax.rem(HD - by, HD), 1)

    def c_send(k):
        where = ctxf.at[pl.ds(here.sides[0] * OWN + BASE[k] // 8, SIZE[k] // 8)]
        return here.remote(0, where, where, csend.at[k], crecv.at[k])

    def merge_heads(level, k):
        o_send(level, k).wait()
        start = own(SIZE[k], level)
        w1 = shift(wts[level, 0], BASE[k] + start)
        w2 = shift(wts[level, 1], BASE[k] + start)
        base = mine_at(k, start)
        for h in range(SIZE[k] // PART[level]):
            ours = mine[base + h] if level else o_in[BASE[k] + start + h]
            mine[base + h] = ours * w1[:, h:h + 1] + o_to[level][BASE[k] // PART[level] + h] * w2[:, h:h + 1]
        if level < 2:
            o_send(level + 1, k).start()
        else:
            l = shift(stats[2], BASE[k] + start)
            for h in range(SIZE[k] // 8):
                value = (mine[base + h] / l[:, 64 + h:65 + h]).astype(BF16)
                ctxf[here.sides[0] * OWN + BASE[k] // 8 + h] = value.astype(F32)
            c_send(k).start()

    def d_send(k):
        src = part.at[pl.ds((1 - here.sides[0]) * HALF + 4 * k, 4)]
        return here.remote(0, src, precv0.at[pl.ds(4 * k, 4)], psend.at[0, k], precv.at[0, k])

    def down_pair(k, carry):
        for side in range(2):
            n = 2 * k + side
            fetch_down(n).wait()
            acc = jnp.dot(act[...], wbuf[lax.rem(n, W_SLOTS)], preferred_element_type=F32)

            @pl.when(n + W_SLOTS < DOWN_STEPS)
            def _():
                fetch_down(n + W_SLOTS).start()

            for t in range(4):
                part[side * HALF + 4 * k + t] = acc[:, t * HD:(t + 1) * HD]
        d_send(k).start()
        return carry

    def down(lo, hi):
        lax.fori_loop(lo, hi, down_pair, 0)

    p_to = (precv0, precv1, precv2)

    def tile(k, level):
        return here.sides[0] * HALF + 4 * k + own(8, level) - own(8, 0)

    def p_send(level, k):
        count = 8 // PART[level]
        src = part.at[pl.ds(here.sides[0] * HALF + 4 * k + other(8, level) - own(8, 0), count)]
        return here.remote(level, src, p_to[level].at[pl.ds(k * count, count)], psend.at[level, k], precv.at[level, k])

    def g_send(level, k):
        where = gath.at[pl.ds(tile(k, level), 8 // PART[level])]
        return here.remote(level, where, where, gsend.at[level, k], grecv.at[level, k])

    def project(k):
        d_send(k).wait()
        acc = jnp.dot(ctx[...], wobuf[:, k * 512:(k + 1) * 512], preferred_element_type=F32)
        for t in range(4):
            part[tile(k, 0) + t] = (part[tile(k, 0) + t] + precv0[4 * k + t]) + acc[:, t * HD:(t + 1) * HD]
        p_send(1, k).start()

    def reduce(level, k):
        p_send(level, k).wait()
        base, count = tile(k, level), 8 // PART[level]
        if level < 2:
            part[pl.ds(base, count)] = part[pl.ds(base, count)] + p_to[level][pl.ds(k * count, count)]
            p_send(level + 1, k).start()
        else:
            col = pl.multiple_of(base * HD, HD)
            total = hid[:, pl.ds(col, HD)].astype(F32) + (part[base] + precv2[k])
            gath[base] = total.astype(BF16).astype(F32)
            g_send(2, k).start()

    def gather(level, k):
        g_send(level, k).wait()
        if level > 0:
            g_send(level - 1, k).start()
        else:
            for t in range(4 * k, 4 * k + 4):
                for col in (t, HALF + t):
                    out[:, col * HD:(col + 1) * HD] = gath[col].astype(BF16)

    here.arrive()
    for s in range(4):
        fetch_down(s).start()
    here.meet()
    m_send(0).start()
    for k in range(CHUNKS):
        o_send(0, k).start()
    merge_stats(0)
    for k in range(CHUNKS):
        merge_heads(0, k)
    for s in range(4, W_SLOTS):
        fetch_down(s).start()
    down(0, 1)
    merge_stats(1)
    merge_heads(1, 0)
    down(1, 3)
    for core in range(2):
        for k in range(CHUNKS):
            wo_copy(core, k).start()
    merge_heads(1, 1)
    merge_stats(2)
    merge_heads(2, 0)
    down(3, 4)
    merge_heads(1, 2)
    down(4, 5)
    merge_heads(1, 3)
    merge_heads(2, 1)
    merge_heads(2, 2)
    down(5, 6)
    for core in range(2):
        for k in range(CHUNKS):
            wo_copy(core, k).wait()
    merge_heads(2, 3)
    for k in range(CHUNKS):
        c_send(k).wait()
    for h in range(2 * OWN):
        ctx[:, h * HD:(h + 1) * HD] = ctxf[h].astype(BF16)
    for k, stage in ORDER:
        if stage == 0:
            project(k)
        elif stage <= 3:
            reduce(stage - 1, k)
        else:
            gather(6 - stage, k)


def tail_call(act, ml, o, hidden, w_down, w_out):
    vm = pl.BlockSpec(memory_space=pltpu.VMEM)
    anyspace = pl.BlockSpec(memory_space=pl.ANY)
    dma = pltpu.SemaphoreType.DMA
    return pl.pallas_call(
        tail_kernel,
        out_shape=jax.ShapeDtypeStruct((ROWS, D), BF16),
        in_specs=[vm, vm, vm, vm, anyspace, anyspace],
        out_specs=vm,
        scratch_shapes=[
            pltpu.VMEM((W_SLOTS, 3072, 512), BF16),
            pltpu.VMEM((2 * OWN * HD, HALF * HD), BF16),
            pltpu.VMEM((NH, ROWS, HD), F32),
            pltpu.VMEM((NH // 2, ROWS, HD), F32),
            pltpu.VMEM((NH // 2, ROWS, HD), F32),
            pltpu.VMEM((NH // 4, ROWS, HD), F32),
            pltpu.VMEM((NH // 8, ROWS, HD), F32),
            pltpu.VMEM((LEVELS, ROWS, HD), F32),
            pltpu.VMEM((LEVELS, ROWS, HD), F32),
            pltpu.VMEM((LEVELS, 2, ROWS, HD), F32),
            pltpu.VMEM((NH // 2, ROWS, HD), F32),
            pltpu.VMEM((NH // 4, ROWS, HD), F32),
            pltpu.VMEM((NH // 8, ROWS, HD), F32),
            pltpu.VMEM((NH, ROWS, HD), F32),
            pltpu.VMEM((2 * OWN, ROWS, HD), F32),
            pltpu.VMEM((ROWS, 2 * OWN * HD), BF16),
            dma((W_SLOTS,)), dma((2, CHUNKS)),
            dma((LEVELS, CHUNKS)), dma((LEVELS, CHUNKS)), dma((LEVELS,)), dma((LEVELS,)), dma((CHUNKS,)), dma((CHUNKS,)),
            dma((LEVELS, F_CHUNKS)), dma((LEVELS, F_CHUNKS)), dma((LEVELS, F_CHUNKS)), dma((LEVELS, F_CHUNKS)),
        ],
        compiler_params=pltpu.CompilerParams(collective_id=1, has_side_effects=True, vmem_limit_bytes=TAIL_LIMIT),
        cost_estimate=pl.CostEstimate(flops=2 * ROWS * D * FF, bytes_accessed=2 * D * FF, transcendentals=0),
        name='tail',
    )(act, ml, o, hidden, w_down, w_out)


def device_step(hidden, ln_gamma, ln_beta, w_qkv, w_out, w_up, w_down, k_cache, v_cache, positions):
    inv_freq = 1.0 / (ROPE_BASE ** (jnp.arange(0, HD, 2, dtype=F32) / HD))
    freq = jnp.concatenate([inv_freq, inv_freq])[None, :]
    inputs = [pltpu.with_memory_space_constraint(v, pltpu.HBM)
              for v in (hidden, ln_gamma[None, :], ln_beta[None, :], positions[None, :])]
    qkv, act = front_call(*inputs, freq, w_qkv, w_up)
    o, ml, k_next, v_next = attn_call(positions, qkv, k_cache, v_cache)
    out = tail_call(act, ml, o, hidden, w_down, w_out)
    return out, k_next, v_next


def solution(mesh):
    cache_spec = P('dp', 'sp', None)
    in_specs = (P('dp', None), P(None), P(None), P(None, None), P(None, None), P(None, 'sp'), P('sp', None), cache_spec, cache_spec, P('dp'))
    out_specs = (P('dp', None), cache_spec, cache_spec)
    return jax.shard_map(device_step, mesh=mesh, in_specs=in_specs, out_specs=out_specs, check_vma=False)
```

```python
import functools

import jax
import jax.numpy as jnp
from jax import lax
from jax.experimental import pallas as pl
from jax.experimental.pallas import tpu as pltpu
from jax.sharding import PartitionSpec as P

LN_EPS = 1e-5
ROPE_BASE = 10000.0
NEG_FILL = -1e30
SCALE2 = 128 ** -0.5 * 1.4426950408889634
MESH = pl.DeviceIdType.MESH
FRONT_LIMIT = 46_000_000
ATTN_LIMIT = 40_000_000
TAIL_LIMIT = 47_000_000

ROWS = 128
D = 6144
HD = 128
NH = 48
SEQ = 512
FF = 3072
F32 = jnp.float32
BF16 = jnp.bfloat16


def device(y, x, core):
    return {'sp': (y * 2 + x) * 2 + core}


class Place:
    def __init__(self):
        sp = lax.axis_index('sp')
        core = lax.rem(sp, 2)
        x = lax.rem(sp // 2, 2)
        y = sp // 4
        self.x, self.y = x, y
        first = 1 - core
        x_peer = device(y, 1 - x, core)['sp']
        y_peer = device(1 - y, x, core)['sp']
        self.sides = (core, x * first + y * core, y * first + x * core)
        self.peers = (device(y, x, first), {'sp': x_peer * first + y_peer * core}, {'sp': y_peer * first + x_peer * core})

    def own(self, tiles, level):
        return sum(self.sides[n] * (tiles // (2, 4, 8)[n]) for n in range(level + 1))

    def other(self, tiles, level):
        start = self.own(tiles, level - 1) if level else 0
        return start + (1 - self.sides[level]) * (tiles // (2, 4, 8)[level])

    def remote(self, level, src, dst, send, recv):
        return pltpu.make_async_remote_copy(src_ref=src, dst_ref=dst, send_sem=send, recv_sem=recv,
                                            device_id=self.peers[level], device_id_type=MESH)

    def arrive(self):
        for peer in self.peers:
            pl.semaphore_signal(pltpu.get_barrier_semaphore(), inc=1, device_id=peer, device_id_type=MESH)

    def meet(self):
        pl.semaphore_wait(pltpu.get_barrier_semaphore(), len(self.peers))


PART = (2, 4, 8)
LEVELS = 3
SIZE = (8, 16, 16, 8)
BASE = (0, 8, 24, 40)
CHUNKS = len(SIZE)


def span(k, level):
    return pl.ds(BASE[k] // PART[level], SIZE[k] // PART[level])


class Spread:
    COPIES = 6

    def __init__(self, here, ref, base, tiles, send, recv):
        n = tiles // 8
        _, a, b = here.sides
        own, near, far = base + (2 * a + b) * n, base + (2 * a + 1 - b) * n, base + 2 * (1 - a) * n
        self.spans = ((2, own, n), (1, own, n), (0, own, n), (1, near, n), (0, near, n), (0, far, 2 * n))
        self.here, self.ref, self.send, self.recv = here, ref, send, recv

    def copy(self, i):
        level, start, count = self.spans[i]
        where = self.ref.at[pl.ds(start, count)]
        return self.here.remote(level, where, where, self.send.at[i], self.recv.at[i])

    def start(self, *which):
        for i in which:
            self.copy(i).start()

    def wait(self, *which):
        for i in which:
            self.copy(i).wait()

    def step(self, n):
        if n == 3:
            self.start(0, 1, 2)
        elif n == 2:
            self.wait(0)
            self.start(3, 4)
        elif n == 1:
            self.wait(1, 3)
            self.start(5)
        else:
            self.wait(2, 4, 5)


U_SLOTS = 6
OWN = NH // 8
UP_STEPS = 12


def front_kernel(hid_hbm, gam_hbm, bet_hbm, pos_hbm, freq, w, w_up, qkv, act,
                 hid, gam, bet, pos, normed, qbuf, kvbuf, wbuf, cos, sin, insem, qsem, wsem, gsend, grecv):
    here = Place()
    inputs = [pltpu.make_async_copy(src, dst, insem.at[n]) for n, (src, dst) in enumerate(
        ((pos_hbm, pos), (hid_hbm, hid), (gam_hbm, gam), (bet_hbm, bet)))]
    for copy in inputs:
        copy.start()
    here.arrive()

    def part_of(k):
        return pl.ds(BASE[k] // 8 * HD, SIZE[k] // 8 * HD)

    def fetch_q(k):
        if k == CHUNKS:
            return pltpu.make_async_copy(w.at[:, pl.ds(NH * HD, 2 * HD)], kvbuf, qsem.at[k])
        col = pl.multiple_of((BASE[k] + here.own(SIZE[k], 2)) * HD, HD)
        return pltpu.make_async_copy(w.at[:, pl.ds(col, SIZE[k] // 8 * HD)], qbuf.at[:, part_of(k)], qsem.at[k])

    def fetch_up(step):
        slot = lax.rem(step, U_SLOTS)
        col = pl.multiple_of((step // 2) * 512, 512)
        row = pl.multiple_of(lax.rem(step, 2) * 3072, 3072)
        return pltpu.make_async_copy(w_up.at[pl.ds(row, 3072), pl.ds(col, 512)], wbuf.at[slot], wsem.at[slot])

    for k in range(CHUNKS + 1):
        fetch_q(k).start()

    inputs[0].wait()
    angle = jnp.transpose(jnp.broadcast_to(pos[...].astype(F32), (ROWS, HD))) * freq[...]
    cos[...] = jnp.cos(angle)
    lanes = lax.broadcasted_iota(jnp.int32, (ROWS, HD), 1)
    sine = jnp.sin(angle)
    sin[...] = jnp.where(lanes < HD // 2, -sine, sine)

    def norm_rows(i, carry):
        rows = pl.ds(pl.multiple_of(i * 16, 16), 16)
        v = hid[rows, :].astype(F32)
        mean = jnp.sum(v, axis=-1, keepdims=True) * (1.0 / D)
        cen = v - mean
        var = jnp.sum(cen * cen, axis=-1, keepdims=True) * (1.0 / D)
        normed[rows, :] = (cen * lax.rsqrt(var + LN_EPS) * gam[...] + bet[...]).astype(BF16)
        return carry

    for copy in inputs[1:]:
        copy.wait()
    for step in range(2):
        fetch_up(step).start()
    lax.fori_loop(0, ROWS // 16, norm_rows, 0, unroll=4)
    here.meet()

    def rotate(v):
        return (v * cos[...] + pltpu.roll(v, HD // 2, 1) * sin[...]).astype(BF16).astype(F32)

    def gather(level, k):
        base = BASE[k] + here.own(SIZE[k], 0)
        Spread(here, qkv, base, SIZE[k], gsend.at[k], grecv.at[k]).step(level)

    def project(weights):
        acc = jnp.dot(normed[...], weights[...], preferred_element_type=F32)
        return [acc[:, h:h + HD].astype(BF16).astype(F32) for h in range(0, acc.shape[1], HD)]

    def queries(chunks):
        for k in chunks:
            fetch_q(k).wait()
        first = BASE[chunks[0]] // 8
        heads = project(qbuf.at[:, pl.ds(first * HD, OWN // 2 * HD)])
        for k in chunks:
            for h in range(SIZE[k] // 8):
                qkv[BASE[k] + here.own(SIZE[k], 2) + h] = rotate(heads[BASE[k] // 8 - first + h])
            gather(3, k)

    def up_block(n, carry):
        fetch_up(2 * n).wait()
        s0 = lax.rem(2 * n, U_SLOTS)
        acc = jnp.dot(normed[:, :3072], wbuf[s0], preferred_element_type=F32)
        fetch_up(2 * n + 1).wait()
        acc += jnp.dot(normed[:, 3072:], wbuf[s0 + 1], preferred_element_type=F32)
        for half in range(2):
            nxt = 2 * n + half + U_SLOTS

            @pl.when(nxt < UP_STEPS)
            def _():
                fetch_up(nxt).start()

        act[:, pl.ds(pl.multiple_of(n * 512, 512), 512)] = (
            0.5 * acc * (1.0 + lax.erf(acc * (2.0 ** -0.5)))).astype(BF16)
        return carry

    def up(lo, hi):
        lax.fori_loop(lo, hi, up_block, 0)

    queries((0, 1))
    queries((2, 3))
    for step in range(2, U_SLOTS):
        fetch_up(step).start()
    fetch_q(CHUNKS).wait()
    k_new, v_new = project(kvbuf)
    qkv[NH] = rotate(k_new)
    qkv[NH + 1] = v_new
    gather(2, 0)
    gather(2, 1)
    up(0, 1)
    gather(2, 2)
    up(1, 2)
    gather(2, 3)
    gather(1, 0)
    up(2, 3)
    gather(0, 0)
    gather(1, 1)
    up(3, 4)
    gather(0, 1)
    up(4, 5)
    gather(1, 2)
    gather(1, 3)
    up(5, 6)
    gather(0, 2)
    gather(0, 3)


def front_call(hidden, gam, bet, pos, freq, w_qkv, w_up):
    vm = pl.BlockSpec(memory_space=pltpu.VMEM)
    hbm = pl.BlockSpec(memory_space=pltpu.HBM)
    dma = pltpu.SemaphoreType.DMA
    return pl.pallas_call(
        front_kernel,
        out_shape=(jax.ShapeDtypeStruct((NH + 2, ROWS, HD), F32), jax.ShapeDtypeStruct((ROWS, FF), BF16)),
        in_specs=[hbm, hbm, hbm, hbm, vm, hbm, hbm],
        out_specs=(vm, vm),
        scratch_shapes=[
            pltpu.VMEM((ROWS, D), BF16),
            pltpu.VMEM((1, D), F32),
            pltpu.VMEM((1, D), F32),
            pltpu.VMEM((1, ROWS), jnp.int32),
            pltpu.VMEM((ROWS, D), BF16),
            pltpu.VMEM((D, OWN * HD), BF16),
            pltpu.VMEM((D, 2 * HD), BF16),
            pltpu.VMEM((U_SLOTS, 3072, 512), BF16),
            pltpu.VMEM((ROWS, HD), F32),
            pltpu.VMEM((ROWS, HD), F32),
            dma((4,)), dma((CHUNKS + 1,)), dma((U_SLOTS,)), dma((CHUNKS, Spread.COPIES)), dma((CHUNKS, Spread.COPIES)),
        ],
        compiler_params=pltpu.CompilerParams(collective_id=0, has_side_effects=True, vmem_limit_bytes=FRONT_LIMIT),
        cost_estimate=pl.CostEstimate(flops=2 * ROWS * D * (FF + 1024), bytes_accessed=2 * D * (FF + 1024), transcendentals=0),
        name='front',
    )(hidden, gam, bet, pos, freq, w_qkv, w_up)


A_ROWS = 8
A_STEPS = ROWS // A_ROWS
A_SLOTS = 6
A_AHEAD = 3


def attn_kernel(pos_ref, qkv, kc, vc, o, ml, kn, vn, kbuf, vbuf, sbuf, ebuf, isem, osem):
    i = pl.program_id(0)
    origin = lax.axis_index('sp') * SEQ

    def fetch(step):
        slot = lax.rem(step, A_SLOTS)
        rows = pl.ds(step * A_ROWS, A_ROWS)
        return (pltpu.make_async_copy(kc.at[rows], kbuf.at[slot], isem.at[0, slot]),
                pltpu.make_async_copy(vc.at[rows], vbuf.at[slot], isem.at[1, slot]))

    def flush(step):
        slot = lax.rem(step, A_SLOTS)
        rows = pl.ds(step * A_ROWS, A_ROWS)
        return (pltpu.make_async_copy(kbuf.at[slot], kn.at[rows], osem.at[0, slot]),
                pltpu.make_async_copy(vbuf.at[slot], vn.at[rows], osem.at[1, slot]))

    @pl.when(i == 0)
    def _():
        for s in range(A_AHEAD):
            for c in fetch(s):
                c.start()

    @pl.when(i >= A_AHEAD)
    def _():
        for c in flush(i - A_AHEAD):
            c.wait()

    @pl.when(i + A_AHEAD < A_STEPS)
    def _():
        for c in fetch(i + A_AHEAD):
            c.start()

    for c in fetch(i):
        c.wait()
    slot = lax.rem(i, A_SLOTS)

    for r in range(A_ROWS):
        lp = pos_ref[i * A_ROWS + r] - origin
        base = pl.multiple_of((jnp.clip(lp, 0, SEQ - 1) // 16) * 16, 16)
        hit = base + lax.broadcasted_iota(jnp.int32, (16, HD), 0) == lp
        for buf, src in ((kbuf, NH), (vbuf, NH + 1)):
            new = jnp.broadcast_to(qkv[src, r:r + 1, :], (16, HD))
            old = buf[slot, r, pl.ds(base, 16), :].astype(F32)
            buf[slot, r, pl.ds(base, 16), :] = jnp.where(hit, new, old).astype(BF16)

    for r in range(A_ROWS):
        q = qkv[0:NH, r, :].astype(BF16)
        sbuf[r] = lax.dot_general(q, kbuf[slot, r], (((1,), (1,)), ((), ())), preferred_element_type=F32)
    lane = lax.broadcasted_iota(jnp.int32, (NH, HD), 1)
    mcol = jnp.zeros((NH, HD), F32)
    lcol = jnp.zeros((NH, HD), F32)
    for r in range(A_ROWS):
        valid = lax.broadcasted_iota(jnp.int32, (NH, SEQ), 1) <= pos_ref[i * A_ROWS + r] - origin
        s = jnp.where(valid, sbuf[r], -jnp.inf)
        m = jnp.max(s, axis=-1, keepdims=True)
        m = jnp.where(m == -jnp.inf, NEG_FILL, m)
        e = jnp.exp2((s - m) * SCALE2)
        l = jnp.sum(e, axis=-1, keepdims=True)
        ebuf[r] = e.astype(BF16)
        mcol = jnp.where(lane == r, m * SCALE2, mcol)
        lcol = jnp.where(lane == r, l, lcol)
    for r in range(A_ROWS):
        o[:, r, :] = jnp.dot(ebuf[r], vbuf[slot, r], preferred_element_type=F32)
    pad = jnp.zeros((16, HD), F32)
    ml[...] = jnp.transpose(jnp.concatenate([mcol, pad, lcol, pad], axis=0))[:A_ROWS]

    for c in flush(i):
        c.start()

    @pl.when(i == A_STEPS - 1)
    def _():
        for step in range(A_STEPS - A_AHEAD, A_STEPS):
            for c in flush(step):
                c.wait()


def attn_call(positions, qkv, k_cache, v_cache):
    anyspace = pl.BlockSpec(memory_space=pl.ANY)
    cache = jax.ShapeDtypeStruct((ROWS, SEQ, HD), BF16)
    return pl.pallas_call(
        attn_kernel,
        out_shape=(jax.ShapeDtypeStruct((NH, ROWS, HD), F32), jax.ShapeDtypeStruct((ROWS, HD), F32), cache, cache),
        grid_spec=pltpu.PrefetchScalarGridSpec(
            num_scalar_prefetch=1,
            grid=(A_STEPS,),
            in_specs=[pl.BlockSpec((NH + 2, A_ROWS, HD), lambda i, p: (0, i, 0)), anyspace, anyspace],
            out_specs=(pl.BlockSpec((NH, A_ROWS, HD), lambda i, p: (0, i, 0)), pl.BlockSpec((A_ROWS, HD), lambda i, p: (i, 0)),
                       anyspace, anyspace),
            scratch_shapes=[
                pltpu.VMEM((A_SLOTS, A_ROWS, SEQ, HD), BF16),
                pltpu.VMEM((A_SLOTS, A_ROWS, SEQ, HD), BF16),
                pltpu.VMEM((A_ROWS, NH, SEQ), F32),
                pltpu.VMEM((A_ROWS, NH, SEQ), BF16),
                pltpu.SemaphoreType.DMA((2, A_SLOTS)),
                pltpu.SemaphoreType.DMA((2, A_SLOTS)),
            ]),
        compiler_params=pltpu.CompilerParams(vmem_limit_bytes=ATTN_LIMIT, dimension_semantics=('arbitrary',)),
        cost_estimate=pl.CostEstimate(flops=4 * ROWS * NH * SEQ * HD, bytes_accessed=8 * ROWS * SEQ * HD, transcendentals=0),
        name='attn',
    )(positions, qkv, k_cache, v_cache)


W_SLOTS = 5
DOWN_STEPS = 12
F_CHUNKS = 6
HALF = NH // 2
ORDER = ((0, 0), (1, 0), (2, 0), (3, 0), (4, 0), (5, 0), (0, 2), (1, 2), (2, 2), (0, 3), (3, 2), (1, 3),
         (2, 3), (4, 2), (0, 4), (5, 2), (3, 3), (1, 4), (2, 4), (4, 3), (0, 5), (5, 3), (0, 6), (3, 4),
         (1, 5), (4, 4), (1, 6), (5, 4), (2, 5), (3, 5), (2, 6), (4, 5), (3, 6), (4, 6), (5, 5), (5, 6))


def tail_kernel(act, ml_in, o_in, hid, w_down, w_out, out,
                wbuf, wobuf, part, mine, orecv0, orecv1, orecv2, stats, mlr, wts,
                precv0, precv1, precv2, gath, ctxf, ctx,
                wsem, wosem, osend, orecv, msend, mrecv, csend, crecv, psend, precv, gsend, grecv):
    here = Place()
    own, other = here.own, here.other

    def fetch_down(step):
        slot = lax.rem(step, W_SLOTS)
        col = pl.multiple_of((lax.rem(step, 2) * F_CHUNKS + step // 2) * 512, 512)
        return pltpu.make_async_copy(w_down.at[:, pl.ds(col, 512)], wbuf.at[slot], wsem.at[slot])

    def head_at(core, k):
        turn = (here.x, here.y) if core == 0 else (here.y, here.x)
        return BASE[k] + core * (SIZE[k] // 2) + turn[0] * (SIZE[k] // 4) + turn[1] * (SIZE[k] // 8)

    def wo_copy(core, k):
        rows = pl.ds(pl.multiple_of(head_at(core, k) * HD, HD), SIZE[k] // 8 * HD)
        cols = pl.ds(pl.multiple_of(here.sides[0] * (HALF * HD), HALF * HD), HALF * HD)
        dst = wobuf.at[pl.ds((core * OWN + BASE[k] // 8) * HD, SIZE[k] // 8 * HD)]
        return pltpu.make_async_copy(w_out.at[rows, cols], dst, wosem.at[core, k])

    o_to = (orecv0, orecv1, orecv2)

    def mine_at(k, start):
        return BASE[k] // 2 + start - own(SIZE[k], 0)

    def o_send(level, k):
        start, count = other(SIZE[k], level), SIZE[k] // PART[level]
        src = mine.at[pl.ds(mine_at(k, start), count)] if level else o_in.at[pl.ds(BASE[k] + start, count)]
        return here.remote(level, src, o_to[level].at[span(k, level)], osend.at[level, k], orecv.at[level, k])

    def m_send(level):
        src = ml_in if level == 0 else stats.at[level - 1]
        return here.remote(level, src, mlr.at[level], msend.at[level], mrecv.at[level])

    lanes = lax.broadcasted_iota(jnp.int32, (ROWS, HD), 1)

    def merge_stats(level):
        m_send(level).wait()
        ours = ml_in[...] if level == 0 else stats[level - 1]
        theirs = mlr[level]
        top = jnp.maximum(ours, theirs)
        w1 = jnp.exp2(ours - top)
        w2 = jnp.exp2(theirs - top)
        total = ours * pltpu.roll(w1, 64, 1) + theirs * pltpu.roll(w2, 64, 1)
        wts[level, 0] = w1
        wts[level, 1] = w2
        stats[level] = jnp.where(lanes < 64, top, total)
        if level < 2:
            m_send(level + 1).start()

    def shift(v, by):
        return pltpu.roll(v, lax.rem(HD - by, HD), 1)

    def c_send(k):
        where = ctxf.at[pl.ds(here.sides[0] * OWN + BASE[k] // 8, SIZE[k] // 8)]
        return here.remote(0, where, where, csend.at[k], crecv.at[k])

    def merge_heads(level, k):
        o_send(level, k).wait()
        start = own(SIZE[k], level)
        w1 = shift(wts[level, 0], BASE[k] + start)
        w2 = shift(wts[level, 1], BASE[k] + start)
        base = mine_at(k, start)
        for h in range(SIZE[k] // PART[level]):
            ours = mine[base + h] if level else o_in[BASE[k] + start + h]
            mine[base + h] = ours * w1[:, h:h + 1] + o_to[level][BASE[k] // PART[level] + h] * w2[:, h:h + 1]
        if level < 2:
            o_send(level + 1, k).start()
        else:
            l = shift(stats[2], BASE[k] + start)
            for h in range(SIZE[k] // 8):
                value = (mine[base + h] / l[:, 64 + h:65 + h]).astype(BF16)
                ctxf[here.sides[0] * OWN + BASE[k] // 8 + h] = value.astype(F32)
            c_send(k).start()

    def d_send(k):
        src = part.at[pl.ds((1 - here.sides[0]) * HALF + 4 * k, 4)]
        return here.remote(0, src, precv0.at[pl.ds(4 * k, 4)], psend.at[0, k], precv.at[0, k])

    def down_pair(k, carry):
        for side in range(2):
            n = 2 * k + side
            fetch_down(n).wait()
            acc = jnp.dot(act[...], wbuf[lax.rem(n, W_SLOTS)], preferred_element_type=F32)

            @pl.when(n + W_SLOTS < DOWN_STEPS)
            def _():
                fetch_down(n + W_SLOTS).start()

            for t in range(4):
                part[side * HALF + 4 * k + t] = acc[:, t * HD:(t + 1) * HD]
        d_send(k).start()
        return carry

    def down(lo, hi):
        lax.fori_loop(lo, hi, down_pair, 0)

    p_to = (precv0, precv1, precv2)

    def tile(k, level):
        return here.sides[0] * HALF + 4 * k + own(8, level) - own(8, 0)

    def p_send(level, k):
        count = 8 // PART[level]
        src = part.at[pl.ds(here.sides[0] * HALF + 4 * k + other(8, level) - own(8, 0), count)]
        return here.remote(level, src, p_to[level].at[pl.ds(k * count, count)], psend.at[level, k], precv.at[level, k])

    def project(k):
        d_send(k).wait()
        acc = jnp.dot(ctx[...], wobuf[:, k * 512:(k + 1) * 512], preferred_element_type=F32)
        for t in range(4):
            part[tile(k, 0) + t] = (part[tile(k, 0) + t] + precv0[4 * k + t]) + acc[:, t * HD:(t + 1) * HD]
        p_send(1, k).start()

    def reduce(level, k):
        p_send(level, k).wait()
        base, count = tile(k, level), 8 // PART[level]
        if level < 2:
            part[pl.ds(base, count)] = part[pl.ds(base, count)] + p_to[level][pl.ds(k * count, count)]
            p_send(level + 1, k).start()
        else:
            col = pl.multiple_of(base * HD, HD)
            total = hid[:, pl.ds(col, HD)].astype(F32) + (part[base] + precv2[k])
            gath[base] = total.astype(BF16).astype(F32)
            spread(k).step(3)

    def spread(k):
        return Spread(here, gath, tile(k, 0), 8, gsend.at[k], grecv.at[k])

    def gather(level, k):
        spread(k).step(level)
        if level == 0:
            for t in range(4 * k, 4 * k + 4):
                for col in (t, HALF + t):
                    out[:, col * HD:(col + 1) * HD] = gath[col].astype(BF16)

    here.arrive()
    for s in range(4):
        fetch_down(s).start()
    here.meet()
    m_send(0).start()
    for k in range(CHUNKS):
        o_send(0, k).start()
    merge_stats(0)
    for k in range(CHUNKS):
        merge_heads(0, k)
    for s in range(4, W_SLOTS):
        fetch_down(s).start()
    down(0, 1)
    merge_stats(1)
    merge_heads(1, 0)
    down(1, 3)
    for core in range(2):
        for k in range(CHUNKS):
            wo_copy(core, k).start()
    merge_heads(1, 1)
    merge_stats(2)
    merge_heads(2, 0)
    down(3, 4)
    merge_heads(1, 2)
    down(4, 5)
    merge_heads(1, 3)
    merge_heads(2, 1)
    merge_heads(2, 2)
    down(5, 6)
    for core in range(2):
        for k in range(CHUNKS):
            wo_copy(core, k).wait()
    merge_heads(2, 3)
    for k in range(CHUNKS):
        c_send(k).wait()
    for h in range(2 * OWN):
        ctx[:, h * HD:(h + 1) * HD] = ctxf[h].astype(BF16)
    for k, stage in ORDER:
        if stage == 0:
            project(k)
        elif stage <= 3:
            reduce(stage - 1, k)
        else:
            gather(6 - stage, k)


def tail_call(act, ml, o, hidden, w_down, w_out):
    vm = pl.BlockSpec(memory_space=pltpu.VMEM)
    anyspace = pl.BlockSpec(memory_space=pl.ANY)
    dma = pltpu.SemaphoreType.DMA
    return pl.pallas_call(
        tail_kernel,
        out_shape=jax.ShapeDtypeStruct((ROWS, D), BF16),
        in_specs=[vm, vm, vm, vm, anyspace, anyspace],
        out_specs=vm,
        scratch_shapes=[
            pltpu.VMEM((W_SLOTS, 3072, 512), BF16),
            pltpu.VMEM((2 * OWN * HD, HALF * HD), BF16),
            pltpu.VMEM((NH, ROWS, HD), F32),
            pltpu.VMEM((NH // 2, ROWS, HD), F32),
            pltpu.VMEM((NH // 2, ROWS, HD), F32),
            pltpu.VMEM((NH // 4, ROWS, HD), F32),
            pltpu.VMEM((NH // 8, ROWS, HD), F32),
            pltpu.VMEM((LEVELS, ROWS, HD), F32),
            pltpu.VMEM((LEVELS, ROWS, HD), F32),
            pltpu.VMEM((LEVELS, 2, ROWS, HD), F32),
            pltpu.VMEM((NH // 2, ROWS, HD), F32),
            pltpu.VMEM((NH // 4, ROWS, HD), F32),
            pltpu.VMEM((NH // 8, ROWS, HD), F32),
            pltpu.VMEM((NH, ROWS, HD), F32),
            pltpu.VMEM((2 * OWN, ROWS, HD), F32),
            pltpu.VMEM((ROWS, 2 * OWN * HD), BF16),
            dma((W_SLOTS,)), dma((2, CHUNKS)),
            dma((LEVELS, CHUNKS)), dma((LEVELS, CHUNKS)), dma((LEVELS,)), dma((LEVELS,)), dma((CHUNKS,)), dma((CHUNKS,)),
            dma((LEVELS, F_CHUNKS)), dma((LEVELS, F_CHUNKS)), dma((F_CHUNKS, Spread.COPIES)), dma((F_CHUNKS, Spread.COPIES)),
        ],
        compiler_params=pltpu.CompilerParams(collective_id=1, has_side_effects=True, vmem_limit_bytes=TAIL_LIMIT),
        cost_estimate=pl.CostEstimate(flops=2 * ROWS * D * FF, bytes_accessed=2 * D * FF, transcendentals=0),
        name='tail',
    )(act, ml, o, hidden, w_down, w_out)


def device_step(hidden, ln_gamma, ln_beta, w_qkv, w_out, w_up, w_down, k_cache, v_cache, positions):
    inv_freq = 1.0 / (ROPE_BASE ** (jnp.arange(0, HD, 2, dtype=F32) / HD))
    freq = jnp.concatenate([inv_freq, inv_freq])[None, :]
    inputs = [pltpu.with_memory_space_constraint(v, pltpu.HBM)
              for v in (hidden, ln_gamma[None, :], ln_beta[None, :], positions[None, :])]
    qkv, act = front_call(*inputs, freq, w_qkv, w_up)
    o, ml, k_next, v_next = attn_call(positions, qkv, k_cache, v_cache)
    out = tail_call(act, ml, o, hidden, w_down, w_out)
    return out, k_next, v_next


def solution(mesh):
    cache_spec = P('dp', 'sp', None)
    in_specs = (P('dp', None), P(None), P(None), P(None, None), P(None, None), P(None, 'sp'), P('sp', None), cache_spec, cache_spec, P('dp'))
    out_specs = (P('dp', None), cache_spec, cache_spec)
    return jax.shard_map(device_step, mesh=mesh, in_specs=in_specs, out_specs=out_specs, check_vma=False)
```

```python
import functools

import jax
import jax.numpy as jnp
from jax import lax
from jax.experimental import pallas as pl
from jax.experimental.pallas import tpu as pltpu
from jax.sharding import PartitionSpec as P

LN_EPS = 1e-5
ROPE_BASE = 10000.0
NEG_FILL = -1e30
SCALE2 = 128 ** -0.5 * 1.4426950408889634
MESH = pl.DeviceIdType.MESH
FRONT_LIMIT = 46_000_000
ATTN_LIMIT = 40_000_000
TAIL_LIMIT = 47_000_000

ROWS = 128
D = 6144
HD = 128
NH = 48
SEQ = 512
FF = 3072
F32 = jnp.float32
BF16 = jnp.bfloat16


def device(y, x, core):
    return {'sp': (y * 2 + x) * 2 + core}


class Place:
    def __init__(self):
        sp = lax.axis_index('sp')
        core = lax.rem(sp, 2)
        x = lax.rem(sp // 2, 2)
        y = sp // 4
        self.x, self.y = x, y
        first = 1 - core
        x_peer = device(y, 1 - x, core)['sp']
        y_peer = device(1 - y, x, core)['sp']
        self.sides = (core, x * first + y * core, y * first + x * core)
        self.peers = (device(y, x, first), {'sp': x_peer * first + y_peer * core}, {'sp': y_peer * first + x_peer * core})

    def own(self, tiles, level):
        return sum(self.sides[n] * (tiles // (2, 4, 8)[n]) for n in range(level + 1))

    def other(self, tiles, level):
        start = self.own(tiles, level - 1) if level else 0
        return start + (1 - self.sides[level]) * (tiles // (2, 4, 8)[level])

    def remote(self, level, src, dst, send, recv):
        return pltpu.make_async_remote_copy(src_ref=src, dst_ref=dst, send_sem=send, recv_sem=recv,
                                            device_id=self.peers[level], device_id_type=MESH)

    def arrive(self):
        for peer in self.peers:
            pl.semaphore_signal(pltpu.get_barrier_semaphore(), inc=1, device_id=peer, device_id_type=MESH)

    def meet(self):
        pl.semaphore_wait(pltpu.get_barrier_semaphore(), len(self.peers))


PART = (2, 4, 8)
LEVELS = 3
SIZE = (8, 16, 16, 8)
BASE = (0, 8, 24, 40)
CHUNKS = len(SIZE)


def span(k, level):
    return pl.ds(BASE[k] // PART[level], SIZE[k] // PART[level])


U_SLOTS = 6
OWN = NH // 8
UP_STEPS = 12


def front_kernel(hid_hbm, gam_hbm, bet_hbm, pos_hbm, freq, w, w_up, qkv, act,
                 hid, gam, bet, pos, normed, qbuf, kvbuf, wbuf, cos, sin, insem, qsem, wsem, gsend, grecv):
    here = Place()
    inputs = [pltpu.make_async_copy(src, dst, insem.at[n]) for n, (src, dst) in enumerate(
        ((pos_hbm, pos), (hid_hbm, hid), (gam_hbm, gam), (bet_hbm, bet)))]
    for copy in inputs:
        copy.start()
    here.arrive()

    def part_of(k):
        return pl.ds(BASE[k] // 8 * HD, SIZE[k] // 8 * HD)

    def fetch_q(k):
        if k == CHUNKS:
            return pltpu.make_async_copy(w.at[:, pl.ds(NH * HD, 2 * HD)], kvbuf, qsem.at[k])
        col = pl.multiple_of((BASE[k] + here.own(SIZE[k], 2)) * HD, HD)
        return pltpu.make_async_copy(w.at[:, pl.ds(col, SIZE[k] // 8 * HD)], qbuf.at[:, part_of(k)], qsem.at[k])

    def fetch_up(step):
        slot = lax.rem(step, U_SLOTS)
        col = pl.multiple_of((step // 2) * 512, 512)
        row = pl.multiple_of(lax.rem(step, 2) * 3072, 3072)
        return pltpu.make_async_copy(w_up.at[pl.ds(row, 3072), pl.ds(col, 512)], wbuf.at[slot], wsem.at[slot])

    for k in range(CHUNKS + 1):
        fetch_q(k).start()

    inputs[0].wait()
    angle = jnp.transpose(jnp.broadcast_to(pos[...].astype(F32), (ROWS, HD))) * freq[...]
    cos[...] = jnp.cos(angle)
    lanes = lax.broadcasted_iota(jnp.int32, (ROWS, HD), 1)
    sine = jnp.sin(angle)
    sin[...] = jnp.where(lanes < HD // 2, -sine, sine)

    def norm_rows(i, carry):
        rows = pl.ds(pl.multiple_of(i * 16, 16), 16)
        v = hid[rows, :].astype(F32)
        mean = jnp.sum(v, axis=-1, keepdims=True) * (1.0 / D)
        cen = v - mean
        var = jnp.sum(cen * cen, axis=-1, keepdims=True) * (1.0 / D)
        normed[rows, :] = (cen * lax.rsqrt(var + LN_EPS) * gam[...] + bet[...]).astype(BF16)
        return carry

    for copy in inputs[1:]:
        copy.wait()
    for step in range(2):
        fetch_up(step).start()
    lax.fori_loop(0, ROWS // 16, norm_rows, 0, unroll=4)
    here.meet()

    def rotate(v):
        return (v * cos[...] + pltpu.roll(v, HD // 2, 1) * sin[...]).astype(BF16).astype(F32)

    def g_send(level, k):
        where = qkv.at[pl.ds(BASE[k] + here.own(SIZE[k], level), SIZE[k] // PART[level])]
        return here.remote(level, where, where, gsend.at[level, k], grecv.at[level, k])

    def project(weights):
        acc = jnp.dot(normed[...], weights[...], preferred_element_type=F32)
        return [acc[:, h:h + HD].astype(BF16).astype(F32) for h in range(0, acc.shape[1], HD)]

    def queries(chunks):
        for k in chunks:
            fetch_q(k).wait()
        first = BASE[chunks[0]] // 8
        heads = project(qbuf.at[:, pl.ds(first * HD, OWN // 2 * HD)])
        for k in chunks:
            for h in range(SIZE[k] // 8):
                qkv[BASE[k] + here.own(SIZE[k], 2) + h] = rotate(heads[BASE[k] // 8 - first + h])
            g_send(2, k).start()

    def gather(level, k):
        g_send(level, k).wait()
        if level:
            g_send(level - 1, k).start()

    def up_block(n, carry):
        fetch_up(2 * n).wait()
        s0 = lax.rem(2 * n, U_SLOTS)
        acc = jnp.dot(normed[:, :3072], wbuf[s0], preferred_element_type=F32)
        fetch_up(2 * n + 1).wait()
        acc += jnp.dot(normed[:, 3072:], wbuf[s0 + 1], preferred_element_type=F32)
        for half in range(2):
            nxt = 2 * n + half + U_SLOTS

            @pl.when(nxt < UP_STEPS)
            def _():
                fetch_up(nxt).start()

        act[:, pl.ds(pl.multiple_of(n * 512, 512), 512)] = (
            0.5 * acc * (1.0 + lax.erf(acc * (2.0 ** -0.5)))).astype(BF16)
        return carry

    def up(lo, hi):
        lax.fori_loop(lo, hi, up_block, 0)

    queries((0, 1))
    queries((2, 3))
    for step in range(2, U_SLOTS):
        fetch_up(step).start()
    fetch_q(CHUNKS).wait()
    k_new, v_new = project(kvbuf)
    qkv[NH] = rotate(k_new)
    qkv[NH + 1] = v_new
    gather(2, 0)
    gather(2, 1)
    up(0, 1)
    gather(2, 2)
    up(1, 2)
    gather(2, 3)
    gather(1, 0)
    up(2, 3)
    gather(0, 0)
    gather(1, 1)
    up(3, 4)
    gather(0, 1)
    up(4, 5)
    gather(1, 2)
    gather(1, 3)
    up(5, 6)
    gather(0, 2)
    gather(0, 3)


def front_call(hidden, gam, bet, pos, freq, w_qkv, w_up):
    vm = pl.BlockSpec(memory_space=pltpu.VMEM)
    hbm = pl.BlockSpec(memory_space=pltpu.HBM)
    dma = pltpu.SemaphoreType.DMA
    return pl.pallas_call(
        front_kernel,
        out_shape=(jax.ShapeDtypeStruct((NH + 2, ROWS, HD), F32), jax.ShapeDtypeStruct((ROWS, FF), BF16)),
        in_specs=[hbm, hbm, hbm, hbm, vm, hbm, hbm],
        out_specs=(vm, vm),
        scratch_shapes=[
            pltpu.VMEM((ROWS, D), BF16),
            pltpu.VMEM((1, D), F32),
            pltpu.VMEM((1, D), F32),
            pltpu.VMEM((1, ROWS), jnp.int32),
            pltpu.VMEM((ROWS, D), BF16),
            pltpu.VMEM((D, OWN * HD), BF16),
            pltpu.VMEM((D, 2 * HD), BF16),
            pltpu.VMEM((U_SLOTS, 3072, 512), BF16),
            pltpu.VMEM((ROWS, HD), F32),
            pltpu.VMEM((ROWS, HD), F32),
            dma((4,)), dma((CHUNKS + 1,)), dma((U_SLOTS,)), dma((LEVELS, CHUNKS)), dma((LEVELS, CHUNKS)),
        ],
        compiler_params=pltpu.CompilerParams(collective_id=0, has_side_effects=True, vmem_limit_bytes=FRONT_LIMIT),
        cost_estimate=pl.CostEstimate(flops=2 * ROWS * D * (FF + 1024), bytes_accessed=2 * D * (FF + 1024), transcendentals=0),
        name='front',
    )(hidden, gam, bet, pos, freq, w_qkv, w_up)


A_ROWS = 8
A_STEPS = ROWS // A_ROWS
A_SLOTS = 6
A_AHEAD = 3


def attn_kernel(pos_ref, qkv, kc, vc, o, ml, kn, vn, kbuf, vbuf, sbuf, ebuf, isem, osem):
    i = pl.program_id(0)
    origin = lax.axis_index('sp') * SEQ

    def fetch(step):
        slot = lax.rem(step, A_SLOTS)
        rows = pl.ds(step * A_ROWS, A_ROWS)
        return (pltpu.make_async_copy(kc.at[rows], kbuf.at[slot], isem.at[0, slot]),
                pltpu.make_async_copy(vc.at[rows], vbuf.at[slot], isem.at[1, slot]))

    def flush(step):
        slot = lax.rem(step, A_SLOTS)
        rows = pl.ds(step * A_ROWS, A_ROWS)
        return (pltpu.make_async_copy(kbuf.at[slot], kn.at[rows], osem.at[0, slot]),
                pltpu.make_async_copy(vbuf.at[slot], vn.at[rows], osem.at[1, slot]))

    @pl.when(i == 0)
    def _():
        for s in range(A_AHEAD):
            for c in fetch(s):
                c.start()

    @pl.when(i >= A_AHEAD)
    def _():
        for c in flush(i - A_AHEAD):
            c.wait()

    @pl.when(i + A_AHEAD < A_STEPS)
    def _():
        for c in fetch(i + A_AHEAD):
            c.start()

    for c in fetch(i):
        c.wait()
    slot = lax.rem(i, A_SLOTS)

    for r in range(A_ROWS):
        lp = pos_ref[i * A_ROWS + r] - origin
        base = pl.multiple_of((jnp.clip(lp, 0, SEQ - 1) // 16) * 16, 16)
        hit = base + lax.broadcasted_iota(jnp.int32, (16, HD), 0) == lp
        for buf, src in ((kbuf, NH), (vbuf, NH + 1)):
            new = jnp.broadcast_to(qkv[src, r:r + 1, :], (16, HD))
            old = buf[slot, r, pl.ds(base, 16), :].astype(F32)
            buf[slot, r, pl.ds(base, 16), :] = jnp.where(hit, new, old).astype(BF16)

    for r in range(A_ROWS):
        q = qkv[0:NH, r, :].astype(BF16)
        sbuf[r] = lax.dot_general(q, kbuf[slot, r], (((1,), (1,)), ((), ())), preferred_element_type=F32)
    lane = lax.broadcasted_iota(jnp.int32, (NH, HD), 1)
    mcol = jnp.zeros((NH, HD), F32)
    lcol = jnp.zeros((NH, HD), F32)
    for r in range(A_ROWS):
        valid = lax.broadcasted_iota(jnp.int32, (NH, SEQ), 1) <= pos_ref[i * A_ROWS + r] - origin
        s = jnp.where(valid, sbuf[r], -jnp.inf)
        m = jnp.max(s, axis=-1, keepdims=True)
        m = jnp.where(m == -jnp.inf, NEG_FILL, m)
        e = jnp.exp2((s - m) * SCALE2)
        l = jnp.sum(e, axis=-1, keepdims=True)
        ebuf[r] = e.astype(BF16)
        mcol = jnp.where(lane == r, m * SCALE2, mcol)
        lcol = jnp.where(lane == r, l, lcol)
    for r in range(A_ROWS):
        o[:, r, :] = jnp.dot(ebuf[r], vbuf[slot, r], preferred_element_type=F32)
    pad = jnp.zeros((16, HD), F32)
    ml[...] = jnp.transpose(jnp.concatenate([mcol, pad, lcol, pad], axis=0))[:A_ROWS]

    for c in flush(i):
        c.start()

    @pl.when(i == A_STEPS - 1)
    def _():
        for step in range(A_STEPS - A_AHEAD, A_STEPS):
            for c in flush(step):
                c.wait()


def attn_call(positions, qkv, k_cache, v_cache):
    anyspace = pl.BlockSpec(memory_space=pl.ANY)
    cache = jax.ShapeDtypeStruct((ROWS, SEQ, HD), BF16)
    return pl.pallas_call(
        attn_kernel,
        out_shape=(jax.ShapeDtypeStruct((NH, ROWS, HD), F32), jax.ShapeDtypeStruct((ROWS, HD), F32), cache, cache),
        grid_spec=pltpu.PrefetchScalarGridSpec(
            num_scalar_prefetch=1,
            grid=(A_STEPS,),
            in_specs=[pl.BlockSpec((NH + 2, A_ROWS, HD), lambda i, p: (0, i, 0)), anyspace, anyspace],
            out_specs=(pl.BlockSpec((NH, A_ROWS, HD), lambda i, p: (0, i, 0)), pl.BlockSpec((A_ROWS, HD), lambda i, p: (i, 0)),
                       anyspace, anyspace),
            scratch_shapes=[
                pltpu.VMEM((A_SLOTS, A_ROWS, SEQ, HD), BF16),
                pltpu.VMEM((A_SLOTS, A_ROWS, SEQ, HD), BF16),
                pltpu.VMEM((A_ROWS, NH, SEQ), F32),
                pltpu.VMEM((A_ROWS, NH, SEQ), BF16),
                pltpu.SemaphoreType.DMA((2, A_SLOTS)),
                pltpu.SemaphoreType.DMA((2, A_SLOTS)),
            ]),
        compiler_params=pltpu.CompilerParams(vmem_limit_bytes=ATTN_LIMIT, dimension_semantics=('arbitrary',)),
        cost_estimate=pl.CostEstimate(flops=4 * ROWS * NH * SEQ * HD, bytes_accessed=8 * ROWS * SEQ * HD, transcendentals=0),
        name='attn',
    )(positions, qkv, k_cache, v_cache)


W_SLOTS = 5
DOWN_STEPS = 12
F_CHUNKS = 6
HALF = NH // 2
ORDER = ((0, 0), (1, 0), (2, 0), (3, 0), (4, 0), (5, 0), (0, 2), (1, 2), (2, 2), (0, 3), (3, 2), (1, 3),
         (2, 3), (4, 2), (0, 4), (5, 2), (3, 3), (1, 4), (2, 4), (4, 3), (0, 5), (5, 3), (0, 6), (3, 4),
         (1, 5), (4, 4), (1, 6), (5, 4), (2, 5), (3, 5), (2, 6), (4, 5), (3, 6), (4, 6), (5, 5), (5, 6))


def tail_kernel(act, ml_in, o_in, hid, w_down, w_out, out,
                wbuf, wobuf, part, mine, orecv0, orecv1, orecv2, stats, mlr, wts,
                precv0, precv1, precv2, gath, ctxf, ctx,
                wsem, wosem, osend, orecv, msend, mrecv, csend, crecv, psend, precv, gsend, grecv):
    here = Place()
    own, other = here.own, here.other

    def fetch_down(step):
        slot = lax.rem(step, W_SLOTS)
        col = pl.multiple_of((lax.rem(step, 2) * F_CHUNKS + step // 2) * 512, 512)
        return pltpu.make_async_copy(w_down.at[:, pl.ds(col, 512)], wbuf.at[slot], wsem.at[slot])

    def head_at(core, k):
        turn = (here.x, here.y) if core == 0 else (here.y, here.x)
        return BASE[k] + core * (SIZE[k] // 2) + turn[0] * (SIZE[k] // 4) + turn[1] * (SIZE[k] // 8)

    def wo_copy(core, k):
        rows = pl.ds(pl.multiple_of(head_at(core, k) * HD, HD), SIZE[k] // 8 * HD)
        cols = pl.ds(pl.multiple_of(here.sides[0] * (HALF * HD), HALF * HD), HALF * HD)
        dst = wobuf.at[pl.ds((core * OWN + BASE[k] // 8) * HD, SIZE[k] // 8 * HD)]
        return pltpu.make_async_copy(w_out.at[rows, cols], dst, wosem.at[core, k])

    o_to = (orecv0, orecv1, orecv2)

    def mine_at(k, start):
        return BASE[k] // 2 + start - own(SIZE[k], 0)

    def o_send(level, k):
        start, count = other(SIZE[k], level), SIZE[k] // PART[level]
        src = mine.at[pl.ds(mine_at(k, start), count)] if level else o_in.at[pl.ds(BASE[k] + start, count)]
        return here.remote(level, src, o_to[level].at[span(k, level)], osend.at[level, k], orecv.at[level, k])

    def m_send(level):
        src = ml_in if level == 0 else stats.at[level - 1]
        return here.remote(level, src, mlr.at[level], msend.at[level], mrecv.at[level])

    lanes = lax.broadcasted_iota(jnp.int32, (ROWS, HD), 1)

    def merge_stats(level):
        m_send(level).wait()
        ours = ml_in[...] if level == 0 else stats[level - 1]
        theirs = mlr[level]
        top = jnp.maximum(ours, theirs)
        w1 = jnp.exp2(ours - top)
        w2 = jnp.exp2(theirs - top)
        total = ours * pltpu.roll(w1, 64, 1) + theirs * pltpu.roll(w2, 64, 1)
        wts[level, 0] = w1
        wts[level, 1] = w2
        stats[level] = jnp.where(lanes < 64, top, total)
        if level < 2:
            m_send(level + 1).start()

    def shift(v, by):
        return pltpu.roll(v, lax.rem(HD - by, HD), 1)

    def c_send(k):
        where = ctxf.at[pl.ds(here.sides[0] * OWN + BASE[k] // 8, SIZE[k] // 8)]
        return here.remote(0, where, where, csend.at[k], crecv.at[k])

    def merge_heads(level, k):
        o_send(level, k).wait()
        start = own(SIZE[k], level)
        w1 = shift(wts[level, 0], BASE[k] + start)
        w2 = shift(wts[level, 1], BASE[k] + start)
        base = mine_at(k, start)
        for h in range(SIZE[k] // PART[level]):
            ours = mine[base + h] if level else o_in[BASE[k] + start + h]
            mine[base + h] = ours * w1[:, h:h + 1] + o_to[level][BASE[k] // PART[level] + h] * w2[:, h:h + 1]
        if level < 2:
            o_send(level + 1, k).start()
        else:
            l = shift(stats[2], BASE[k] + start)
            for h in range(SIZE[k] // 8):
                value = (mine[base + h] / l[:, 64 + h:65 + h]).astype(BF16)
                ctxf[here.sides[0] * OWN + BASE[k] // 8 + h] = value.astype(F32)
            c_send(k).start()

    def d_send(k):
        src = part.at[pl.ds((1 - here.sides[0]) * HALF + 4 * k, 4)]
        return here.remote(0, src, precv0.at[pl.ds(4 * k, 4)], psend.at[0, k], precv.at[0, k])

    def down_pair(k, carry):
        for side in range(2):
            n = 2 * k + side
            fetch_down(n).wait()
            acc = jnp.dot(act[...], wbuf[lax.rem(n, W_SLOTS)], preferred_element_type=F32)

            @pl.when(n + W_SLOTS < DOWN_STEPS)
            def _():
                fetch_down(n + W_SLOTS).start()

            for t in range(4):
                part[side * HALF + 4 * k + t] = acc[:, t * HD:(t + 1) * HD]
        d_send(k).start()
        return carry

    def down(lo, hi):
        lax.fori_loop(lo, hi, down_pair, 0)

    p_to = (precv0, precv1, precv2)

    def tile(k, level):
        return here.sides[0] * HALF + 4 * k + own(8, level) - own(8, 0)

    def p_send(level, k):
        count = 8 // PART[level]
        src = part.at[pl.ds(here.sides[0] * HALF + 4 * k + other(8, level) - own(8, 0), count)]
        return here.remote(level, src, p_to[level].at[pl.ds(k * count, count)], psend.at[level, k], precv.at[level, k])

    def g_send(level, k):
        where = gath.at[pl.ds(tile(k, level), 8 // PART[level])]
        return here.remote(level, where, where, gsend.at[level, k], grecv.at[level, k])

    def project(k):
        d_send(k).wait()
        acc = jnp.dot(ctx[...], wobuf[:, k * 512:(k + 1) * 512], preferred_element_type=F32)
        for t in range(4):
            part[tile(k, 0) + t] = (part[tile(k, 0) + t] + precv0[4 * k + t]) + acc[:, t * HD:(t + 1) * HD]
        p_send(1, k).start()

    def reduce(level, k):
        p_send(level, k).wait()
        base, count = tile(k, level), 8 // PART[level]
        if level < 2:
            part[pl.ds(base, count)] = part[pl.ds(base, count)] + p_to[level][pl.ds(k * count, count)]
            p_send(level + 1, k).start()
        else:
            col = pl.multiple_of(base * HD, HD)
            total = hid[:, pl.ds(col, HD)].astype(F32) + (part[base] + precv2[k])
            gath[base] = total.astype(BF16).astype(F32)
            g_send(2, k).start()

    def gather(level, k):
        g_send(level, k).wait()
        if level > 0:
            g_send(level - 1, k).start()
        else:
            for t in range(4 * k, 4 * k + 4):
                for col in (t, HALF + t):
                    out[:, col * HD:(col + 1) * HD] = gath[col].astype(BF16)

    here.arrive()
    for s in range(4):
        fetch_down(s).start()
    here.meet()
    m_send(0).start()
    for k in range(CHUNKS):
        o_send(0, k).start()
    merge_stats(0)
    for k in range(CHUNKS):
        merge_heads(0, k)
    for s in range(4, W_SLOTS):
        fetch_down(s).start()
    down(0, 1)
    merge_stats(1)
    merge_heads(1, 0)
    down(1, 3)
    merge_heads(1, 1)
    merge_stats(2)
    merge_heads(2, 0)
    down(3, 4)
    for core in range(2):
        for k in range(CHUNKS):
            wo_copy(core, k).start()
    merge_heads(1, 2)
    down(4, 5)
    merge_heads(1, 3)
    merge_heads(2, 1)
    merge_heads(2, 2)
    down(5, 6)
    for core in range(2):
        for k in range(CHUNKS):
            wo_copy(core, k).wait()
    merge_heads(2, 3)
    for k in range(CHUNKS):
        c_send(k).wait()
    for h in range(2 * OWN):
        ctx[:, h * HD:(h + 1) * HD] = ctxf[h].astype(BF16)
    for k, stage in ORDER:
        if stage == 0:
            project(k)
        elif stage <= 3:
            reduce(stage - 1, k)
        else:
            gather(6 - stage, k)


def tail_call(act, ml, o, hidden, w_down, w_out):
    vm = pl.BlockSpec(memory_space=pltpu.VMEM)
    anyspace = pl.BlockSpec(memory_space=pl.ANY)
    dma = pltpu.SemaphoreType.DMA
    return pl.pallas_call(
        tail_kernel,
        out_shape=jax.ShapeDtypeStruct((ROWS, D), BF16),
        in_specs=[vm, vm, vm, vm, anyspace, anyspace],
        out_specs=vm,
        scratch_shapes=[
            pltpu.VMEM((W_SLOTS, 3072, 512), BF16),
            pltpu.VMEM((2 * OWN * HD, HALF * HD), BF16),
            pltpu.VMEM((NH, ROWS, HD), F32),
            pltpu.VMEM((NH // 2, ROWS, HD), F32),
            pltpu.VMEM((NH // 2, ROWS, HD), F32),
            pltpu.VMEM((NH // 4, ROWS, HD), F32),
            pltpu.VMEM((NH // 8, ROWS, HD), F32),
            pltpu.VMEM((LEVELS, ROWS, HD), F32),
            pltpu.VMEM((LEVELS, ROWS, HD), F32),
            pltpu.VMEM((LEVELS, 2, ROWS, HD), F32),
            pltpu.VMEM((NH // 2, ROWS, HD), F32),
            pltpu.VMEM((NH // 4, ROWS, HD), F32),
            pltpu.VMEM((NH // 8, ROWS, HD), F32),
            pltpu.VMEM((NH, ROWS, HD), F32),
            pltpu.VMEM((2 * OWN, ROWS, HD), F32),
            pltpu.VMEM((ROWS, 2 * OWN * HD), BF16),
            dma((W_SLOTS,)), dma((2, CHUNKS)),
            dma((LEVELS, CHUNKS)), dma((LEVELS, CHUNKS)), dma((LEVELS,)), dma((LEVELS,)), dma((CHUNKS,)), dma((CHUNKS,)),
            dma((LEVELS, F_CHUNKS)), dma((LEVELS, F_CHUNKS)), dma((LEVELS, F_CHUNKS)), dma((LEVELS, F_CHUNKS)),
        ],
        compiler_params=pltpu.CompilerParams(collective_id=1, has_side_effects=True, vmem_limit_bytes=TAIL_LIMIT),
        cost_estimate=pl.CostEstimate(flops=2 * ROWS * D * FF, bytes_accessed=2 * D * FF, transcendentals=0),
        name='tail',
    )(act, ml, o, hidden, w_down, w_out)


def device_step(hidden, ln_gamma, ln_beta, w_qkv, w_out, w_up, w_down, k_cache, v_cache, positions):
    inv_freq = 1.0 / (ROPE_BASE ** (jnp.arange(0, HD, 2, dtype=F32) / HD))
    freq = jnp.concatenate([inv_freq, inv_freq])[None, :]
    inputs = [pltpu.with_memory_space_constraint(v, pltpu.HBM)
              for v in (hidden, ln_gamma[None, :], ln_beta[None, :], positions[None, :])]
    qkv, act = front_call(*inputs, freq, w_qkv, w_up)
    o, ml, k_next, v_next = attn_call(positions, qkv, k_cache, v_cache)
    out = tail_call(act, ml, o, hidden, w_down, w_out)
    return out, k_next, v_next


def solution(mesh):
    cache_spec = P('dp', 'sp', None)
    in_specs = (P('dp', None), P(None), P(None), P(None, None), P(None, None), P(None, 'sp'), P('sp', None), cache_spec, cache_spec, P('dp'))
    out_specs = (P('dp', None), cache_spec, cache_spec)
    return jax.shard_map(device_step, mesh=mesh, in_specs=in_specs, out_specs=out_specs, check_vma=False)
```
